32 devices in a mesh: fsdp: 4 (over z), ctx: 2 (over core), tp: 4 (over y, x).
Axes of the slice: x: 2, y: 2, z: 4, core: 2. Of those that a mesh axis runs over, the one named last changes fastest.
Arguments:
- characters: bfloat16 [8192, 16, 256], P(('fsdp', 'ctx', 'tp')), may hold values from -6 to 6
- counts: int32 [8192], P(('fsdp', 'ctx', 'tp')), may hold values from 1 to 16, as said below
- words_in: bfloat16 [8192, 512], P(('fsdp', 'ctx', 'tp')), may hold values from -6 to 6
- cotangent: bfloat16 [8192, 512], P(('fsdp', 'ctx', 'tp')), may hold values from -6 to 6
- char_prenorm: bfloat16 [256], P('fsdp'), may hold values from 0.099609375 to 1.8984375
- char_qkv: bfloat16 [256, 768], P('fsdp'), may hold values from -0.5 to 0.5
- char_out: bfloat16 [256, 256], P('fsdp'), may hold values from -0.375 to 0.375
- char_midnorm: bfloat16 [256], P('fsdp'), may hold values from 0.099609375 to 1.8984375
- char_up: bfloat16 [256, 1024], P('fsdp'), may hold values from -0.375 to 0.375
- char_down: bfloat16 [1024, 256], P('fsdp'), may hold values from -0.1875 to 0.1875
- pool_query: bfloat16 [256], P('fsdp'), may hold values from -0.375 to 0.375
- char_proj: bfloat16 [256, 512], P('fsdp'), may hold values from -0.375 to 0.375
- word_prenorm: bfloat16 [512], P('fsdp'), may hold values from 0.099609375 to 1.8984375
- word_qkv: bfloat16 [512, 3, 512], P('fsdp', None, 'tp'), may hold values from -0.375 to 0.375
- word_out: bfloat16 [512, 512], P('tp', 'fsdp'), may hold values from -0.5 to 0.5
- word_midnorm: bfloat16 [512], P('fsdp'), may hold values from 0.099609375 to 1.8984375
- word_up: bfloat16 [512, 2048], P('fsdp', 'tp'), may hold values from -0.25 to 0.25
- word_down: bfloat16 [2048, 512], P('tp', 'fsdp'), may hold values from -0.125 to 0.125
Outputs:
- block_out: bfloat16 [8192, 512], P(('fsdp', 'ctx', 'tp'))
- chars_grad: float32 [8192, 16, 256], P(('fsdp', 'ctx', 'tp'))
- words_grad: float32 [8192, 512], P(('fsdp', 'ctx', 'tp'))
- branch_rms: float32 [3, 8192], P(None, ('fsdp', 'ctx', 'tp'))
- char_prenorm_grad: float32 [256], P('fsdp')
- char_qkv_grad: float32 [256, 768], P('fsdp')
- char_out_grad: float32 [256, 256], P('fsdp')
- char_midnorm_grad: float32 [256], P('fsdp')
- char_up_grad: float32 [256, 1024], P('fsdp')
- char_down_grad: float32 [1024, 256], P('fsdp')
- pool_query_grad: float32 [256], P('fsdp')
- char_proj_grad: float32 [256, 512], P('fsdp')
- word_prenorm_grad: float32 [512], P('fsdp')
- word_qkv_grad: float32 [512, 3, 512], P('fsdp', None, 'tp')
- word_out_grad: float32 [512, 512], P('tp', 'fsdp')
- word_midnorm_grad: float32 [512], P('fsdp')
- word_up_grad: float32 [512, 2048], P('fsdp', 'tp')
- word_down_grad: float32 [2048, 512], P('tp', 'fsdp')
The draws below stay inside these ranges and needn't reach their ends.
Inputs may be any that keep to these rules, and one draw needn't show every extreme that they name: `counts`: the number of real characters of each word; slots from it to 15 are padding.
All inputs are finite; a program needn't handle non-finite values.
Results may differ from the reference program's by a relative error of at most 0.03.
The reference program's roundings to bfloat16 on the way count: a program that leaves them out, or rounds other values in their place, can miss the bound.
Values may be sent and summed in bfloat16 or wider, within the bound.
A program may use at most 256 MiB of HBM per device.

```python
import math
import jax
import jax.numpy as jnp
from jax import lax

CH = 16
DC = 256
CHEADS = 4
CFF = 1024
D = 512
HEADS = 8
FF = 2048
BLOCK = 256
SEQLEN = 2048
WORDS = 8192


def draw_counts(key, part):
    key_cap, key_len = jax.random.split(jax.random.fold_in(key, 17))
    groups = WORDS // BLOCK
    caps = jax.random.randint(key_cap, (groups,), 2, CH + 1)
    caps = caps.at[0].set(CH)
    per_word = jnp.repeat(caps, BLOCK)
    drawn = jax.random.randint(key_len, (WORDS,), 1, per_word + 1)
    position = jnp.arange(WORDS) % BLOCK
    drawn = jnp.where(position == 0, per_word, drawn)
    drawn = jnp.where(position == 1, 1, drawn)
    return drawn.astype(jnp.int32)


def steps_of(own_key, shape, shards, smallest, largest):
    def one(dim, blocks):
        steps = jax.random.uniform(jax.random.fold_in(jax.random.fold_in(own_key, 6), dim), (blocks,), jnp.float32, smallest / len(shards), largest / len(shards))
        return jnp.repeat(jnp.exp(steps), shape[dim] // blocks).reshape((-1,) + (1,) * (len(shape) - dim - 1))

    factor_of = one(*shards[0])
    for cut in shards[1:]:
        factor_of = factor_of * one(*cut)
    return factor_of


def gaussian(stream_key, shape, scale, bound, shards=(), dtype=jnp.bfloat16):
    loudness = steps_of(stream_key, shape, shards, -0.22, 0.18) if shards else 1.0
    array = jax.random.normal(stream_key, shape, jnp.float32) * scale * loudness
    return jnp.minimum(jnp.maximum(array, -bound), bound).astype(dtype)


def setup_inputs(seed: int = 0) -> dict:
    splits = jax.random.split(jax.random.key(seed), 19)
    characters = gaussian(splits[0], (WORDS, CH, DC), 1.0, 6.0, ((0, 32),))
    counts = draw_counts(jax.random.fold_in(splits[18], 71), 0)
    words_in = gaussian(splits[2], (WORDS, D), 1.0, 6.0, ((0, 32),))
    cotangent = gaussian(splits[3], (WORDS, D), 1.0, 6.0, ((0, 32),))
    char_prenorm = jnp.clip(1.0 + 0.18 * jax.random.normal(splits[4], (DC,), jnp.float32), 0.099609375, 1.8984375).astype(jnp.bfloat16)
    char_qkv = gaussian(splits[5], (DC, 3 * DC), (DC // 2) ** -0.5, 0.5, ((0, 4),))
    char_out = gaussian(splits[6], (DC, DC), DC ** -0.5, 0.375, ((0, 4),))
    char_midnorm = jnp.clip(1.0 + 0.18 * jax.random.normal(splits[7], (DC,), jnp.float32), 0.099609375, 1.8984375).astype(jnp.bfloat16)
    char_up = gaussian(splits[8], (DC, CFF), DC ** -0.5, 0.375, ((0, 4),))
    char_down = gaussian(splits[9], (CFF, DC), CFF ** -0.5, 0.1875, ((0, 4),))
    pool_query = gaussian(splits[10], (DC,), DC ** -0.5, 0.375, ((0, 4),))
    char_proj = gaussian(splits[11], (DC, D), DC ** -0.5, 0.375, ((0, 4),))
    word_prenorm = jnp.clip(1.0 + 0.18 * jax.random.normal(splits[12], (D,), jnp.float32), 0.099609375, 1.8984375).astype(jnp.bfloat16)
    word_qkv = gaussian(splits[13], (D, 3, D), (D // 2) ** -0.5, 0.375, ((0, 4), (2, 4)))
    word_out = gaussian(splits[14], (D, D), (D // 4) ** -0.5, 0.5, ((0, 4), (1, 4)))
    word_midnorm = jnp.clip(1.0 + 0.18 * jax.random.normal(splits[15], (D,), jnp.float32), 0.099609375, 1.8984375).astype(jnp.bfloat16)
    word_up = gaussian(splits[16], (D, FF), D ** -0.5, 0.25, ((0, 4), (1, 4)))
    word_down = gaussian(splits[17], (FF, D), FF ** -0.5, 0.125, ((0, 4), (1, 4)))
    return {"characters": characters, "counts": counts, "words_in": words_in, "cotangent": cotangent, "char_prenorm": char_prenorm, "char_qkv": char_qkv, "char_out": char_out, "char_midnorm": char_midnorm, "char_up": char_up, "char_down": char_down, "pool_query": pool_query, "char_proj": char_proj, "word_prenorm": word_prenorm, "word_qkv": word_qkv, "word_out": word_out, "word_midnorm": word_midnorm, "word_up": word_up, "word_down": word_down}


EPSILON = 1e-05
MASKED = -1e+30
HIGHEST = lax.Precision.HIGHEST

@jax.custom_vjp
def low(v):
    return lax.optimization_barrier(v.astype(jnp.bfloat16)).astype(jnp.float32)

@jax.custom_vjp
def low_back(v):
    return v

def low_keep(v):
    return (low(v), None)

def low_pass(kept, grad):
    return (grad,)

def back_keep(v):
    return (v, None)

def back_low(kept, grad):
    return (low(grad),)
low.defvjp(low_keep, low_pass)
low_back.defvjp(back_keep, back_low)

def layer_norm(row_values, gain_vec):
    centered = row_values - lax.optimization_barrier(jnp.mean(row_values, axis=-1, keepdims=True))
    spread = lax.optimization_barrier(jnp.mean(centered * centered, axis=-1, keepdims=True))
    return centered * lax.rsqrt(spread + EPSILON) * gain_vec

def product(left_side, right_side):
    return low_back(jnp.dot(left_side, right_side, precision=HIGHEST, preferred_element_type=jnp.float32))

def pool_words(states, query_vec, present):
    logits = lax.optimization_barrier(jnp.sum(states * query_vec, axis=-1))
    logits = jnp.where(present, logits, MASKED)
    weights = jax.nn.softmax(logits, axis=-1)
    return lax.optimization_barrier(jnp.sum(weights[:, :, None] * states, axis=1))

def char_block(params, characters, present):
    prenorm, qkv_w, out_w, midnorm, up_w, down_w, pool_vec, proj_w = params
    word_count = characters.shape[0]
    head_size = DC // CHEADS
    embedded = characters.reshape(word_count * CH, DC)
    normed = low(layer_norm(embedded, prenorm))
    packed = low(product(normed, qkv_w)).reshape(word_count, CH, 3, CHEADS, head_size)
    scores = low_back(jnp.einsum('wqhe,wkhe->whqk', packed[:, :, 0], packed[:, :, 1], precision=HIGHEST)) * head_size ** (-0.5)
    scores = jnp.where(present[:, None, None, :], scores, MASKED)
    attention = low(jax.nn.softmax(scores, axis=-1))
    mixed_rows = low(low_back(jnp.einsum('whqk,wkhe->wqhe', attention, packed[:, :, 2], precision=HIGHEST)))
    after_attn = embedded + product(mixed_rows.reshape(word_count * CH, DC), out_w)
    middle = low(layer_norm(after_attn, midnorm))
    upper_rows = low(jax.nn.gelu(product(middle, up_w)))
    after_mlp = after_attn + product(upper_rows, down_w)
    pooled = pool_words(after_mlp.reshape(word_count, CH, DC), pool_vec, present)
    return product(low(pooled), proj_w)

def attend_core(query_blk, query_pos, key_rows, value_rows):
    head_size = D // HEADS
    scores = low_back(jnp.einsum('qhe,khe->hqk', query_blk, key_rows, precision=HIGHEST)) * head_size ** (-0.5)
    key_block = jnp.arange(key_rows.shape[0]) // BLOCK
    allowed = key_block[None, :] <= (query_pos // BLOCK)[:, None]
    scores = jnp.where(allowed[None], scores, MASKED)
    attention = low(jax.nn.softmax(scores, axis=-1))
    return low(low_back(jnp.einsum('hqk,khe->qhe', attention, value_rows, precision=HIGHEST)))

def word_block(params, start_rows):
    prenorm, qkv_w, out_w, midnorm, up_w, down_w = params
    row_count = start_rows.shape[0]
    head_size = D // HEADS
    normed = low(layer_norm(start_rows, prenorm))
    packed = low(product(normed, qkv_w.reshape(D, 3 * D))).reshape(row_count, 3, HEADS, head_size)
    key_rows = packed[:, 1]
    value_rows = packed[:, 2]
    block_rows = math.gcd(row_count, 512)
    block_count = row_count // block_rows
    positions = jnp.arange(row_count)
    attend_saved = jax.checkpoint(attend_core)
    mixed_rows = lax.map(lambda item: attend_saved(item[0], item[1], key_rows, value_rows), (packed[:, 0].reshape(block_count, block_rows, HEADS, head_size), positions.reshape(block_count, block_rows)))
    attn_out = product(mixed_rows.reshape(row_count, D), out_w)
    after_attn = start_rows + attn_out
    upper_rows = low(jax.nn.gelu(product(low(layer_norm(after_attn, midnorm)), up_w)))
    mlp_out = product(upper_rows, down_w)
    return (after_attn + mlp_out, (attn_out, mlp_out))

def root_mean(row_values):
    return jnp.sqrt(lax.optimization_barrier(jnp.mean(row_values * row_values, axis=-1)))

def reference(characters, counts, words_in, cotangent, char_prenorm, char_qkv, char_out, char_midnorm, char_up, char_down, pool_query, char_proj, word_prenorm, word_qkv, word_out, word_midnorm, word_up, word_down):
    weights = tuple((weight.astype(jnp.float32) for weight in (char_prenorm, char_qkv, char_out, char_midnorm, char_up, char_down, pool_query, char_proj, word_prenorm, word_qkv, word_out, word_midnorm, word_up, word_down)))
    seq_count = WORDS // SEQLEN
    chars_seq = characters.reshape(seq_count, SEQLEN, CH, DC)
    counts_seq = counts.reshape(seq_count, SEQLEN)
    words_seq = words_in.reshape(seq_count, SEQLEN, D)
    cot_seq = cotangent.reshape(seq_count, SEQLEN, D)

    def one_sequence(totals, inputs):
        chars_one, counts_one, words_one, cot_one = inputs
        present = jnp.arange(CH)[None, :] < counts_one[:, None]

        def whole_layer(params, chars_float, words_float):
            start_rows = words_float + char_block(params[:8], chars_float, present)
            return word_block(params[8:], start_rows)
        final_rows, pullback, branches = jax.vjp(whole_layer, weights, chars_one.astype(jnp.float32), words_one.astype(jnp.float32), has_aux=True)
        param_grads, chars_grad, words_grad = pullback(cot_one.astype(jnp.float32))
        totals = tuple((first_sum + other_sum for first_sum, other_sum in zip(totals, param_grads)))
        rms_rows = jnp.stack([root_mean(branches[0]), root_mean(branches[1]), root_mean(final_rows)])
        return (totals, (final_rows.astype(jnp.bfloat16), chars_grad, words_grad, rms_rows))
    zero_sums = tuple((jnp.zeros(weight.shape, jnp.float32) for weight in weights))
    totals, results = lax.scan(one_sequence, zero_sums, (chars_seq, counts_seq, words_seq, cot_seq))
    block_out = results[0].reshape(WORDS, D)
    chars_grad = results[1].reshape(WORDS, CH, DC)
    words_grad = results[2].reshape(WORDS, D)
    branch_rms = jnp.moveaxis(results[3], 0, 1).reshape(3, WORDS)
    return (block_out, chars_grad, words_grad, branch_rms, totals[0], totals[1], totals[2], totals[3], totals[4], totals[5], totals[6], totals[7], totals[8], totals[9], totals[10], totals[11], totals[12], totals[13])
```

```python
import functools

import jax
import jax.numpy as jnp
from jax import lax
from jax.experimental import pallas as pl
from jax.experimental.pallas import tpu as pltpu
from jax.sharding import PartitionSpec as P

CHEADS = 4
HEADS = 8
HEAD = 64
EPSILON = 1e-05
MASKED = -1e30
CGELU = 0.7978845608028654
AGELU = 0.044715
ROWS = 512
GROUP = 128
F32 = jnp.float32
BF16 = jnp.bfloat16
VMEM_LIMIT = 66_000_000


def mm(a, b):
    return lax.dot_general(a, b, (((1,), (0,)), ((), ())), preferred_element_type=F32)


def mm_nt(a, b):
    return lax.dot_general(a, b, (((1,), (1,)), ((), ())), preferred_element_type=F32)


def mm_tn(a, b):
    return lax.dot_general(a, b, (((0,), (0,)), ((), ())), preferred_element_type=F32)


def ln_parts(x):
    c = x - jnp.mean(x, axis=-1, keepdims=True)
    r = lax.rsqrt(jnp.mean(c * c, axis=-1, keepdims=True) + EPSILON)
    return c * r, r


def ln_back(xhat, r, gain, g):
    gg = g * gain
    a = jnp.mean(gg, axis=-1, keepdims=True)
    b = jnp.mean(gg * xhat, axis=-1, keepdims=True)
    return r * (gg - a - xhat * b)


def gelu_both(x):
    x2 = x * x
    y = (CGELU * AGELU) * x2 + CGELU
    hp = 0.5 * jnp.tanh(x * y) + 0.5
    g = x * hp
    d = hp + (g - g * hp) * (6.0 * y - 4.0 * CGELU)
    return g, d


def pair_masks(rows):
    lane = lax.broadcasted_iota(jnp.int32, (rows, 128), 1)
    return lane < HEAD


def split_heads(x, low_lanes):
    zero = jnp.zeros_like(x)
    return jnp.where(low_lanes, x, zero), jnp.where(low_lanes, zero, x)


def stack_heads(x, low_lanes):
    a, b = split_heads(x, low_lanes)
    return jnp.concatenate([a, b], axis=0)


def word_of_lane(width):
    return (lax.broadcasted_iota(jnp.int32, (16, width), 1) % GROUP) // 16


def compress(blocks, lane_word):
    out = blocks[0:16, :]
    for w in range(1, GROUP // 16):
        out = jnp.where(lane_word == w, blocks[16 * w : 16 * w + 16, :], out)
    return out


def expand(dense, lane_word):
    zero = jnp.zeros_like(dense)
    return jnp.concatenate(
        [jnp.where(lane_word == w, dense, zero) for w in range(GROUP // 16)], axis=0
    )


def pool_weights(am, q_row, cnt_col):
    words = am.shape[0] // 16
    am3 = am.reshape(words, 16, am.shape[1])
    logits = jnp.sum(am * q_row, axis=-1, keepdims=True)
    slot = (lax.broadcasted_iota(jnp.int32, (am.shape[0], 1), 0) % 16).astype(F32)
    logits = jnp.where(slot < cnt_col, logits, MASKED).reshape(words, 16, 1)
    e = jnp.exp(logits - jnp.max(logits, axis=1, keepdims=True))
    w = e / jnp.sum(e, axis=1, keepdims=True)
    return am3, w


def count_column(cnt_row):
    return jnp.transpose(jnp.broadcast_to(cnt_row, (GROUP, GROUP)))[:, 0:1]


def char_fwd_tile(x, cnt, weights):
    g1, wqkv, wout, g2, wup, wdown, pq = weights
    rows = x.shape[0]
    groups = rows // GROUP
    xf = x.astype(F32)
    xhat, _ = ln_parts(xf)
    normed = (xhat * g1).astype(BF16)
    packed = mm(normed, wqkv).astype(BF16)
    low = pair_masks(GROUP)
    lw = word_of_lane(2 * GROUP)
    slot = lax.broadcasted_iota(jnp.int32, (16, 2 * GROUP), 0).astype(F32)
    probs, mixed, cols = [], [], []
    for g in range(groups):
        r = slice(g * GROUP, (g + 1) * GROUP)
        cnt_row = cnt[g : g + 1, :]
        cols.append(count_column(cnt_row))
        cnt2 = jnp.concatenate([cnt_row, cnt_row], axis=1)
        valid = slot < cnt2
        pg, mg = [], []
        for p in range(CHEADS // 2):
            q = packed[r, 128 * p : 128 * p + 128] * BF16(0.125)
            k = packed[r, 256 + 128 * p : 384 + 128 * p]
            v = packed[r, 512 + 128 * p : 640 + 128 * p]
            st = mm_nt(k, stack_heads(q, low))
            s = jnp.where(valid, compress(st, lw), MASKED)
            e = jnp.exp(s - jnp.max(s, axis=0, keepdims=True))
            pr = e / jnp.sum(e, axis=0, keepdims=True)
            pt = expand(pr.astype(BF16), lw)
            o = mm_tn(pt, v)
            pg.append(pr)
            mg.append(jnp.where(low, o[:GROUP], o[GROUP:]))
        probs.append(jnp.concatenate(pg, axis=1))
        mixed.append(jnp.concatenate(mg, axis=1))
    probs = jnp.concatenate(probs, axis=0)
    mixed = jnp.concatenate(mixed, axis=0).astype(BF16)
    aa = xf + mm(mixed, wout)
    ahat, _ = ln_parts(aa)
    middle = (ahat * g2).astype(BF16)
    upper, dgelu = gelu_both(mm(middle, wup))
    upper = upper.astype(BF16)
    am = aa + mm(upper, wdown)
    am3, w = pool_weights(am, pq, jnp.concatenate(cols, axis=0))
    pooled = jnp.sum(w * am3, axis=1)
    return packed, probs, mixed, aa, upper, dgelu.astype(BF16), am, pooled.astype(BF16)


def char_fwd_kernel(x, cnt, g1, wqkv, wout, g2, wup, wdown, pq, *outs):
    weights = (g1[...].astype(F32), wqkv[...], wout[...], g2[...].astype(F32), wup[...], wdown[...], pq[...].astype(F32))
    for ref, val in zip(outs, char_fwd_tile(x[...], cnt[0], weights)):
        ref[...] = val


def full_spec(shape):
    return pl.BlockSpec(shape, lambda i: (0,) * len(shape))


def rows_spec(rows, width):
    return pl.BlockSpec((rows, width), lambda i: (i, 0))


def char_forward(x, cnt, weights):
    total = x.shape[0]
    tiles = total // ROWS
    widths = [(ROWS, 768, BF16), (ROWS // 8, 512, F32), (ROWS, 256, BF16), (ROWS, 256, F32), (ROWS, 1024, BF16), (ROWS, 1024, BF16), (ROWS, 256, F32), (ROWS // 16, 256, BF16)]
    return pl.pallas_call(
        char_fwd_kernel,
        grid=(tiles,),
        in_specs=[rows_spec(ROWS, 256), pl.BlockSpec((1, ROWS // GROUP, GROUP), lambda i: (i, 0, 0))] + [full_spec(w.shape) for w in weights],
        out_specs=[rows_spec(r, w) for r, w, _ in widths],
        out_shape=[jax.ShapeDtypeStruct((r * tiles, w), d) for r, w, d in widths],
        compiler_params=pltpu.CompilerParams(vmem_limit_bytes=VMEM_LIMIT, dimension_semantics=("arbitrary",)),
        name="char_forward",
    )(x, cnt, *weights)


def char_bwd_tile(x, cnt, packed, probs, mixed, aa, upper, dgelu, am, gpool_ref, base, weights):
    g1, wqkv, wout, g2, wup, wdown, pq = weights
    rows = x.shape[0]
    groups = rows // GROUP
    words = rows // 16
    low = pair_masks(GROUP)
    lw = word_of_lane(2 * GROUP)
    cols = jnp.concatenate([count_column(cnt[g : g + 1, :]) for g in range(groups)], axis=0)
    am3, w = pool_weights(am, pq, cols)
    gp = jnp.concatenate(
        [jnp.broadcast_to(gpool_ref[pl.ds(base + i, 1), :], (16, 256)) for i in range(words)], axis=0
    )
    dw = jnp.sum(gp * am, axis=-1, keepdims=True).reshape(words, 16, 1)
    dlog = (w * (dw - jnp.sum(w * dw, axis=1, keepdims=True))).reshape(rows, 1)
    gm = w.reshape(rows, 1) * gp + dlog * pq
    d_pq = jnp.sum(dlog * am, axis=0, keepdims=True)
    gdl = gm.astype(BF16)
    d_down_t = mm_tn(gdl, upper)
    ghid = (dgelu.astype(F32) * mm_nt(gdl, wdown)).astype(BF16)
    ahat, ar = ln_parts(aa)
    middle = (ahat * g2).astype(BF16)
    d_up = mm_tn(middle, ghid)
    gmid = mm_nt(ghid, wup)
    gca = gm + ln_back(ahat, ar, g2, gmid)
    d_g2 = jnp.sum(gmid * ahat, axis=0, keepdims=True)
    gcl = gca.astype(BF16)
    d_out = mm_tn(mixed, gcl)
    gcm = mm_nt(gcl, wout).astype(BF16)
    dqkv = []
    for g in range(groups):
        r = slice(g * GROUP, (g + 1) * GROUP)
        dq_g, dk_g, dv_g = [], [], []
        for p in range(CHEADS // 2):
            q = packed[r, 128 * p : 128 * p + 128] * BF16(0.125)
            k = packed[r, 256 + 128 * p : 384 + 128 * p]
            v = packed[r, 512 + 128 * p : 640 + 128 * p]
            do = stack_heads(gcm[r, 128 * p : 128 * p + 128], low)
            pr = probs[16 * g : 16 * g + 16, 256 * p : 256 * p + 256]
            dp = compress(mm_nt(v, do), lw)
            ds = (pr * (dp - jnp.sum(pr * dp, axis=0, keepdims=True))).astype(BF16)
            dst = expand(ds, lw)
            pt = expand(pr.astype(BF16), lw)
            dv_g.append(mm(pt, do))
            dk_g.append(mm(dst, stack_heads(q, low)))
            o = mm_tn(dst, k)
            dq_g.append(jnp.where(low, o[:GROUP], o[GROUP:]) * 0.125)
        dqkv.append(jnp.concatenate(dq_g + dk_g + dv_g, axis=1))
    dqkv = jnp.concatenate(dqkv, axis=0).astype(BF16)
    xf = x.astype(F32)
    xhat, xr = ln_parts(xf)
    normed = (xhat * g1).astype(BF16)
    d_qkv = mm_tn(normed, dqkv)
    gn = mm_nt(dqkv, wqkv)
    d_g1 = jnp.sum(gn * xhat, axis=0, keepdims=True)
    cg = gca + ln_back(xhat, xr, g1, gn)
    return cg, (d_g1, d_qkv, d_out, d_g2, d_up, d_down_t, d_pq)


def char_bwd_kernel(x, cnt, packed, probs, mixed, aa, upper, dgelu, am, gpool, g1, wqkv, wout, g2, wup, wdown, pq, cg, *accs):
    weights = (g1[...].astype(F32), wqkv[...], wout[...], g2[...].astype(F32), wup[...], wdown[...], pq[...].astype(F32))
    step = pl.program_id(0)

    @pl.when(step == 0)
    def _():
        for acc in accs:
            acc[...] = jnp.zeros_like(acc)

    out, sums = char_bwd_tile(
        x[...], cnt[0], packed[...], probs[...], mixed[...], aa[...], upper[...], dgelu[...], am[...],
        gpool, step * (ROWS // 16), weights,
    )
    cg[...] = out
    for acc, val in zip(accs, sums):
        acc[...] += val


def char_backward(x, cnt, saved, gpool, weights):
    total = x.shape[0]
    tiles = total // ROWS
    widths = [(ROWS, 768), (ROWS // 8, 512), (ROWS, 256), (ROWS, 256), (ROWS, 1024), (ROWS, 1024), (ROWS, 256)]
    acc_shapes = [(1, 256), (256, 768), (256, 256), (1, 256), (256, 1024), (256, 1024), (1, 256)]
    return pl.pallas_call(
        char_bwd_kernel,
        grid=(tiles,),
        in_specs=[rows_spec(ROWS, 256), pl.BlockSpec((1, ROWS // GROUP, GROUP), lambda i: (i, 0, 0))]
        + [rows_spec(r, w) for r, w in widths]
        + [full_spec(gpool.shape)]
        + [full_spec(w.shape) for w in weights],
        out_specs=[rows_spec(ROWS, 256)] + [full_spec(s) for s in acc_shapes],
        out_shape=[jax.ShapeDtypeStruct((total, 256), F32)] + [jax.ShapeDtypeStruct(s, F32) for s in acc_shapes],
        compiler_params=pltpu.CompilerParams(vmem_limit_bytes=VMEM_LIMIT, dimension_semantics=("arbitrary",)),
        name="char_backward",
    )(x, cnt, *saved, gpool, *weights)


def word_kernel(
    axes, nblk,
    xall, start, cot, wq, wk, wv, wout, g2, wup, wdown,
    block_out, rms, gaa, dx, d_q, d_k, d_v, d_out, d_g2, d_up, d_down,
    kk, vv, kt, vt, ss, ee, qm, dom, mx, ll, ot, dqt, wkt, wvt, dk_acc, dv_acc, dlt, dk_sum, dv_sum, dx_own,
):
    own = axes()
    blk = start.shape[0]
    low = pair_masks(blk)

    def rows(j):
        return pl.ds(pl.multiple_of(j * blk, blk), blk)

    wkt[...] = jnp.transpose(wk[...])
    wvt[...] = jnp.transpose(wv[...])
    xown = xall[rows(own), :]
    q = mm(xown, wq[...]).astype(BF16) * BF16(0.125)
    for p in range(HEADS // 2):
        a, b = split_heads(q[:, 128 * p : 128 * p + 128], low)
        qm[2 * p] = a
        qm[2 * p + 1] = b
    mx[...] = jnp.full(mx.shape, MASKED, F32)
    ll[...] = jnp.zeros(ll.shape, F32)
    ot[...] = jnp.zeros(ot.shape, F32)
    dqt[...] = jnp.zeros(dqt.shape, F32)
    dk_sum[...] = jnp.zeros(dk_sum.shape, F32)
    dv_sum[...] = jnp.zeros(dv_sum.shape, F32)
    dx[...] = jnp.zeros(dx.shape, BF16)

    half = HEADS // 2

    def scores_of(j, heads):
        for h in heads:
            p = h // 2
            s = mm_nt(kk[j, :, 128 * p : 128 * p + 128], qm[h])
            ss[j, h % half] = s
            mx[h] = jnp.maximum(mx[h], jnp.max(s.reshape(blk // 8, 8, blk), axis=0))

    def mix_of(j, heads):
        for h in heads:
            e = jnp.exp(ss[j, h % half] - mx[h, 0:1, :])
            ll[h] += jnp.sum(e.reshape(blk // 8, 8, blk), axis=0)
            eb = e.astype(BF16)
            ee[j, h] = eb
            ot[64 * h : 64 * h + 64, :] += mm(vt[j, 64 * h : 64 * h + 64, :], eb)

    def top_of(heads):
        for h in heads:
            mx[h] = jnp.broadcast_to(jnp.max(mx[h], axis=0, keepdims=True), (8, blk))

    first, second = range(half), range(half, HEADS)

    @pl.loop(0, own + 1)
    def _(j):
        xj = xall[rows(j), :]
        kk[j] = mm(xj, wk[...]).astype(BF16)
        vv[j] = mm(xj, wv[...]).astype(BF16)
        kt[j] = mm_nt(wkt[...], xj).astype(BF16)
        vt[j] = mm_nt(wvt[...], xj).astype(BF16)
        scores_of(j, first)

    top_of(first)

    @pl.loop(0, own + 1)
    def _(j):
        mix_of(j, first)
        scores_of(j, second)

    top_of(second)

    @pl.loop(0, own + 1)
    def _(j):
        mix_of(j, second)

    for h in range(HEADS):
        linv = 1.0 / jnp.sum(ll[h], axis=0, keepdims=True)
        ll[h] = jnp.broadcast_to(linv, (8, blk))
        ot[64 * h : 64 * h + 64, :] = ot[64 * h : 64 * h + 64, :] * linv
    mixed_t = ot[...].astype(BF16)
    attn = mm(jnp.transpose(mixed_t), wout[...])
    awa = start[...] + attn
    ahat, ar = ln_parts(awa)
    g2v = g2[...].astype(F32)
    n2 = (ahat * g2v).astype(BF16)
    upper, dgelu = gelu_both(mm(n2, wup[...]))
    upper = upper.astype(BF16)
    mlp = mm(upper, wdown[...])
    final = awa + mlp
    block_out[...] = final.astype(BF16)
    lane = lax.broadcasted_iota(jnp.int32, (blk, 128), 1)
    cols = [jnp.sqrt(jnp.mean(v * v, axis=-1, keepdims=True)) for v in (attn, mlp, final)]
    rms[...] = jnp.transpose(jnp.where(lane == 0, cols[0], jnp.where(lane == 1, cols[1], cols[2])))[0:8, :]
    cotv = cot[...]
    d_down[...] = mm_tn(upper, cotv).astype(BF16)
    ghid = (dgelu * mm_nt(cotv, wdown[...])).astype(BF16)
    d_up[...] = mm_tn(n2, ghid).astype(BF16)
    gn2 = mm_nt(ghid, wup[...])
    d_g2[...] = jnp.sum(gn2 * ahat, axis=0, keepdims=True)
    ga = cotv.astype(F32) + ln_back(ahat, ar, g2v, gn2)
    gaa[...] = ga
    gal = ga.astype(BF16)
    d_out[...] = mm(mixed_t, gal).astype(BF16)
    do_t = mm_nt(wout[...], gal).astype(BF16)
    do_s = []
    for h in range(HEADS):
        r = slice(64 * h, 64 * h + 64)
        d = do_t[r, :].astype(F32)
        linv = ll[h, 0:1, :]
        dlt[h] = jnp.broadcast_to(jnp.sum(d * ot[r, :], axis=0, keepdims=True) * linv, (8, blk))
        do_s.append((d * linv).astype(BF16))
    do = jnp.transpose(jnp.concatenate(do_s, axis=0))
    for p in range(HEADS // 2):
        a, b = split_heads(do[:, 128 * p : 128 * p + 128], low)
        dom[2 * p] = a
        dom[2 * p + 1] = b

    def back_of(j, _):
        for p in range(HEADS // 2):
            c = slice(128 * p, 128 * p + 128)
            vp = vv[j, :, c]
            dk = None
            for h in (2 * p, 2 * p + 1):
                e = ee[j, h]
                dp = mm_nt(vp, dom[h])
                ds = (e.astype(F32) * (dp - dlt[h, 0:1, :])).astype(BF16)
                dvh = mm(e, dom[h])
                dkh = mm(ds, qm[h])
                dk, dv = (dkh, dvh) if dk is None else (dk + dkh, dv + dvh)
                dqt[64 * h : 64 * h + 64, :] += mm(kt[j, 64 * h : 64 * h + 64, :], ds)
            dk_acc[:, c] = dk.astype(BF16)
            dv_acc[:, c] = dv.astype(BF16)
        dk = dk_acc[...]
        dv = dv_acc[...]
        xj = xall[rows(j), :]
        dxj = mm_nt(dk, wk[...]) + mm_nt(dv, wv[...])
        dx[rows(j), :] = dxj.astype(BF16)
        dx_own[...] = dxj
        xt = jnp.transpose(xj)
        dk_sum[...] += mm(xt, dk)
        dv_sum[...] += mm(xt, dv)
        return 0

    lax.fori_loop(0, own + 1, back_of, 0)
    dq = jnp.transpose((dqt[...] * 0.125).astype(BF16))
    d_q[...] = mm_tn(xown, dq).astype(BF16)
    d_k[...] = dk_sum[...].astype(BF16)
    d_v[...] = dv_sum[...].astype(BF16)
    dx[rows(own), :] = (dx_own[...] + mm_nt(dq, wq[...])).astype(BF16)


def word_section(xall, start, cot, wq, wk, wv, wout, g2, wup, wdown):
    blk, width = start.shape
    nblk = xall.shape[0] // blk
    ff = wup.shape[1]

    def axes():
        return lax.axis_index("ctx") * lax.axis_size("tp") + lax.axis_index("tp")

    out_shapes = [((blk, width), BF16), ((8, blk), F32), ((blk, width), F32), ((nblk * blk, width), BF16)]
    out_shapes += [((width, width), BF16)] * 4 + [((1, width), F32), ((width, ff), BF16), ((ff, width), BF16)]
    vm = pl.BlockSpec(memory_space=pltpu.VMEM)
    return pl.pallas_call(
        functools.partial(word_kernel, axes, nblk),
        in_specs=[vm] * 10,
        out_specs=[vm] * len(out_shapes),
        out_shape=[jax.ShapeDtypeStruct(s, d) for s, d in out_shapes],
        scratch_shapes=[
            pltpu.VMEM((nblk, blk, width), BF16),
            pltpu.VMEM((nblk, blk, width), BF16),
            pltpu.VMEM((nblk, width, blk), BF16),
            pltpu.VMEM((nblk, width, blk), BF16),
            pltpu.VMEM((nblk, HEADS // 2, blk, blk), F32),
            pltpu.VMEM((nblk, HEADS, blk, blk), BF16),
            pltpu.VMEM((HEADS, blk, 128), BF16),
            pltpu.VMEM((HEADS, blk, 128), BF16),
            pltpu.VMEM((HEADS, 8, blk), F32),
            pltpu.VMEM((HEADS, 8, blk), F32),
            pltpu.VMEM((width, blk), F32),
            pltpu.VMEM((width, blk), F32),
            pltpu.VMEM((width, width), BF16),
            pltpu.VMEM((width, width), BF16),
            pltpu.VMEM((blk, width), BF16),
            pltpu.VMEM((blk, width), BF16),
            pltpu.VMEM((HEADS, 8, blk), F32),
            pltpu.VMEM((width, width), F32),
            pltpu.VMEM((width, width), F32),
            pltpu.VMEM((blk, width), F32),
        ],
        compiler_params=pltpu.CompilerParams(vmem_limit_bytes=VMEM_LIMIT),
        name="word_section",
    )(xall, start, cot, wq, wk, wv, wout, g2, wup, wdown)


def gather(x, name, axis):
    return lax.all_gather(x, name, axis=axis, tiled=True)


def scatter(x, name, axis):
    return lax.psum_scatter(x, name, scatter_dimension=axis, tiled=True)


def local(characters, counts, words_in, cotangent, char_prenorm, char_qkv, char_out, char_midnorm, char_up, char_down,
          pool_query, char_proj, word_prenorm, word_qkv, word_out, word_midnorm, word_up, word_down):
    words, slots, cdim = characters.shape
    x = characters.reshape(words * slots, cdim)
    cnt = jnp.repeat(counts.astype(F32), slots).reshape(words * slots // ROWS, ROWS // GROUP, GROUP)
    names = (char_prenorm, char_qkv, char_out, char_midnorm, char_up, char_down, pool_query)
    weights = [gather(w, "fsdp", 0) for w in names]
    weights = [w.reshape(1, -1) if w.ndim == 1 else w for w in weights]
    proj = gather(char_proj, "fsdp", 0)
    g_word1 = gather(word_prenorm, "fsdp", 0).astype(F32)
    g_word2 = gather(word_midnorm, "fsdp", 0).reshape(1, -1)
    wqkv = gather(gather(jnp.moveaxis(word_qkv, 1, 0), "fsdp", 1), "tp", 2)
    wout = gather(gather(word_out, "fsdp", 1), "tp", 0)
    wup = gather(gather(word_up, "fsdp", 0), "tp", 1)
    wdown = gather(gather(word_down, "fsdp", 1), "tp", 0)

    *saved, pooled_low = char_forward(x, cnt, weights)
    start = words_in.astype(F32) + mm(pooled_low, proj)
    shat, sr = ln_parts(start)
    normed_first = (shat * g_word1).astype(BF16)
    xall = gather(normed_first, ("ctx", "tp"), 0)
    (block_out, rms, gaa, dx, d_q, d_k, d_v, d_wout, d_g2w, d_wup, d_wdown) = word_section(
        xall, start, cotangent, wqkv[0], wqkv[1], wqkv[2], wout, g_word2, wup, wdown
    )
    gnf = scatter(dx.astype(BF16), ("ctx", "tp"), 0).astype(F32)
    words_grad = gaa + ln_back(shat, sr, g_word1, gnf)
    d_g1w = jnp.sum(gnf * shat, axis=0)
    gproj = words_grad.astype(BF16)
    d_proj = mm_tn(pooled_low, gproj)
    gpool = mm_nt(gproj, proj)
    cg, d_g1, d_qkv, d_out, d_g2, d_up, d_down_t, d_pq = char_backward(x, cnt, saved, gpool, weights)

    def reduce_char(g):
        g = lax.psum(g.astype(BF16), ("ctx", "tp"))
        return scatter(g, "fsdp", 0).astype(F32)

    def reduce_word(g, tp_axis, fsdp_axis):
        g = scatter(g.astype(BF16), "tp", tp_axis)
        g = lax.psum(g, "ctx")
        return scatter(g, "fsdp", fsdp_axis).astype(F32)

    d_wqkv = reduce_word(jnp.stack([d_q, d_k, d_v], axis=0), 2, 1)
    return (
        block_out,
        cg.reshape(words, slots, cdim),
        words_grad,
        rms[:3],
        reduce_char(d_g1[0]),
        reduce_char(d_qkv),
        reduce_char(d_out),
        reduce_char(d_g2[0]),
        reduce_char(d_up),
        reduce_char(d_down_t.T),
        reduce_char(d_pq[0]),
        reduce_char(d_proj),
        reduce_char(d_g1w),
        jnp.moveaxis(d_wqkv, 0, 1),
        reduce_word(d_wout, 0, 1),
        reduce_char(d_g2w[0]),
        reduce_word(d_wup, 1, 0),
        reduce_word(d_wdown, 0, 1),
    )


def solution(mesh):
    rows = ("fsdp", "ctx", "tp")
    v, m = P("fsdp"), P("fsdp", None)
    return jax.shard_map(
        local,
        mesh=mesh,
        in_specs=(
            P(rows, None, None), P(rows), P(rows, None), P(rows, None),
            v, m, m, v, m, m, v, m, v, P("fsdp", None, "tp"), P("tp", "fsdp"), v, P("fsdp", "tp"), P("tp", "fsdp"),
        ),
        out_specs=(
            P(rows, None), P(rows, None, None), P(rows, None), P(None, rows),
            v, m, m, v, m, m, v, m, v, P("fsdp", None, "tp"), P("tp", "fsdp"), v, P("fsdp", "tp"), P("tp", "fsdp"),
        ),
        check_vma=False,
    )
```

```python
import functools

import jax
import jax.numpy as jnp
from jax import lax
from jax.experimental import pallas as pl
from jax.experimental.pallas import tpu as pltpu
from jax.sharding import PartitionSpec as P

CHEADS = 4
HEADS = 8
HEAD = 64
EPSILON = 1e-05
MASKED = -1e30
CGELU = 0.7978845608028654
AGELU = 0.044715
ROWS = 512
GROUP = 128
F32 = jnp.float32
BF16 = jnp.bfloat16
VMEM_LIMIT = 66_000_000


def mm(a, b):
    return lax.dot_general(a, b, (((1,), (0,)), ((), ())), preferred_element_type=F32)


def mm_nt(a, b):
    return lax.dot_general(a, b, (((1,), (1,)), ((), ())), preferred_element_type=F32)


def mm_tn(a, b):
    return lax.dot_general(a, b, (((0,), (0,)), ((), ())), preferred_element_type=F32)


def ln_parts(x):
    c = x - jnp.mean(x, axis=-1, keepdims=True)
    r = lax.rsqrt(jnp.mean(c * c, axis=-1, keepdims=True) + EPSILON)
    return c * r, r


def ln_back(xhat, r, gain, g):
    gg = g * gain
    a = jnp.mean(gg, axis=-1, keepdims=True)
    b = jnp.mean(gg * xhat, axis=-1, keepdims=True)
    return r * (gg - a - xhat * b)


def gelu_both(x):
    x2 = x * x
    y = (CGELU * AGELU) * x2 + CGELU
    hp = 0.5 * jnp.tanh(x * y) + 0.5
    g = x * hp
    d = hp + (g - g * hp) * (6.0 * y - 4.0 * CGELU)
    return g, d


def pair_masks(rows):
    lane = lax.broadcasted_iota(jnp.int32, (rows, 128), 1)
    return lane < HEAD


def split_heads(x, low_lanes):
    zero = jnp.zeros_like(x)
    return jnp.where(low_lanes, x, zero), jnp.where(low_lanes, zero, x)


def stack_heads(x, low_lanes):
    a, b = split_heads(x, low_lanes)
    return jnp.concatenate([a, b], axis=0)


def word_of_lane(width):
    return (lax.broadcasted_iota(jnp.int32, (16, width), 1) % GROUP) // 16


def compress(blocks, lane_word):
    out = blocks[0:16, :]
    for w in range(1, GROUP // 16):
        out = jnp.where(lane_word == w, blocks[16 * w : 16 * w + 16, :], out)
    return out


def expand(dense, lane_word):
    zero = jnp.zeros_like(dense)
    return jnp.concatenate(
        [jnp.where(lane_word == w, dense, zero) for w in range(GROUP // 16)], axis=0
    )


def pool_weights(am, q_row, cnt_col):
    words = am.shape[0] // 16
    am3 = am.reshape(words, 16, am.shape[1])
    logits = jnp.sum(am * q_row, axis=-1, keepdims=True)
    slot = (lax.broadcasted_iota(jnp.int32, (am.shape[0], 1), 0) % 16).astype(F32)
    logits = jnp.where(slot < cnt_col, logits, MASKED).reshape(words, 16, 1)
    e = jnp.exp(logits - jnp.max(logits, axis=1, keepdims=True))
    w = e / jnp.sum(e, axis=1, keepdims=True)
    return am3, w


def count_column(cnt_row):
    return jnp.transpose(jnp.broadcast_to(cnt_row, (GROUP, GROUP)))[:, 0:1]


def char_fwd_tile(x, cnt, weights):
    g1, wqkv, wout, g2, wup, wdown, pq = weights
    rows = x.shape[0]
    groups = rows // GROUP
    xf = x.astype(F32)
    xhat, _ = ln_parts(xf)
    normed = (xhat * g1).astype(BF16)
    packed = mm(normed, wqkv).astype(BF16)
    low = pair_masks(GROUP)
    lw = word_of_lane(2 * GROUP)
    slot = lax.broadcasted_iota(jnp.int32, (16, 2 * GROUP), 0).astype(F32)
    probs, mixed, cols = [], [], []
    for g in range(groups):
        r = slice(g * GROUP, (g + 1) * GROUP)
        cnt_row = cnt[g : g + 1, :]
        cols.append(count_column(cnt_row))
        cnt2 = jnp.concatenate([cnt_row, cnt_row], axis=1)
        valid = slot < cnt2
        pg, mg = [], []
        for p in range(CHEADS // 2):
            q = packed[r, 128 * p : 128 * p + 128] * BF16(0.125)
            k = packed[r, 256 + 128 * p : 384 + 128 * p]
            v = packed[r, 512 + 128 * p : 640 + 128 * p]
            st = mm_nt(k, stack_heads(q, low))
            s = jnp.where(valid, compress(st, lw), MASKED)
            e = jnp.exp(s - jnp.max(s, axis=0, keepdims=True))
            pr = e / jnp.sum(e, axis=0, keepdims=True)
            pt = expand(pr.astype(BF16), lw)
            o = mm_tn(pt, v)
            pg.append(pr)
            mg.append(jnp.where(low, o[:GROUP], o[GROUP:]))
        probs.append(jnp.concatenate(pg, axis=1))
        mixed.append(jnp.concatenate(mg, axis=1))
    probs = jnp.concatenate(probs, axis=0)
    mixed = jnp.concatenate(mixed, axis=0).astype(BF16)
    aa = xf + mm(mixed, wout)
    ahat, _ = ln_parts(aa)
    middle = (ahat * g2).astype(BF16)
    upper, dgelu = gelu_both(mm(middle, wup))
    upper = upper.astype(BF16)
    am = aa + mm(upper, wdown)
    am3, w = pool_weights(am, pq, jnp.concatenate(cols, axis=0))
    pooled = jnp.sum(w * am3, axis=1)
    return packed, probs, mixed, aa, upper, dgelu.astype(BF16), am, pooled.astype(BF16)


def full_spec(shape):
    return pl.BlockSpec(shape, lambda i: (0,) * len(shape))


def rows_spec(rows, width):
    return pl.BlockSpec((rows, width), lambda i: (i, 0))


def char_bwd_tile(x, cnt, packed, probs, mixed, aa, upper, dgelu, am, gpool_ref, base, weights):
    g1, wqkv, wout, g2, wup, wdown, pq = weights
    rows = x.shape[0]
    groups = rows // GROUP
    words = rows // 16
    low = pair_masks(GROUP)
    lw = word_of_lane(2 * GROUP)
    cols = jnp.concatenate([count_column(cnt[g : g + 1, :]) for g in range(groups)], axis=0)
    am3, w = pool_weights(am, pq, cols)
    gp = jnp.concatenate(
        [jnp.broadcast_to(gpool_ref[pl.ds(base + i, 1), :], (16, 256)) for i in range(words)], axis=0
    )
    dw = jnp.sum(gp * am, axis=-1, keepdims=True).reshape(words, 16, 1)
    dlog = (w * (dw - jnp.sum(w * dw, axis=1, keepdims=True))).reshape(rows, 1)
    gm = w.reshape(rows, 1) * gp + dlog * pq
    d_pq = jnp.sum(dlog * am, axis=0, keepdims=True)
    gdl = gm.astype(BF16)
    d_down_t = mm_tn(gdl, upper)
    ghid = (dgelu.astype(F32) * mm_nt(gdl, wdown)).astype(BF16)
    ahat, ar = ln_parts(aa)
    middle = (ahat * g2).astype(BF16)
    d_up = mm_tn(middle, ghid)
    gmid = mm_nt(ghid, wup)
    gca = gm + ln_back(ahat, ar, g2, gmid)
    d_g2 = jnp.sum(gmid * ahat, axis=0, keepdims=True)
    gcl = gca.astype(BF16)
    d_out = mm_tn(mixed, gcl)
    gcm = mm_nt(gcl, wout).astype(BF16)
    dqkv = []
    for g in range(groups):
        r = slice(g * GROUP, (g + 1) * GROUP)
        dq_g, dk_g, dv_g = [], [], []
        for p in range(CHEADS // 2):
            q = packed[r, 128 * p : 128 * p + 128] * BF16(0.125)
            k = packed[r, 256 + 128 * p : 384 + 128 * p]
            v = packed[r, 512 + 128 * p : 640 + 128 * p]
            do = stack_heads(gcm[r, 128 * p : 128 * p + 128], low)
            pr = probs[16 * g : 16 * g + 16, 256 * p : 256 * p + 256]
            dp = compress(mm_nt(v, do), lw)
            ds = (pr * (dp - jnp.sum(pr * dp, axis=0, keepdims=True))).astype(BF16)
            dst = expand(ds, lw)
            pt = expand(pr.astype(BF16), lw)
            dv_g.append(mm(pt, do))
            dk_g.append(mm(dst, stack_heads(q, low)))
            o = mm_tn(dst, k)
            dq_g.append(jnp.where(low, o[:GROUP], o[GROUP:]) * 0.125)
        dqkv.append(jnp.concatenate(dq_g + dk_g + dv_g, axis=1))
    dqkv = jnp.concatenate(dqkv, axis=0).astype(BF16)
    xf = x.astype(F32)
    xhat, xr = ln_parts(xf)
    normed = (xhat * g1).astype(BF16)
    d_qkv = mm_tn(normed, dqkv)
    gn = mm_nt(dqkv, wqkv)
    d_g1 = jnp.sum(gn * xhat, axis=0, keepdims=True)
    cg = gca + ln_back(xhat, xr, g1, gn)
    return cg, (d_g1, d_qkv, d_out, d_g2, d_up, d_down_t, d_pq)


def char_bwd_kernel(x, cnt, packed, probs, mixed, aa, upper, dgelu, am, gpool, vec, qo, up, dn, cg, *accs):
    weights = char_weights(vec, qo, up, dn)
    step = pl.program_id(0)

    @pl.when(step == 0)
    def _():
        for acc in accs:
            acc[...] = jnp.zeros_like(acc)

    out, sums = char_bwd_tile(
        x[...], cnt[0], packed[...], probs[...], mixed[...], aa[...], upper[...], dgelu[...], am[...],
        gpool, step * (ROWS // 16), weights,
    )
    cg[...] = out
    for acc, val in zip(accs, sums):
        acc[...] += val


def char_backward(x, cnt, saved, gpool, weights):
    total = x.shape[0]
    tiles = total // ROWS
    widths = [(ROWS, 768), (ROWS // 8, 512), (ROWS, 256), (ROWS, 256), (ROWS, 1024), (ROWS, 1024), (ROWS, 256)]
    acc_shapes = [(1, 256), (256, 768), (256, 256), (1, 256), (256, 1024), (256, 1024), (1, 256)]
    return pl.pallas_call(
        char_bwd_kernel,
        grid=(tiles,),
        in_specs=[rows_spec(ROWS, 256), pl.BlockSpec((1, ROWS // GROUP, GROUP), lambda i: (i, 0, 0))]
        + [rows_spec(r, w) for r, w in widths]
        + [full_spec(gpool.shape)]
        + [full_spec(w.shape) for w in weights],
        out_specs=[rows_spec(ROWS, 256)] + [full_spec(s) for s in acc_shapes],
        out_shape=[jax.ShapeDtypeStruct((total, 256), F32)] + [jax.ShapeDtypeStruct(s, F32) for s in acc_shapes],
        compiler_params=pltpu.CompilerParams(vmem_limit_bytes=VMEM_LIMIT, dimension_semantics=("arbitrary",)),
        name="char_backward",
    )(x, cnt, *saved, gpool, *weights)


MESH = pl.DeviceIdType.MESH


def remote(src, dst, sems, index, where):
    return pltpu.make_async_remote_copy(
        src_ref=src, dst_ref=dst,
        send_sem=sems[0] if index is None else sems[0].at[index],
        recv_sem=sems[1] if index is None else sems[1].at[index],
        device_id=where, device_id_type=MESH,
    )


def span(start, size):
    return pl.ds(pl.multiple_of(start, size), size)


class Place:
    def __init__(self):
        self.f, self.c, self.t = lax.axis_index("fsdp"), lax.axis_index("ctx"), lax.axis_index("tp")
        self.F, self.T = lax.axis_size("fsdp"), lax.axis_size("tp")

    def fs(self, k):
        return lax.rem(self.f + k + self.F, self.F)

    def tp(self, k):
        return lax.rem(self.t + k + self.T, self.T)

    def peers(self):
        out = [{"fsdp": self.fs(k)} for k in range(1, self.F)]
        out += [{"tp": self.tp(k)} for k in range(1, self.T)]
        return out + [{"ctx": 1 - self.c}]


def greet(peers):
    barrier = pltpu.get_barrier_semaphore()
    for where in peers:
        pl.semaphore_signal(barrier, inc=1, device_id=where, device_id_type=MESH)
    pl.semaphore_wait(barrier, len(peers))


class Piece:
    def __init__(self, at, shard, whole, mine, landing, region, cores, planar, sems, local_sem, first):
        self.at, self.shard, self.whole = at, shard, whole
        self.mine, self.landing, self.region = mine, landing, region
        self.cores, self.planar = cores, planar
        self.sems, self.local_sem, self.first = sems, local_sem, first

    @staticmethod
    def slots(F, T):
        return (F - 1) + (T - 1) + T

    def local(self):
        at = self.at
        return pltpu.make_async_copy(self.shard.at[self.mine(at.c, at.t)], self.whole.at[self.landing(at.f, at.c, at.t)], self.local_sem)

    def z(self, k, incoming=False):
        at = self.at
        f = at.fs(-k) if incoming else at.f
        dst = self.whole.at[self.landing(f, at.c, at.t)]
        src = dst if incoming else self.shard.at[self.mine(at.c, at.t)]
        return remote(src, dst, self.sems, self.first + k - 1, {"fsdp": at.fs(k)})

    def plane(self, k, incoming=False):
        at = self.at
        r = self.whole.at[self.region(at.c, at.tp(-k) if incoming else at.t)]
        return remote(r, r, self.sems, self.first + at.F - 1 + k - 1, {"tp": at.tp(k)})

    def side(self, k, incoming=False):
        at = self.at
        r = self.whole.at[self.region(1 - at.c if incoming else at.c, at.tp(-k))]
        return remote(r, r, self.sems, self.first + at.F + at.T - 2 + k, {"ctx": 1 - at.c})

    def begin(self):
        self.local().start()
        for k in range(1, self.at.F):
            self.z(k).start()

    def spread(self):
        self.local().wait()
        for k in range(1, self.at.F):
            self.z(k, True).wait_recv()
        if self.planar:
            for k in range(1, self.at.T):
                self.plane(k).start()
            if self.cores:
                self.side(0).start()

    def pass_on(self):
        if self.planar:
            for k in range(1, self.at.T):
                self.plane(k, True).wait_recv()
                if self.cores:
                    self.side(k).start()

    def arrive(self):
        if self.planar and self.cores:
            for k in range(self.at.T):
                self.side(k, True).wait_recv()

    def drain(self):
        for k in range(1, self.at.F):
            self.z(k).wait_send()
        if self.planar:
            for k in range(1, self.at.T):
                self.plane(k).wait_send()
            if self.cores:
                for k in range(self.at.T):
                    self.side(k).wait_send()


ALL = slice(None)


def gather_pieces(at, shards, wholes, sems, local_sems):
    F, T = at.F, at.T
    qo, up, dn, pj, sm, w4, wu, wd = shards
    rq, rd, rw = qo.shape[0], dn.shape[0], w4.shape[1]
    cu = wu.shape[1]
    lanes = lambda c, t: span(256 * t + 128 * c, 128)
    table = [
        (lambda c, t: (ALL, lanes(c, t)), lambda f, c, t: (span(f * rq, rq), lanes(c, t)), lambda c, t: (ALL, lanes(c, t)), True, True),
        (lambda c, t: (ALL, lanes(c, t)), lambda f, c, t: (span(f * rq, rq), lanes(c, t)), lambda c, t: (ALL, lanes(c, t)), True, True),
        (lambda c, t: (span(rd // T * t, rd // T), span(128 * c, 128)), lambda f, c, t: (f, span(rd // T * t, rd // T), span(128 * c, 128)), lambda c, t: (ALL, span(rd // T * t, rd // T), span(128 * c, 128)), True, True),
        (lambda c, t: (ALL, span(128 * t, 128)), lambda f, c, t: (span(f * rq, rq), span(128 * t, 128)), lambda c, t: (ALL, span(128 * t, 128)), False, True),
        (lambda c, t: (ALL, ALL), lambda f, c, t: (f,), lambda c, t: (ALL,), False, False),
        (lambda c, t: (span(2 * c, 2),), lambda f, c, t: (span(2 * c, 2), span(f * rw, rw), span(128 * t, 128)), lambda c, t: (span(2 * c, 2), ALL, span(128 * t, 128)), True, True),
        (lambda c, t: (ALL, span(cu // 2 * c, cu // 2)), lambda f, c, t: (span(f * rw, rw), span(cu * t + cu // 2 * c, cu // 2)), lambda c, t: (ALL, span(cu * t + cu // 2 * c, cu // 2)), True, True),
        (lambda c, t: (span(cu // 2 * c, cu // 2), ALL), lambda f, c, t: (span(cu * t + cu // 2 * c, cu // 2), span(f * rw, rw)), lambda c, t: (span(cu * t + cu // 2 * c, cu // 2), ALL), True, True),
    ]
    slots = Piece.slots(F, T)
    return [
        Piece(at, shard, whole, mine, landing, region, cores, planar, sems, local_sems.at[i], i * slots)
        for i, (shard, whole, (mine, landing, region, cores, planar)) in enumerate(zip(shards, wholes, table))
    ]


FWD_OUTS = [(ROWS, 768, BF16), (ROWS // 8, 512, F32), (ROWS, 256, BF16), (ROWS, 256, F32), (ROWS, 1024, BF16), (ROWS, 1024, BF16), (ROWS, 256, F32), (ROWS // 16, 256, BF16)]


def char_weights(vec, qo, up, dn):
    return (vec[0:1, :256], qo[:, :768], qo[:, 768:], vec[1:2, :256], up[...], dn[...], vec[2:3, :256])


def char_fwd_kernel(x, cnt, vec, qo, up, dn, *outs):
    for ref, val in zip(outs, char_fwd_tile(x[...], cnt[0], char_weights(vec, qo, up, dn))):
        ref[...] = val


def char_forward(x, cnt, *weights):
    tiles = x.shape[0] // ROWS
    return pl.pallas_call(
        char_fwd_kernel,
        grid=(tiles,),
        in_specs=[rows_spec(ROWS, 256), pl.BlockSpec((1, ROWS // GROUP, GROUP), lambda i: (i, 0, 0))] + [full_spec(w.shape) for w in weights],
        out_specs=[rows_spec(r, w) for r, w, _ in FWD_OUTS],
        out_shape=[jax.ShapeDtypeStruct((r * tiles, w), d) for r, w, d in FWD_OUTS],
        compiler_params=pltpu.CompilerParams(vmem_limit_bytes=VMEM_LIMIT, dimension_semantics=("arbitrary",)),
        name="char_forward",
    )(x, cnt, *weights)


GATHERED = [((256, 1024), BF16), ((256, 1024), BF16), ((4, 256, 256), BF16), ((256, 512), BF16), ((4, 8, 128), F32), ((4, 512, 512), BF16), ((512, 2048), BF16), ((2048, 512), BF16)]


def vectors(sm):
    rows = []
    for i, n in ((0, 64), (1, 64), (2, 64), (3, 128), (4, 128)):
        v = jnp.concatenate([sm[f, i : i + 1, :n] for f in range(sm.shape[0])], axis=1)
        rows.append(v if n == 128 else jnp.concatenate([v, jnp.zeros_like(v)], axis=1))
    return jnp.concatenate(rows + [jnp.zeros((3, 512), F32)], axis=0)


def gather_fwd_kernel(*refs):
    n = len(GATHERED)
    x, cnt = refs[:2]
    shards = refs[2 : 2 + n]
    outs = refs[2 + n : 2 + n + len(FWD_OUTS)]
    full_out = refs[2 + n + len(FWD_OUTS) : 2 + 2 * n + len(FWD_OUTS)]
    vec_out = refs[2 + 2 * n + len(FWD_OUTS)]
    wholes = refs[3 + 2 * n + len(FWD_OUTS) : 3 + 3 * n + len(FWD_OUTS)]
    vec, send, recv, local_sems = refs[3 + 3 * n + len(FWD_OUTS) :]
    at = Place()
    pieces = gather_pieces(at, shards, wholes, (send, recv), local_sems)
    qo, up, dn, pj, sm, w4, wu, wd = pieces
    step = pl.program_id(0)
    last = pl.num_programs(0) - 1

    @pl.when(step == 0)
    def _():
        greet(at.peers())
        for p in pieces:
            p.begin()
        first = (qo, up, dn, sm)
        for p in first:
            p.spread()
        for p in first:
            p.pass_on()
        for p in first:
            p.arrive()
        vec[...] = vectors(wholes[4])
        vec_out[...] = vec[...]

    @pl.when(step == 1)
    def _():
        for p in (pj, w4, wu, wd):
            p.spread()

    @pl.when(step == 4)
    def _():
        pj.pass_on()
        w4.pass_on()

    dn2 = wholes[2][...].reshape(1024, 256)
    for ref, val in zip(outs, char_fwd_tile(x[...], cnt[0], char_weights(vec, wholes[0], wholes[1], dn2))):
        ref[...] = val

    @pl.when(step == last)
    def _():
        def out(i):
            return pltpu.make_async_copy(wholes[i], full_out[i], local_sems.at[i])

        for i in (0, 1, 2, 3):
            out(i).start()
        for p in (wu, wd):
            p.pass_on()
        for i, p in ((5, w4), (6, wu), (7, wd)):
            p.arrive()
            out(i).start()
        for p in pieces:
            p.drain()
        for i in (0, 1, 2, 3, 5, 6, 7):
            out(i).wait()


def gather_forward(x, cnt, shards):
    tiles = x.shape[0] // ROWS
    any_ = pl.BlockSpec(memory_space=pl.ANY)
    count = len(GATHERED) * Piece.slots(lax.axis_size("fsdp"), lax.axis_size("tp"))
    return pl.pallas_call(
        gather_fwd_kernel,
        grid=(tiles,),
        in_specs=[rows_spec(ROWS, 256), pl.BlockSpec((1, ROWS // GROUP, GROUP), lambda i: (i, 0, 0))] + [any_] * len(shards),
        out_specs=[rows_spec(r, w) for r, w, _ in FWD_OUTS] + [any_] * len(GATHERED) + [full_spec((8, 512))],
        out_shape=[jax.ShapeDtypeStruct((r * tiles, w), d) for r, w, d in FWD_OUTS] + [jax.ShapeDtypeStruct(sh, d) for sh, d in GATHERED] + [jax.ShapeDtypeStruct((8, 512), F32)],
        scratch_shapes=[pltpu.VMEM(sh, d) for sh, d in GATHERED]
        + [pltpu.VMEM((8, 512), F32), pltpu.SemaphoreType.DMA((count,)), pltpu.SemaphoreType.DMA((count,)), pltpu.SemaphoreType.DMA((len(GATHERED),))],
        compiler_params=pltpu.CompilerParams(vmem_limit_bytes=VMEM_LIMIT, collective_id=0, has_side_effects=True, dimension_semantics=("arbitrary",)),
        name="gather_forward",
    )(x, cnt, *shards)


def word_kernel(
    pooled, proj, words_in, cot, vec, w4, wup, wdown,
    block_out, rms, words_grad, gpool, d_proj, d_vec, d_w4, d_up, d_down,
    xall, kk, vv, kt, vt, ss, ee, qm, dom, mx, ll, ot, dqt, wkt, wvt, wout, dk_acc, dv_acc, dlt, dk_sum, dv_sum,
    dx, dx_in, dx_own, ag_send, ag_recv, rs_send, rs_recv,
):
    at = Place()
    T = at.T
    own = at.c * T + at.t
    nblk, blk, width = xall.shape
    half = HEADS // 2
    low = pair_masks(blk)
    first, second = range(half), range(half, HEADS)

    start = words_in[...].astype(F32) + mm(pooled[...], proj[...])
    shat, sr = ln_parts(start)
    g1v = vec[3:4, :]
    xall[own] = (shat * g1v).astype(BF16)
    greet([{"ctx": i, "tp": at.tp(k)} for i in (at.c, 1 - at.c) for k in range(T) if k > 0] + [{"ctx": 1 - at.c}])

    def row_copy(k, incoming=False):
        r = xall.at[at.c * T + (at.tp(-k) if incoming else at.t)]
        return remote(r, r, (ag_send, ag_recv), k - 1, {"tp": at.tp(k)})

    def side_copy(k):
        r = xall.at[at.tp(-k)]
        return remote(r, r, (ag_send, ag_recv), T - 1 + k, {"ctx": 1 - at.c})

    for k in range(1, T):

        @pl.when((at.c == 0) | (at.t + k < T))
        def _():
            row_copy(k).start()

    @pl.when(at.c == 0)
    def _():
        side_copy(0).start()

    wq, wk, wv, wot = w4.at[0], w4.at[1], w4.at[2], w4.at[3]
    wkt[...] = jnp.transpose(wk[...])
    wvt[...] = jnp.transpose(wv[...])
    wout[...] = jnp.transpose(wot[...])
    xown = xall[own]
    q = mm(xown, wq[...]).astype(BF16) * BF16(0.125)
    for p in range(HEADS // 2):
        a, b = split_heads(q[:, 128 * p : 128 * p + 128], low)
        qm[2 * p] = a
        qm[2 * p + 1] = b
    mx[...] = jnp.full(mx.shape, MASKED, F32)
    ll[...] = jnp.zeros(ll.shape, F32)
    ot[...] = jnp.zeros(ot.shape, F32)
    dqt[...] = jnp.zeros(dqt.shape, F32)
    dk_sum[...] = jnp.zeros(dk_sum.shape, F32)
    dv_sum[...] = jnp.zeros(dv_sum.shape, F32)

    def scores_of(j, heads):
        for h in heads:
            p = h // 2
            s = mm_nt(kk[j, :, 128 * p : 128 * p + 128], qm[h])
            ss[j, h % half] = s
            mx[h] = jnp.maximum(mx[h], jnp.max(s.reshape(blk // 8, 8, blk), axis=0))

    def mix_of(j, heads):
        for h in heads:
            e = jnp.exp(ss[j, h % half] - mx[h, 0:1, :])
            ll[h] += jnp.sum(e.reshape(blk // 8, 8, blk), axis=0)
            eb = e.astype(BF16)
            ee[j, h] = eb
            ot[64 * h : 64 * h + 64, :] += mm(vt[j, 64 * h : 64 * h + 64, :], eb)

    def top_of(heads):
        for h in heads:
            mx[h] = jnp.broadcast_to(jnp.max(mx[h], axis=0, keepdims=True), (8, blk))

    @pl.when(at.c == 0)
    def _():
        for k in range(1, T):
            row_copy(k, True).wait_recv()
            side_copy(k).start()

    @pl.loop(0, 2 * T)
    def _(m):
        k0 = m - 1
        k1 = m - T
        early = (m >= 1) & (m <= T)
        late = (m > T) & (at.c == 1) & (at.t >= k1)

        @pl.when(early & (at.c == 1))
        def _():
            r = xall.at[lax.rem(at.t - k0 + T, T)]
            remote(r, r, (ag_send, ag_recv), T - 1 + k0, {"ctx": 1 - at.c}).wait_recv()

        @pl.when(late)
        def _():
            r = xall.at[own - k1]
            remote(r, r, (ag_send, ag_recv), k1 - 1, {"tp": at.t - k1}).wait_recv()

        @pl.when((m == 0) | (early & ((at.c == 1) | ((m >= 2) & (at.t >= k0)))) | late)
        def _():
            is_early = early.astype(jnp.int32)
            is_late = (m > T).astype(jnp.int32)
            j = own + is_early * (lax.rem(at.t - k0 + T, T) - own) - is_late * k1
            xj = xall[j]
            kk[j] = mm(xj, wk[...]).astype(BF16)
            vv[j] = mm(xj, wv[...]).astype(BF16)
            kt[j] = mm_nt(wkt[...], xj).astype(BF16)
            vt[j] = mm_nt(wvt[...], xj).astype(BF16)
            scores_of(j, first)

    top_of(first)

    @pl.loop(0, own + 1)
    def _(j):
        mix_of(j, first)
        scores_of(j, second)

    top_of(second)

    @pl.loop(0, own + 1)
    def _(j):
        mix_of(j, second)

    for h in range(HEADS):
        linv = 1.0 / jnp.sum(ll[h], axis=0, keepdims=True)
        ll[h] = jnp.broadcast_to(linv, (8, blk))
        ot[64 * h : 64 * h + 64, :] = ot[64 * h : 64 * h + 64, :] * linv
    mixed_t = ot[...].astype(BF16)
    mixed = jnp.transpose(mixed_t)
    attn = mm(mixed, wout[...])
    awa = start + attn
    ahat, ar = ln_parts(awa)
    g2v = vec[4:5, :]
    n2 = (ahat * g2v).astype(BF16)
    upper, dgelu = gelu_both(mm(n2, wup[...]))
    upper = upper.astype(BF16)
    mlp = mm(upper, wdown[...])
    final = awa + mlp
    block_out[...] = final.astype(BF16)
    lane = lax.broadcasted_iota(jnp.int32, (blk, 128), 1)
    cols = [jnp.sqrt(jnp.mean(v * v, axis=-1, keepdims=True)) for v in (attn, mlp, final)]
    rms[...] = jnp.transpose(jnp.where(lane == 0, cols[0], jnp.where(lane == 1, cols[1], cols[2])))[0:3, :]
    cotv = cot[...]
    ff = wup.shape[1]
    cu = ff // T // 2
    gdown = mm_tn(upper, cotv).astype(BF16)
    ghid = (dgelu * mm_nt(cotv, wdown[...])).astype(BF16)
    gup = mm_tn(n2, ghid).astype(BF16)
    for c in range(2):
        for t in range(T):
            d_down[c, cu * t : cu * t + cu, :] = gdown[cu * (2 * t + c) : cu * (2 * t + c) + cu, :]
            d_up[c, :, cu * t : cu * t + cu] = gup[:, cu * (2 * t + c) : cu * (2 * t + c) + cu]
    gn2 = mm_nt(ghid, wup[...])
    d_g2 = jnp.sum(gn2 * ahat, axis=0, keepdims=True)
    ga = cotv.astype(F32) + ln_back(ahat, ar, g2v, gn2)
    gal = ga.astype(BF16)
    d_w4[3] = mm_tn(gal, mixed).astype(BF16)
    do_t = mm_nt(wout[...], gal).astype(BF16)
    do_s = []
    for h in range(HEADS):
        r = slice(64 * h, 64 * h + 64)
        d = do_t[r, :].astype(F32)
        linv = ll[h, 0:1, :]
        dlt[h] = jnp.broadcast_to(jnp.sum(d * ot[r, :], axis=0, keepdims=True) * linv, (8, blk))
        do_s.append((d * linv).astype(BF16))
    do = jnp.transpose(jnp.concatenate(do_s, axis=0))
    for p in range(HEADS // 2):
        a, b = split_heads(do[:, 128 * p : 128 * p + 128], low)
        dom[2 * p] = a
        dom[2 * p + 1] = b

    def grad_copy(j):
        return remote(dx.at[j], dx_in.at[own], (rs_send.at[j], rs_recv.at[own]), None, {"ctx": j // T, "tp": lax.rem(j, T)})

    @pl.loop(0, own + 1)
    def _(j):
        @pl.when(j > 0)
        def _():
            grad_copy(j - 1).start()

        for p in range(HEADS // 2):
            c = slice(128 * p, 128 * p + 128)
            vp = vv[j, :, c]
            dk = None
            for h in (2 * p, 2 * p + 1):
                e = ee[j, h]
                dp = mm_nt(vp, dom[h])
                ds = (e.astype(F32) * (dp - dlt[h, 0:1, :])).astype(BF16)
                dvh = mm(e, dom[h])
                dkh = mm(ds, qm[h])
                dk, dv = (dkh, dvh) if dk is None else (dk + dkh, dv + dvh)
                dqt[64 * h : 64 * h + 64, :] += mm(kt[j, 64 * h : 64 * h + 64, :], ds)
            dk_acc[:, c] = dk.astype(BF16)
            dv_acc[:, c] = dv.astype(BF16)
        dk = dk_acc[...]
        dv = dv_acc[...]
        dxj = mm_nt(dk, wk[...]) + mm_nt(dv, wv[...])
        dx[j] = dxj.astype(BF16)
        dx_own[...] = dxj
        xt = jnp.transpose(xall[j])
        dk_sum[...] += mm(xt, dk)
        dv_sum[...] += mm(xt, dv)

    dq = jnp.transpose((dqt[...] * 0.125).astype(BF16))
    d_w4[0] = mm_tn(xown, dq).astype(BF16)
    d_w4[1] = dk_sum[...].astype(BF16)
    d_w4[2] = dv_sum[...].astype(BF16)
    dx_own[...] += mm_nt(dq, wq[...])

    @pl.loop(own + 1, nblk)
    def _(b):
        remote(dx.at[own], dx_in.at[b], (rs_send.at[b], rs_recv.at[b]), None, {"ctx": 1 - at.c}).wait_recv()
        dx_own[...] += dx_in[b].astype(F32)

    gnf = dx_own[...]
    grad = ga + ln_back(shat, sr, g1v, gnf)
    words_grad[...] = grad
    d_vec[...] = jnp.concatenate([jnp.sum(gnf * shat, axis=0, keepdims=True), d_g2, jnp.zeros((6, width), F32)], axis=0)
    gproj = grad.astype(BF16)
    d_proj[...] = mm_tn(pooled[...], gproj).astype(BF16)
    gpool[...] = mm_nt(gproj, proj[...])

    for k in range(1, T):

        @pl.when((at.c == 0) | (at.t + k < T))
        def _():
            row_copy(k).wait_send()

    @pl.when(at.c == 0)
    def _():
        for k in range(T):
            side_copy(k).wait_send()

    @pl.loop(0, own)
    def _(j):
        grad_copy(j).wait_send()


def word_section(pooled, proj, words_in, cot, vec, w4, wup, wdown):
    blk, width = words_in.shape
    T = lax.axis_size("tp")
    nblk = 2 * T
    ff = wup.shape[1]
    out_shapes = [((blk, width), BF16), ((3, blk), F32), ((blk, width), F32), ((blk, pooled.shape[1]), F32), (proj.shape, BF16), ((8, width), F32)]
    out_shapes += [(w4.shape, BF16), ((2, width, ff // 2), BF16), ((2, ff // 2, width), BF16)]
    vm = pl.BlockSpec(memory_space=pltpu.VMEM)
    return pl.pallas_call(
        word_kernel,
        in_specs=[vm] * 8,
        out_specs=[vm] * len(out_shapes),
        out_shape=[jax.ShapeDtypeStruct(s, d) for s, d in out_shapes],
        scratch_shapes=[
            pltpu.VMEM((nblk, blk, width), BF16),
            pltpu.VMEM((nblk, blk, width), BF16),
            pltpu.VMEM((nblk, blk, width), BF16),
            pltpu.VMEM((nblk, width, blk), BF16),
            pltpu.VMEM((nblk, width, blk), BF16),
            pltpu.VMEM((nblk, HEADS // 2, blk, blk), F32),
            pltpu.VMEM((nblk, HEADS, blk, blk), BF16),
            pltpu.VMEM((HEADS, blk, 128), BF16),
            pltpu.VMEM((HEADS, blk, 128), BF16),
            pltpu.VMEM((HEADS, 8, blk), F32),
            pltpu.VMEM((HEADS, 8, blk), F32),
            pltpu.VMEM((width, blk), F32),
            pltpu.VMEM((width, blk), F32),
            pltpu.VMEM((width, width), BF16),
            pltpu.VMEM((width, width), BF16),
            pltpu.VMEM((width, width), BF16),
            pltpu.VMEM((blk, width), BF16),
            pltpu.VMEM((blk, width), BF16),
            pltpu.VMEM((HEADS, 8, blk), F32),
            pltpu.VMEM((width, width), F32),
            pltpu.VMEM((width, width), F32),
            pltpu.VMEM((nblk, blk, width), BF16),
            pltpu.VMEM((nblk, blk, width), BF16),
            pltpu.VMEM((blk, width), F32),
            pltpu.SemaphoreType.DMA((2 * T,)),
            pltpu.SemaphoreType.DMA((2 * T,)),
            pltpu.SemaphoreType.DMA((nblk,)),
            pltpu.SemaphoreType.DMA((nblk,)),
        ],
        compiler_params=pltpu.CompilerParams(vmem_limit_bytes=VMEM_LIMIT, collective_id=1, has_side_effects=True),
        name="word_section",
    )(pooled, proj, words_in, cot, vec, w4, wup, wdown)


def gather(x, name, axis):
    return lax.all_gather(x, name, axis=axis, tiled=True)


def scatter(x, name, axis):
    return lax.psum_scatter(x, name, scatter_dimension=axis, tiled=True)


def fits(rows):
    return lax.axis_size("fsdp") == 4 and lax.axis_size("tp") == 4 and rows == 64


def local(characters, counts, words_in, cotangent, char_prenorm, char_qkv, char_out, char_midnorm, char_up, char_down,
          pool_query, char_proj, word_prenorm, word_qkv, word_out, word_midnorm, word_up, word_down):
    words, slots, cdim = characters.shape
    x = characters.reshape(words * slots, cdim)
    cnt = jnp.repeat(counts.astype(F32), slots).reshape(words * slots // ROWS, ROWS // GROUP, GROUP)
    vectors_in = (char_prenorm, char_midnorm, pool_query, word_prenorm, word_midnorm)
    qo = jnp.concatenate([char_qkv, char_out], axis=1)
    w4 = jnp.concatenate([jnp.moveaxis(word_qkv, 1, 0), word_out.T[None]], axis=0)
    direct = fits(char_prenorm.shape[0])
    if direct:
        pad = lambda v: jnp.pad(v.astype(F32), (0, 128 - v.shape[0]))
        small = jnp.stack([pad(v) for v in vectors_in] + [jnp.zeros((128,), F32)] * 3)
        *saved, pooled_low, qo, up, dn, proj, _, w4, wup, wdown, vec = gather_forward(x, cnt, [qo, char_up, char_down, char_proj, small, w4, word_up, word_down])
        dn = dn.reshape(1024, 256)
    else:
        wide = [gather(v.astype(F32), "fsdp", 0) for v in vectors_in]
        vec = jnp.stack([jnp.pad(v, (0, 512 - v.shape[0])) for v in wide] + [jnp.zeros((512,), F32)] * 3)
        qo, up, dn, proj = (gather(w, "fsdp", 0) for w in (qo, char_up, char_down, char_proj))
        w4 = gather(gather(w4, "fsdp", 1), "tp", 2)
        wup = gather(gather(word_up, "fsdp", 0), "tp", 1)
        wdown = gather(gather(word_down, "fsdp", 1), "tp", 0)
        *saved, pooled_low = char_forward(x, cnt, vec, qo, up, dn)
    (block_out, rms, words_grad, gpool, d_proj, d_vec, d_w4, d_wup, d_wdown) = word_section(pooled_low, proj, words_in, cotangent, vec, w4, wup, wdown)
    cg, d_g1, d_qkv, d_out, d_g2, d_up, d_down_t, d_pq = char_backward(x, cnt, saved, gpool, [vec, qo, up, dn])
    ff = word_up.shape[1] // 2
    d_q, d_k, d_v, d_wout = d_w4[0], d_w4[1], d_w4[2], d_w4[3].T
    d_wup = jnp.moveaxis(d_wup.reshape(2, 512, 4, ff), 0, 2).reshape(512, 2048)
    d_wdown = jnp.moveaxis(d_wdown.reshape(2, 4, ff, 512), 0, 1).reshape(2048, 512)
    d_g1w, d_g2w = d_vec[0], d_vec[1:2]

    def reduce_char(g):
        g = lax.psum(g.astype(BF16), ("ctx", "tp"))
        return scatter(g, "fsdp", 0).astype(F32)

    def reduce_word(g, tp_axis, fsdp_axis):
        g = scatter(g.astype(BF16), "tp", tp_axis)
        g = lax.psum(g, "ctx")
        return scatter(g, "fsdp", fsdp_axis).astype(F32)

    d_wqkv = reduce_word(jnp.stack([d_q, d_k, d_v], axis=0), 2, 1)
    return (
        block_out,
        cg.reshape(words, slots, cdim),
        words_grad,
        rms,
        reduce_char(d_g1[0]),
        reduce_char(d_qkv),
        reduce_char(d_out),
        reduce_char(d_g2[0]),
        reduce_char(d_up),
        reduce_char(d_down_t.T),
        reduce_char(d_pq[0]),
        reduce_char(d_proj),
        reduce_char(d_g1w),
        jnp.moveaxis(d_wqkv, 0, 1),
        reduce_word(d_wout, 0, 1),
        reduce_char(d_g2w[0]),
        reduce_word(d_wup, 1, 0),
        reduce_word(d_wdown, 0, 1),
    )


def solution(mesh):
    rows = ("fsdp", "ctx", "tp")
    v, m = P("fsdp"), P("fsdp", None)
    return jax.shard_map(
        local,
        mesh=mesh,
        in_specs=(
            P(rows, None, None), P(rows), P(rows, None), P(rows, None),
            v, m, m, v, m, m, v, m, v, P("fsdp", None, "tp"), P("tp", "fsdp"), v, P("fsdp", "tp"), P("tp", "fsdp"),
        ),
        out_specs=(
            P(rows, None), P(rows, None, None), P(rows, None), P(None, rows),
            v, m, m, v, m, m, v, m, v, P("fsdp", None, "tp"), P("tp", "fsdp"), v, P("fsdp", "tp"), P("tp", "fsdp"),
        ),
        check_vma=False,
    )
```

```python
import functools

import jax
import jax.numpy as jnp
from jax import lax
from jax.experimental import pallas as pl
from jax.experimental.pallas import tpu as pltpu
from jax.sharding import PartitionSpec as P

CHEADS = 4
HEADS = 8
HEAD = 64
EPSILON = 1e-05
MASKED = -1e30
CGELU = 0.7978845608028654
AGELU = 0.044715
ROWS = 512
GROUP = 128
F32 = jnp.float32
BF16 = jnp.bfloat16
VMEM_LIMIT = 66_000_000


def mm(a, b):
    return lax.dot_general(a, b, (((1,), (0,)), ((), ())), preferred_element_type=F32)


def mm_nt(a, b):
    return lax.dot_general(a, b, (((1,), (1,)), ((), ())), preferred_element_type=F32)


def mm_tn(a, b):
    return lax.dot_general(a, b, (((0,), (0,)), ((), ())), preferred_element_type=F32)


def ln_parts(x):
    c = x - jnp.mean(x, axis=-1, keepdims=True)
    r = lax.rsqrt(jnp.mean(c * c, axis=-1, keepdims=True) + EPSILON)
    return c * r, r


def ln_back(xhat, r, gain, g):
    gg = g * gain
    a = jnp.mean(gg, axis=-1, keepdims=True)
    b = jnp.mean(gg * xhat, axis=-1, keepdims=True)
    return r * (gg - a - xhat * b)


def gelu_both(x):
    x2 = x * x
    y = (CGELU * AGELU) * x2 + CGELU
    hp = 0.5 * jnp.tanh(x * y) + 0.5
    g = x * hp
    d = hp + (g - g * hp) * (6.0 * y - 4.0 * CGELU)
    return g, d


def pair_masks(rows):
    lane = lax.broadcasted_iota(jnp.int32, (rows, 128), 1)
    return lane < HEAD


def split_heads(x, low_lanes):
    zero = jnp.zeros_like(x)
    return jnp.where(low_lanes, x, zero), jnp.where(low_lanes, zero, x)


def stack_heads(x, low_lanes):
    a, b = split_heads(x, low_lanes)
    return jnp.concatenate([a, b], axis=0)


def word_of_lane(width):
    return (lax.broadcasted_iota(jnp.int32, (16, width), 1) % GROUP) // 16


def compress(blocks, lane_word):
    out = blocks[0:16, :]
    for w in range(1, GROUP // 16):
        out = jnp.where(lane_word == w, blocks[16 * w : 16 * w + 16, :], out)
    return out


def expand(dense, lane_word):
    zero = jnp.zeros_like(dense)
    return jnp.concatenate(
        [jnp.where(lane_word == w, dense, zero) for w in range(GROUP // 16)], axis=0
    )


def pool_weights(am, q_row, cnt_col):
    words = am.shape[0] // 16
    am3 = am.reshape(words, 16, am.shape[1])
    logits = jnp.sum(am * q_row, axis=-1, keepdims=True)
    slot = (lax.broadcasted_iota(jnp.int32, (am.shape[0], 1), 0) % 16).astype(F32)
    logits = jnp.where(slot < cnt_col, logits, MASKED).reshape(words, 16, 1)
    e = jnp.exp(logits - jnp.max(logits, axis=1, keepdims=True))
    w = e / jnp.sum(e, axis=1, keepdims=True)
    return am3, w


def count_column(cnt_row):
    return jnp.transpose(jnp.broadcast_to(cnt_row, (GROUP, GROUP)))[:, 0:1]


def char_fwd_tile(x, cnt, weights):
    g1, wqkv, wout, g2, wup, wdown, pq = weights
    rows = x.shape[0]
    groups = rows // GROUP
    xf = x.astype(F32)
    xhat, _ = ln_parts(xf)
    normed = (xhat * g1).astype(BF16)
    packed = mm(normed, wqkv).astype(BF16)
    low = pair_masks(GROUP)
    lw = word_of_lane(2 * GROUP)
    slot = lax.broadcasted_iota(jnp.int32, (16, 2 * GROUP), 0).astype(F32)
    probs, mixed, cols = [], [], []
    for g in range(groups):
        r = slice(g * GROUP, (g + 1) * GROUP)
        cnt_row = cnt[g : g + 1, :]
        cols.append(count_column(cnt_row))
        cnt2 = jnp.concatenate([cnt_row, cnt_row], axis=1)
        valid = slot < cnt2
        pg, mg = [], []
        for p in range(CHEADS // 2):
            q = packed[r, 128 * p : 128 * p + 128] * BF16(0.125)
            k = packed[r, 256 + 128 * p : 384 + 128 * p]
            v = packed[r, 512 + 128 * p : 640 + 128 * p]
            st = mm_nt(k, stack_heads(q, low))
            s = jnp.where(valid, compress(st, lw), MASKED)
            e = jnp.exp(s - jnp.max(s, axis=0, keepdims=True))
            pr = e / jnp.sum(e, axis=0, keepdims=True)
            pt = expand(pr.astype(BF16), lw)
            o = mm_tn(pt, v)
            pg.append(pr)
            mg.append(jnp.where(low, o[:GROUP], o[GROUP:]))
        probs.append(jnp.concatenate(pg, axis=1))
        mixed.append(jnp.concatenate(mg, axis=1))
    probs = jnp.concatenate(probs, axis=0)
    mixed = jnp.concatenate(mixed, axis=0).astype(BF16)
    aa = xf + mm(mixed, wout)
    ahat, _ = ln_parts(aa)
    middle = (ahat * g2).astype(BF16)
    upper, dgelu = gelu_both(mm(middle, wup))
    upper = upper.astype(BF16)
    am = aa + mm(upper, wdown)
    am3, w = pool_weights(am, pq, jnp.concatenate(cols, axis=0))
    pooled = jnp.sum(w * am3, axis=1)
    return packed, probs, mixed, aa, upper, dgelu.astype(BF16), am, pooled.astype(BF16)


def full_spec(shape):
    return pl.BlockSpec(shape, lambda i: (0,) * len(shape))


def rows_spec(rows, width):
    return pl.BlockSpec((rows, width), lambda i: (i, 0))


def char_mlp_back(cnt, aa, upper, dgelu, am, gpool_ref, base, weights):
    _, _, _, g2, wup, wdown, pq = weights
    rows = aa.shape[0]
    words = rows // 16
    cols = jnp.concatenate([count_column(cnt[g : g + 1, :]) for g in range(rows // GROUP)], axis=0)
    _, w = pool_weights(am, pq, cols)
    gp = jnp.concatenate(
        [jnp.broadcast_to(gpool_ref[pl.ds(base + i, 1), :], (16, 256)) for i in range(words)], axis=0
    )
    dw = jnp.sum(gp * am, axis=-1, keepdims=True).reshape(words, 16, 1)
    dlog = (w * (dw - jnp.sum(w * dw, axis=1, keepdims=True))).reshape(rows, 1)
    gm = w.reshape(rows, 1) * gp + dlog * pq
    d_pq = jnp.sum(dlog * am, axis=0, keepdims=True)
    gdl = gm.astype(BF16)
    d_down_t = mm_tn(gdl, upper)
    ghid = (dgelu.astype(F32) * mm_nt(gdl, wdown)).astype(BF16)
    ahat, ar = ln_parts(aa)
    middle = (ahat * g2).astype(BF16)
    d_up = mm_tn(middle, ghid)
    gmid = mm_nt(ghid, wup)
    gca = gm + ln_back(ahat, ar, g2, gmid)
    d_g2 = jnp.sum(gmid * ahat, axis=0, keepdims=True)
    return gca, d_up, d_down_t, d_g2, d_pq


def char_attn_back(x, packed, probs, mixed, gca, weights):
    g1, wqkv, wout = weights[:3]
    groups = x.shape[0] // GROUP
    low = pair_masks(GROUP)
    lw = word_of_lane(2 * GROUP)
    gcl = gca.astype(BF16)
    d_out = mm_tn(mixed, gcl)
    gcm = mm_nt(gcl, wout).astype(BF16)
    dqkv = []
    for g in range(groups):
        r = slice(g * GROUP, (g + 1) * GROUP)
        dq_g, dk_g, dv_g = [], [], []
        for p in range(CHEADS // 2):
            q = packed[r, 128 * p : 128 * p + 128] * BF16(0.125)
            k = packed[r, 256 + 128 * p : 384 + 128 * p]
            v = packed[r, 512 + 128 * p : 640 + 128 * p]
            do = stack_heads(gcm[r, 128 * p : 128 * p + 128], low)
            pr = probs[16 * g : 16 * g + 16, 256 * p : 256 * p + 256]
            dp = compress(mm_nt(v, do), lw)
            ds = (pr * (dp - jnp.sum(pr * dp, axis=0, keepdims=True))).astype(BF16)
            dst = expand(ds, lw)
            pt = expand(pr.astype(BF16), lw)
            dv_g.append(mm(pt, do))
            dk_g.append(mm(dst, stack_heads(q, low)))
            o = mm_tn(dst, k)
            dq_g.append(jnp.where(low, o[:GROUP], o[GROUP:]) * 0.125)
        dqkv.append(jnp.concatenate(dq_g + dk_g + dv_g, axis=1))
    dqkv = jnp.concatenate(dqkv, axis=0).astype(BF16)
    xhat, xr = ln_parts(x.astype(F32))
    normed = (xhat * g1).astype(BF16)
    d_qkv = mm_tn(normed, dqkv)
    gn = mm_nt(dqkv, wqkv)
    d_g1 = jnp.sum(gn * xhat, axis=0, keepdims=True)
    cg = gca + ln_back(xhat, xr, g1, gn)
    return cg, d_qkv, d_out, d_g1


def char_back_step(step, tiles, ins, cg, gca, accs):
    x, cnt, packed, probs, mixed, aa, upper, dgelu, am, gpool, vec, qo, up, dn = ins
    a_qo, a_up, a_dn, a_vec = accs
    weights = char_weights(vec, qo, up, dn)

    @pl.when(step == 0)
    def _():
        for acc in accs:
            acc[...] = jnp.zeros_like(acc)

    @pl.when(step < tiles)
    def _():
        grad, d_up, d_dn, d_g2, d_pq = char_mlp_back(cnt[0], aa[...], upper[...], dgelu[...], am[...], gpool, step * (ROWS // 16), weights)
        gca[span(step * ROWS, ROWS), :] = grad
        a_vec[1:2, :256] += d_g2
        a_vec[2:3, :256] += d_pq
        for i in range(8):
            t, c = i // 2, i % 2
            a_up[c, :, 128 * t : 128 * t + 128] += d_up[:, 128 * i : 128 * i + 128]
        for c in range(2):
            a_dn[c] += d_dn[128 * c : 128 * c + 128, :]

    @pl.when(step >= tiles)
    def _():
        grad, d_qkv, d_out, d_g1 = char_attn_back(x[...], packed[...], probs[...], mixed[...], gca[span((step - tiles) * ROWS, ROWS), :], weights)
        cg[...] = grad
        a_vec[0:1, :256] += d_g1
        for i in range(8):
            t, c = i // 2, i % 2
            val = d_qkv[:, 128 * i : 128 * i + 128] if i < 6 else d_out[:, 128 * (i - 6) : 128 * (i - 6) + 128]
            a_qo[c, :, 128 * t : 128 * t + 128] += val


ACCS = [(2, 256, 512), (2, 256, 512), (2, 128, 1024), (8, 512)]


def back_specs(tiles, gpool, weights):
    one = lambda i: jnp.minimum(i, tiles - 1)
    two = lambda i: jnp.maximum(i - tiles, 0)

    def rows_at(where, r, w):
        return pl.BlockSpec((r, w), lambda i: (where(i), 0))

    once = lambda sh: pl.BlockSpec(sh, lambda i: (0,) * len(sh), pipeline_mode=pl.Buffered(1))
    ins = [rows_at(two, ROWS, 256), pl.BlockSpec((1, ROWS // GROUP, GROUP), lambda i: (one(i), 0, 0))]
    ins += [rows_at(two, ROWS, 768), rows_at(two, ROWS // 8, 512), rows_at(two, ROWS, 256)]
    ins += [rows_at(one, ROWS, 256), rows_at(one, ROWS, 1024), rows_at(one, ROWS, 1024), rows_at(one, ROWS, 256)]
    ins += [once(gpool.shape)] + [once(w.shape) for w in weights]
    return ins, rows_at(two, ROWS, 256)


def char_bwd_kernel(tiles, *refs):
    ins, (cg, *accs), gca = refs[:14], refs[14:19], refs[19]
    char_back_step(pl.program_id(0), tiles, ins, cg, gca, accs)


def char_backward(x, cnt, saved, gpool, *weights):
    total = x.shape[0]
    tiles = total // ROWS
    ins, out = back_specs(tiles, gpool, weights)
    return pl.pallas_call(
        functools.partial(char_bwd_kernel, tiles),
        grid=(2 * tiles,),
        in_specs=ins,
        out_specs=[out] + [full_spec(s) for s in ACCS],
        out_shape=[jax.ShapeDtypeStruct((total, 256), F32)] + [jax.ShapeDtypeStruct(s, F32) for s in ACCS],
        scratch_shapes=[pltpu.VMEM((total, 256), F32)],
        compiler_params=pltpu.CompilerParams(vmem_limit_bytes=VMEM_LIMIT, dimension_semantics=("arbitrary",)),
        name="char_backward",
    )(x, cnt, *saved, gpool, *weights)


MESH = pl.DeviceIdType.MESH


def remote(src, dst, sems, index, where):
    return pltpu.make_async_remote_copy(
        src_ref=src, dst_ref=dst,
        send_sem=sems[0] if index is None else sems[0].at[index],
        recv_sem=sems[1] if index is None else sems[1].at[index],
        device_id=where, device_id_type=MESH,
    )


def span(start, size):
    return pl.ds(pl.multiple_of(start, size), size)


class Place:
    def __init__(self):
        self.f, self.c, self.t = lax.axis_index("fsdp"), lax.axis_index("ctx"), lax.axis_index("tp")
        self.F, self.T = lax.axis_size("fsdp"), lax.axis_size("tp")

    def fs(self, k):
        return lax.rem(self.f + k + self.F, self.F)

    def tp(self, k):
        return lax.rem(self.t + k + self.T, self.T)

    def peers(self):
        out = [{"fsdp": self.fs(k)} for k in range(1, self.F)]
        out += [{"tp": self.tp(k)} for k in range(1, self.T)]
        return out + [{"ctx": 1 - self.c}]


def greet(peers):
    barrier = pltpu.get_barrier_semaphore()
    for where in peers:
        pl.semaphore_signal(barrier, inc=1, device_id=where, device_id_type=MESH)
    pl.semaphore_wait(barrier, len(peers))


class Piece:
    def __init__(self, at, shard, whole, mine, landing, region, cores, planar, sems, local_sem, first):
        self.at, self.shard, self.whole = at, shard, whole
        self.mine, self.landing, self.region = mine, landing, region
        self.cores, self.planar = cores, planar
        self.sems, self.local_sem, self.first = sems, local_sem, first

    @staticmethod
    def slots(F, T):
        return (F - 1) + (T - 1) + T

    def local(self):
        at = self.at
        return pltpu.make_async_copy(self.shard.at[self.mine(at.c, at.t)], self.whole.at[self.landing(at.f, at.c, at.t)], self.local_sem)

    def z(self, k, incoming=False):
        at = self.at
        f = at.fs(-k) if incoming else at.f
        dst = self.whole.at[self.landing(f, at.c, at.t)]
        src = dst if incoming else self.shard.at[self.mine(at.c, at.t)]
        return remote(src, dst, self.sems, self.first + k - 1, {"fsdp": at.fs(k)})

    def plane(self, k, incoming=False):
        at = self.at
        r = self.whole.at[self.region(at.c, at.tp(-k) if incoming else at.t)]
        return remote(r, r, self.sems, self.first + at.F - 1 + k - 1, {"tp": at.tp(k)})

    def side(self, k, incoming=False):
        at = self.at
        r = self.whole.at[self.region(1 - at.c if incoming else at.c, at.tp(-k))]
        return remote(r, r, self.sems, self.first + at.F + at.T - 2 + k, {"ctx": 1 - at.c})

    def begin(self):
        self.local().start()
        for k in range(1, self.at.F):
            self.z(k).start()

    def spread(self):
        self.local().wait()
        for k in range(1, self.at.F):
            self.z(k, True).wait_recv()
        if self.planar:
            for k in range(1, self.at.T):
                self.plane(k).start()
            if self.cores:
                self.side(0).start()

    def pass_on(self):
        if self.planar:
            for k in range(1, self.at.T):
                self.plane(k, True).wait_recv()
                if self.cores:
                    self.side(k).start()

    def arrive(self):
        if self.planar and self.cores:
            for k in range(self.at.T):
                self.side(k, True).wait_recv()

    def drain(self):
        for k in range(1, self.at.F):
            self.z(k).wait_send()
        if self.planar:
            for k in range(1, self.at.T):
                self.plane(k).wait_send()
            if self.cores:
                for k in range(self.at.T):
                    self.side(k).wait_send()


ALL = slice(None)


def gather_pieces(at, shards, wholes, sems, local_sems):
    F, T = at.F, at.T
    qo, up, dn, pj, sm, w4, wu, wd = shards
    rq, rd, rw = qo.shape[0], dn.shape[0], w4.shape[1]
    cu = wu.shape[1]
    lanes = lambda c, t: span(256 * t + 128 * c, 128)
    table = [
        (lambda c, t: (ALL, lanes(c, t)), lambda f, c, t: (span(f * rq, rq), lanes(c, t)), lambda c, t: (ALL, lanes(c, t)), True, True),
        (lambda c, t: (ALL, lanes(c, t)), lambda f, c, t: (span(f * rq, rq), lanes(c, t)), lambda c, t: (ALL, lanes(c, t)), True, True),
        (lambda c, t: (span(rd // T * t, rd // T), span(128 * c, 128)), lambda f, c, t: (f, span(rd // T * t, rd // T), span(128 * c, 128)), lambda c, t: (ALL, span(rd // T * t, rd // T), span(128 * c, 128)), True, True),
        (lambda c, t: (ALL, span(128 * t, 128)), lambda f, c, t: (span(f * rq, rq), span(128 * t, 128)), lambda c, t: (ALL, span(128 * t, 128)), False, True),
        (lambda c, t: (ALL, ALL), lambda f, c, t: (f,), lambda c, t: (ALL,), False, False),
        (lambda c, t: (span(2 * c, 2),), lambda f, c, t: (span(2 * c, 2), span(f * rw, rw), span(128 * t, 128)), lambda c, t: (span(2 * c, 2), ALL, span(128 * t, 128)), True, True),
        (lambda c, t: (ALL, span(cu // 2 * c, cu // 2)), lambda f, c, t: (span(f * rw, rw), span(cu * t + cu // 2 * c, cu // 2)), lambda c, t: (ALL, span(cu * t + cu // 2 * c, cu // 2)), True, True),
        (lambda c, t: (span(cu // 2 * c, cu // 2), ALL), lambda f, c, t: (span(cu * t + cu // 2 * c, cu // 2), span(f * rw, rw)), lambda c, t: (span(cu * t + cu // 2 * c, cu // 2), ALL), True, True),
    ]
    slots = Piece.slots(F, T)
    return [
        Piece(at, shard, whole, mine, landing, region, cores, planar, sems, local_sems.at[i], i * slots)
        for i, (shard, whole, (mine, landing, region, cores, planar)) in enumerate(zip(shards, wholes, table))
    ]


FWD_OUTS = [(ROWS, 768, BF16), (ROWS // 8, 512, F32), (ROWS, 256, BF16), (ROWS, 256, F32), (ROWS, 1024, BF16), (ROWS, 1024, BF16), (ROWS, 256, F32), (ROWS // 16, 256, BF16)]


def char_weights(vec, qo, up, dn):
    return (vec[0:1, :256], qo[:, :768], qo[:, 768:], vec[1:2, :256], up[...], dn[...], vec[2:3, :256])


def char_fwd_kernel(x, cnt, vec, qo, up, dn, *outs):
    for ref, val in zip(outs, char_fwd_tile(x[...], cnt[0], char_weights(vec, qo, up, dn))):
        ref[...] = val


def char_forward(x, cnt, *weights):
    tiles = x.shape[0] // ROWS
    return pl.pallas_call(
        char_fwd_kernel,
        grid=(tiles,),
        in_specs=[rows_spec(ROWS, 256), pl.BlockSpec((1, ROWS // GROUP, GROUP), lambda i: (i, 0, 0))] + [full_spec(w.shape) for w in weights],
        out_specs=[rows_spec(r, w) for r, w, _ in FWD_OUTS],
        out_shape=[jax.ShapeDtypeStruct((r * tiles, w), d) for r, w, d in FWD_OUTS],
        compiler_params=pltpu.CompilerParams(vmem_limit_bytes=VMEM_LIMIT, dimension_semantics=("arbitrary",)),
        name="char_forward",
    )(x, cnt, *weights)


GATHERED = [((256, 1024), BF16), ((256, 1024), BF16), ((4, 256, 256), BF16), ((256, 512), BF16), ((4, 8, 128), F32), ((4, 512, 512), BF16), ((512, 2048), BF16), ((2048, 512), BF16)]


def vectors(sm):
    rows = []
    for i, n in ((0, 64), (1, 64), (2, 64), (3, 128), (4, 128)):
        v = jnp.concatenate([sm[f, i : i + 1, :n] for f in range(sm.shape[0])], axis=1)
        rows.append(v if n == 128 else jnp.concatenate([v, jnp.zeros_like(v)], axis=1))
    return jnp.concatenate(rows + [jnp.zeros((3, 512), F32)], axis=0)


def gather_fwd_kernel(*refs):
    n = len(GATHERED)
    x, cnt = refs[:2]
    shards = refs[2 : 2 + n]
    outs = refs[2 + n : 2 + n + len(FWD_OUTS)]
    full_out = refs[2 + n + len(FWD_OUTS) : 2 + 2 * n + len(FWD_OUTS)]
    vec_out = refs[2 + 2 * n + len(FWD_OUTS)]
    wholes = refs[3 + 2 * n + len(FWD_OUTS) : 3 + 3 * n + len(FWD_OUTS)]
    vec, send, recv, local_sems = refs[3 + 3 * n + len(FWD_OUTS) :]
    at = Place()
    pieces = gather_pieces(at, shards, wholes, (send, recv), local_sems)
    qo, up, dn, pj, sm, w4, wu, wd = pieces
    step = pl.program_id(0)
    last = pl.num_programs(0) - 1

    @pl.when(step == 0)
    def _():
        greet(at.peers())
        for p in pieces:
            p.begin()
        first = (qo, up, dn, sm)
        for p in first:
            p.spread()
        for p in first:
            p.pass_on()
        for p in first:
            p.arrive()
        vec[...] = vectors(wholes[4])
        vec_out[...] = vec[...]

    @pl.when(step == 1)
    def _():
        for p in (pj, w4, wu, wd):
            p.spread()

    @pl.when(step == 4)
    def _():
        pj.pass_on()
        w4.pass_on()

    dn2 = wholes[2][...].reshape(1024, 256)
    for ref, val in zip(outs, char_fwd_tile(x[...], cnt[0], char_weights(vec, wholes[0], wholes[1], dn2))):
        ref[...] = val

    @pl.when(step == last)
    def _():
        def out(i):
            return pltpu.make_async_copy(wholes[i], full_out[i], local_sems.at[i])

        for i in (0, 1, 2, 3):
            out(i).start()
        for p in (wu, wd):
            p.pass_on()
        for i, p in ((5, w4), (6, wu), (7, wd)):
            p.arrive()
            out(i).start()
        for p in pieces:
            p.drain()
        for i in (0, 1, 2, 3, 5, 6, 7):
            out(i).wait()


def gather_forward(x, cnt, shards):
    tiles = x.shape[0] // ROWS
    any_ = pl.BlockSpec(memory_space=pl.ANY)
    count = len(GATHERED) * Piece.slots(lax.axis_size("fsdp"), lax.axis_size("tp"))
    return pl.pallas_call(
        gather_fwd_kernel,
        grid=(tiles,),
        in_specs=[rows_spec(ROWS, 256), pl.BlockSpec((1, ROWS // GROUP, GROUP), lambda i: (i, 0, 0))] + [any_] * len(shards),
        out_specs=[rows_spec(r, w) for r, w, _ in FWD_OUTS] + [any_] * len(GATHERED) + [full_spec((8, 512))],
        out_shape=[jax.ShapeDtypeStruct((r * tiles, w), d) for r, w, d in FWD_OUTS] + [jax.ShapeDtypeStruct(sh, d) for sh, d in GATHERED] + [jax.ShapeDtypeStruct((8, 512), F32)],
        scratch_shapes=[pltpu.VMEM(sh, d) for sh, d in GATHERED]
        + [pltpu.VMEM((8, 512), F32), pltpu.SemaphoreType.DMA((count,)), pltpu.SemaphoreType.DMA((count,)), pltpu.SemaphoreType.DMA((len(GATHERED),))],
        compiler_params=pltpu.CompilerParams(vmem_limit_bytes=VMEM_LIMIT, collective_id=0, has_side_effects=True, dimension_semantics=("arbitrary",)),
        name="gather_forward",
    )(x, cnt, *shards)


def word_kernel(
    pooled, proj, words_in, cot, vec, w4, wup, wdown,
    block_out, rms, words_grad, gpool, d_proj, d_vec, d_w4, d_up, d_down,
    xall, kk, vv, kt, vt, ss, ee, qm, dom, mx, ll, ot, dqt, wkt, wvt, wout, dk_acc, dv_acc, dlt, dk_sum, dv_sum,
    dx, dx_in, dx_own, ag_send, ag_recv, rs_send, rs_recv,
):
    at = Place()
    T = at.T
    own = at.c * T + at.t
    nblk, blk, width = xall.shape
    half = HEADS // 2
    low = pair_masks(blk)
    first, second = range(half), range(half, HEADS)

    start = words_in[...].astype(F32) + mm(pooled[...], proj[...])
    shat, sr = ln_parts(start)
    g1v = vec[3:4, :]
    xall[own] = (shat * g1v).astype(BF16)
    greet([{"ctx": i, "tp": at.tp(k)} for i in (at.c, 1 - at.c) for k in range(T) if k > 0] + [{"ctx": 1 - at.c}])

    def row_copy(k, incoming=False):
        r = xall.at[at.c * T + (at.tp(-k) if incoming else at.t)]
        return remote(r, r, (ag_send, ag_recv), k - 1, {"tp": at.tp(k)})

    def side_copy(k):
        r = xall.at[at.tp(-k)]
        return remote(r, r, (ag_send, ag_recv), T - 1 + k, {"ctx": 1 - at.c})

    for k in range(1, T):

        @pl.when((at.c == 0) | (at.t + k < T))
        def _():
            row_copy(k).start()

    @pl.when(at.c == 0)
    def _():
        side_copy(0).start()

    wq, wk, wv, wot = w4.at[0], w4.at[1], w4.at[2], w4.at[3]
    wkt[...] = jnp.transpose(wk[...])
    wvt[...] = jnp.transpose(wv[...])
    wout[...] = jnp.transpose(wot[...])
    xown = xall[own]
    q = mm(xown, wq[...]).astype(BF16) * BF16(0.125)
    for p in range(HEADS // 2):
        a, b = split_heads(q[:, 128 * p : 128 * p + 128], low)
        qm[2 * p] = a
        qm[2 * p + 1] = b
    mx[...] = jnp.full(mx.shape, MASKED, F32)
    ll[...] = jnp.zeros(ll.shape, F32)
    ot[...] = jnp.zeros(ot.shape, F32)
    dqt[...] = jnp.zeros(dqt.shape, F32)
    dk_sum[...] = jnp.zeros(dk_sum.shape, F32)
    dv_sum[...] = jnp.zeros(dv_sum.shape, F32)

    def scores_of(j, heads):
        for h in heads:
            p = h // 2
            s = mm_nt(kk[j, :, 128 * p : 128 * p + 128], qm[h])
            ss[j, h % half] = s
            mx[h] = jnp.maximum(mx[h], jnp.max(s.reshape(blk // 8, 8, blk), axis=0))

    def mix_of(j, heads):
        for h in heads:
            e = jnp.exp(ss[j, h % half] - mx[h, 0:1, :])
            ll[h] += jnp.sum(e.reshape(blk // 8, 8, blk), axis=0)
            eb = e.astype(BF16)
            ee[j, h] = eb
            ot[64 * h : 64 * h + 64, :] += mm(vt[j, 64 * h : 64 * h + 64, :], eb)

    def top_of(heads):
        for h in heads:
            mx[h] = jnp.broadcast_to(jnp.max(mx[h], axis=0, keepdims=True), (8, blk))

    @pl.when(at.c == 0)
    def _():
        for k in range(1, T):
            row_copy(k, True).wait_recv()
            side_copy(k).start()

    @pl.loop(0, 2 * T)
    def _(m):
        k0 = m - 1
        k1 = m - T
        early = (m >= 1) & (m <= T)
        late = (m > T) & (at.c == 1) & (at.t >= k1)

        @pl.when(early & (at.c == 1))
        def _():
            r = xall.at[lax.rem(at.t - k0 + T, T)]
            remote(r, r, (ag_send, ag_recv), T - 1 + k0, {"ctx": 1 - at.c}).wait_recv()

        @pl.when(late)
        def _():
            r = xall.at[own - k1]
            remote(r, r, (ag_send, ag_recv), k1 - 1, {"tp": at.t - k1}).wait_recv()

        @pl.when((m == 0) | (early & ((at.c == 1) | ((m >= 2) & (at.t >= k0)))) | late)
        def _():
            is_early = early.astype(jnp.int32)
            is_late = (m > T).astype(jnp.int32)
            j = own + is_early * (lax.rem(at.t - k0 + T, T) - own) - is_late * k1
            xj = xall[j]
            kk[j] = mm(xj, wk[...]).astype(BF16)
            vv[j] = mm(xj, wv[...]).astype(BF16)
            kt[j] = mm_nt(wkt[...], xj).astype(BF16)
            vt[j] = mm_nt(wvt[...], xj).astype(BF16)
            scores_of(j, first)

    top_of(first)

    @pl.loop(0, own + 1)
    def _(j):
        mix_of(j, first)
        scores_of(j, second)

    top_of(second)

    @pl.loop(0, own + 1)
    def _(j):
        mix_of(j, second)

    for h in range(HEADS):
        linv = 1.0 / jnp.sum(ll[h], axis=0, keepdims=True)
        ll[h] = jnp.broadcast_to(linv, (8, blk))
        ot[64 * h : 64 * h + 64, :] = ot[64 * h : 64 * h + 64, :] * linv
    mixed_t = ot[...].astype(BF16)
    mixed = jnp.transpose(mixed_t)
    attn = mm(mixed, wout[...])
    awa = start + attn
    ahat, ar = ln_parts(awa)
    g2v = vec[4:5, :]
    n2 = (ahat * g2v).astype(BF16)
    upper, dgelu = gelu_both(mm(n2, wup[...]))
    upper = upper.astype(BF16)
    mlp = mm(upper, wdown[...])
    final = awa + mlp
    block_out[...] = final.astype(BF16)
    lane = lax.broadcasted_iota(jnp.int32, (blk, 128), 1)
    cols = [jnp.sqrt(jnp.mean(v * v, axis=-1, keepdims=True)) for v in (attn, mlp, final)]
    rms[...] = jnp.transpose(jnp.where(lane == 0, cols[0], jnp.where(lane == 1, cols[1], cols[2])))[0:3, :]
    cotv = cot[...]
    ff = wup.shape[1]
    cu = ff // T // 2
    gdown = mm_tn(upper, cotv).astype(BF16)
    ghid = (dgelu * mm_nt(cotv, wdown[...])).astype(BF16)
    gup = mm_tn(n2, ghid).astype(BF16)
    for c in range(2):
        for t in range(T):
            d_down[c, cu * t : cu * t + cu, :] = gdown[cu * (2 * t + c) : cu * (2 * t + c) + cu, :]
            d_up[c, :, cu * t : cu * t + cu] = gup[:, cu * (2 * t + c) : cu * (2 * t + c) + cu]
    gn2 = mm_nt(ghid, wup[...])
    d_g2 = jnp.sum(gn2 * ahat, axis=0, keepdims=True)
    ga = cotv.astype(F32) + ln_back(ahat, ar, g2v, gn2)
    gal = ga.astype(BF16)
    d_w4[1, 1] = mm_tn(gal, mixed).astype(BF16)
    do_t = mm_nt(wout[...], gal).astype(BF16)
    do_s = []
    for h in range(HEADS):
        r = slice(64 * h, 64 * h + 64)
        d = do_t[r, :].astype(F32)
        linv = ll[h, 0:1, :]
        dlt[h] = jnp.broadcast_to(jnp.sum(d * ot[r, :], axis=0, keepdims=True) * linv, (8, blk))
        do_s.append((d * linv).astype(BF16))
    do = jnp.transpose(jnp.concatenate(do_s, axis=0))
    for p in range(HEADS // 2):
        a, b = split_heads(do[:, 128 * p : 128 * p + 128], low)
        dom[2 * p] = a
        dom[2 * p + 1] = b

    def grad_copy(j):
        return remote(dx.at[j], dx_in.at[own], (rs_send.at[j], rs_recv.at[own]), None, {"ctx": j // T, "tp": lax.rem(j, T)})

    @pl.loop(0, own + 1)
    def _(j):
        @pl.when(j > 0)
        def _():
            grad_copy(j - 1).start()

        for p in range(HEADS // 2):
            c = slice(128 * p, 128 * p + 128)
            vp = vv[j, :, c]
            dk = None
            for h in (2 * p, 2 * p + 1):
                e = ee[j, h]
                dp = mm_nt(vp, dom[h])
                ds = (e.astype(F32) * (dp - dlt[h, 0:1, :])).astype(BF16)
                dvh = mm(e, dom[h])
                dkh = mm(ds, qm[h])
                dk, dv = (dkh, dvh) if dk is None else (dk + dkh, dv + dvh)
                dqt[64 * h : 64 * h + 64, :] += mm(kt[j, 64 * h : 64 * h + 64, :], ds)
            dk_acc[:, c] = dk.astype(BF16)
            dv_acc[:, c] = dv.astype(BF16)
        dk = dk_acc[...]
        dv = dv_acc[...]
        dxj = mm_nt(dk, wk[...]) + mm_nt(dv, wv[...])
        dx[j] = dxj.astype(BF16)
        dx_own[...] = dxj
        xt = jnp.transpose(xall[j])
        dk_sum[...] += mm(xt, dk)
        dv_sum[...] += mm(xt, dv)

    dq = jnp.transpose((dqt[...] * 0.125).astype(BF16))
    d_w4[0, 0] = mm_tn(xown, dq).astype(BF16)
    d_w4[0, 1] = dk_sum[...].astype(BF16)
    d_w4[1, 0] = dv_sum[...].astype(BF16)
    dx_own[...] += mm_nt(dq, wq[...])

    @pl.loop(own + 1, nblk)
    def _(b):
        remote(dx.at[own], dx_in.at[b], (rs_send.at[b], rs_recv.at[b]), None, {"ctx": 1 - at.c}).wait_recv()
        dx_own[...] += dx_in[b].astype(F32)

    gnf = dx_own[...]
    grad = ga + ln_back(shat, sr, g1v, gnf)
    words_grad[...] = grad
    d_vec[...] = jnp.concatenate([jnp.sum(gnf * shat, axis=0, keepdims=True), d_g2, jnp.zeros((6, width), F32)], axis=0)
    gproj = grad.astype(BF16)
    gproj_w = mm_tn(pooled[...], gproj).astype(BF16)
    hr = gproj_w.shape[0] // (2 * at.F)
    for i in range(at.F):
        for c in range(2):
            d_proj[c, hr * i : hr * i + hr, :] = gproj_w[hr * (2 * i + c) : hr * (2 * i + c) + hr, :]
    gpool[...] = mm_nt(gproj, proj[...])

    for k in range(1, T):

        @pl.when((at.c == 0) | (at.t + k < T))
        def _():
            row_copy(k).wait_send()

    @pl.when(at.c == 0)
    def _():
        for k in range(T):
            side_copy(k).wait_send()

    @pl.loop(0, own)
    def _(j):
        grad_copy(j).wait_send()


def word_section(pooled, proj, words_in, cot, vec, w4, wup, wdown):
    blk, width = words_in.shape
    T = lax.axis_size("tp")
    nblk = 2 * T
    ff = wup.shape[1]
    out_shapes = [((blk, width), BF16), ((3, blk), F32), ((blk, width), F32), ((blk, pooled.shape[1]), F32), ((2, proj.shape[0] // 2, width), BF16), ((8, width), F32)]
    out_shapes += [((2, 2) + w4.shape[1:], BF16), ((2, width, ff // 2), BF16), ((2, ff // 2, width), BF16)]
    vm = pl.BlockSpec(memory_space=pltpu.VMEM)
    return pl.pallas_call(
        word_kernel,
        in_specs=[vm] * 8,
        out_specs=[vm] * len(out_shapes),
        out_shape=[jax.ShapeDtypeStruct(s, d) for s, d in out_shapes],
        scratch_shapes=[
            pltpu.VMEM((nblk, blk, width), BF16),
            pltpu.VMEM((nblk, blk, width), BF16),
            pltpu.VMEM((nblk, blk, width), BF16),
            pltpu.VMEM((nblk, width, blk), BF16),
            pltpu.VMEM((nblk, width, blk), BF16),
            pltpu.VMEM((nblk, HEADS // 2, blk, blk), F32),
            pltpu.VMEM((nblk, HEADS, blk, blk), BF16),
            pltpu.VMEM((HEADS, blk, 128), BF16),
            pltpu.VMEM((HEADS, blk, 128), BF16),
            pltpu.VMEM((HEADS, 8, blk), F32),
            pltpu.VMEM((HEADS, 8, blk), F32),
            pltpu.VMEM((width, blk), F32),
            pltpu.VMEM((width, blk), F32),
            pltpu.VMEM((width, width), BF16),
            pltpu.VMEM((width, width), BF16),
            pltpu.VMEM((width, width), BF16),
            pltpu.VMEM((blk, width), BF16),
            pltpu.VMEM((blk, width), BF16),
            pltpu.VMEM((HEADS, 8, blk), F32),
            pltpu.VMEM((width, width), F32),
            pltpu.VMEM((width, width), F32),
            pltpu.VMEM((nblk, blk, width), BF16),
            pltpu.VMEM((nblk, blk, width), BF16),
            pltpu.VMEM((blk, width), F32),
            pltpu.SemaphoreType.DMA((2 * T,)),
            pltpu.SemaphoreType.DMA((2 * T,)),
            pltpu.SemaphoreType.DMA((nblk,)),
            pltpu.SemaphoreType.DMA((nblk,)),
        ],
        compiler_params=pltpu.CompilerParams(vmem_limit_bytes=VMEM_LIMIT, collective_id=1, has_side_effects=True),
        name="word_section",
    )(pooled, proj, words_in, cot, vec, w4, wup, wdown)


class Sum:
    def __init__(self, at, source, bufs, tp_cut, fs_cut, sems, first, wide):
        self.at, self.source, self.sems, self.first, self.wide = at, source, sems, first, wide
        self.own, self.away, self.got, self.blocks, self.block, self.pieces, self.done = bufs
        self.tp_cut, self.fs_cut = tp_cut, fs_cut

    @staticmethod
    def slots(F, T):
        return 1 + (T - 1) + (F - 1) + (T - 1) + T

    @staticmethod
    def buffers(half, block, piece, F, T, wide):
        shapes = [half, half, half, (T - 1,) + block, block, (F - 1,) + piece, ((2, T) if wide else (2,)) + piece]
        return [pltpu.VMEM(sh, BF16) for sh in shapes]

    def swap(self):
        at = self.at
        return remote(self.away, self.got, self.sems, self.first, {"ctx": 1 - at.c})

    def to_tp(self, k):
        return remote(self.own.at[self.tp_cut(self.at.tp(k))], self.blocks.at[k - 1], self.sems, self.first + k, {"tp": self.at.tp(k)})

    def to_fs(self, k):
        return remote(self.block.at[self.fs_cut(self.at.fs(k))], self.pieces.at[k - 1], self.sems, self.first + self.at.T - 1 + k, {"fsdp": self.at.fs(k)})

    def spread(self, k, incoming=False):
        at = self.at
        r = self.done.at[at.c, at.tp(-k) if incoming else at.t]
        return remote(r, r, self.sems, self.first + at.T + at.F - 2 + k, {"tp": at.tp(k)})

    def side(self, k, incoming=False):
        at = self.at
        c = 1 - at.c if incoming else at.c
        r = self.done.at[c, at.tp(-k)] if self.wide else self.done.at[c]
        return remote(r, r, self.sems, self.first + 2 * at.T + at.F - 2 + k, {"ctx": 1 - at.c})

    def local(self, i):
        src = self.source.at[self.at.c if i == 0 else 1 - self.at.c]
        return pltpu.make_async_copy(src, self.own if i == 0 else self.away, self.loc.at[i])

    def fetch(self, loc):
        self.loc = loc
        for i in range(2):
            self.local(i).start()

    def begin_fetched(self):
        for i in range(2):
            self.local(i).wait()
        self.swap().start()

    def begin(self):
        self.own[...] = self.source[self.at.c].astype(BF16)
        self.away[...] = self.source[1 - self.at.c].astype(BF16)
        self.swap().start()

    def halves(self):
        self.swap().wait_recv()
        self.own[...] = (self.own[...].astype(F32) + self.got[...].astype(F32)).astype(BF16)
        for k in range(1, self.at.T):
            self.to_tp(k).start()

    def over_tp(self):
        total = self.own[self.tp_cut(self.at.t)].astype(F32)
        for k in range(1, self.at.T):
            self.to_tp(k).wait_recv()
            total += self.blocks[k - 1].astype(F32)
        self.block[...] = total.astype(BF16)
        for k in range(1, self.at.F):
            self.to_fs(k).start()

    def over_fsdp(self):
        at = self.at
        total = self.block[self.fs_cut(at.f)].astype(F32)
        for k in range(1, at.F):
            self.to_fs(k).wait_recv()
            total += self.pieces[k - 1].astype(F32)
        if self.wide:
            self.done[at.c, at.t] = total.astype(BF16)
            for k in range(1, at.T):
                self.spread(k).start()
        else:
            self.done[at.c] = total.astype(BF16)
        self.side(0).start()

    def pass_on(self):
        if self.wide:
            for k in range(1, self.at.T):
                self.spread(k, True).wait_recv()
                self.side(k).start()

    def finish(self):
        at = self.at
        for k in range(at.T if self.wide else 1):
            self.side(k, True).wait_recv()

    def drain(self):
        at = self.at
        self.swap().wait_send()
        for k in range(1, at.T):
            self.to_tp(k).wait_send()
        for k in range(1, at.F):
            self.to_fs(k).wait_send()
        if self.wide:
            for k in range(1, at.T):
                self.spread(k).wait_send()
        for k in range(at.T if self.wide else 1):
            self.side(k).wait_send()


SUMS = [
    ((2, 512, 512), (2, 512, 128), (2, 128, 128), 2, 1, False),
    ((512, 1024), (512, 256), (128, 256), 1, 0, False),
    ((1024, 512), (256, 512), (256, 128), 0, 1, False),
    ((128, 512), (128, 128), (32, 128), 1, 0, True),
    ((256, 512), (256, 128), (64, 128), 1, 0, True),
    ((128, 1024), (32, 1024), (32, 256), 0, 1, True),
    ((256, 512), (256, 128), (64, 128), 1, 0, True),
]


def cutter(shape, axis, size):
    def cut(i):
        return tuple(span(i * size, size) if d == axis else ALL for d in range(len(shape)))

    return cut


RESULTS = [(3, 128, 128), (128, 128), (128, 512), (512, 128), (64, 512), (64, 1024), (256, 256), (64, 768), (64, 256), (8, 128)]


def reduce_bwd_kernel(tiles, *refs):
    ins = refs[:14]
    sources = refs[14:18]
    d_vec = refs[18]
    cg = refs[19]
    results = refs[20 : 20 + len(RESULTS)]
    rest = list(refs[20 + len(RESULTS) :])
    gca = rest.pop(0)
    accs = [rest.pop(0) for _ in ACCS]
    at = Place()
    bufs = [[rest.pop(0) for _ in range(7)] for _ in SUMS]
    vec_in, send, recv, vsend, vrecv, local_sems = rest
    slots = Sum.slots(at.F, at.T)
    a_qo, a_up, a_dn, a_vec = accs
    origin = list(sources) + [a_up, a_dn, a_qo]
    sums = []
    for i, (half, block, piece, ta, fa, wide) in enumerate(SUMS):
        sums.append(Sum(at, origin[i], bufs[i], cutter(half, ta, block[ta]), cutter(block, fa, piece[fa]), (send, recv), i * slots, wide))
        sums[i].loc = local_sems.at[i]
    w4, wup, wdn, pj, up, dn, qo = sums
    step = pl.program_id(0)
    last = 2 * tiles - 1

    def when(i, *acts):
        @pl.when(step == i)
        def _():
            for act in acts:
                act()

    def open_():
        for s in (w4, wup, wdn, pj):
            s.fetch(s.loc)
        greet(at.peers())
        for s in (w4, wup, wdn, pj):
            s.begin_fetched()

    when(0, open_)
    when(1, w4.halves)
    when(2, wup.halves)
    when(3, wdn.halves, pj.halves)
    when(6, w4.over_tp)
    when(8, up.begin, dn.begin)
    when(10, up.halves, dn.halves, w4.over_fsdp, wup.over_tp)
    when(13, wup.over_fsdp, wdn.over_tp, pj.over_tp)
    char_back_step(step, tiles, ins, cg, gca, accs)

    @pl.when(step == last)
    def _():
        qo.begin()
        a_vec[3:5, :] = d_vec[0:2, :]

        def vec_copy(i, where):
            return remote(a_vec, vec_in.at[i], (vsend, vrecv), i, where)

        vec_copy(0, {"ctx": 1 - at.c}).start()
        wdn.over_fsdp()
        pj.over_fsdp()
        up.over_tp()
        dn.over_tp()
        qo.halves()
        vec_copy(0, {"ctx": 1 - at.c}).wait()
        a_vec[...] += vec_in[0]
        for k in range(1, at.T):
            vec_copy(k, {"tp": at.tp(k)}).start()
        up.over_fsdp()
        dn.over_fsdp()
        pj.pass_on()
        for k in range(1, at.T):
            vec_copy(k, {"tp": at.tp(k)}).wait()
        a_vec[...] += vec_in[1] + vec_in[2] + vec_in[3]
        for k in range(1, at.F):
            vec_copy(at.T - 1 + k, {"fsdp": at.fs(k)}).start()
        qo.over_tp()
        up.pass_on()
        dn.pass_on()
        for k in range(1, at.F):
            vec_copy(at.T - 1 + k, {"fsdp": at.fs(k)}).wait()
        total = a_vec[...] + (vec_in[4] + vec_in[5] + vec_in[6])
        rows = []
        for i, n in ((0, 64), (1, 64), (2, 64), (3, 128), (4, 128)):
            v = jnp.zeros((1, n), F32)
            for f in range(4):
                v = jnp.where(at.f == f, total[i : i + 1, f * n : f * n + n], v)
            rows.append(v if n == 128 else jnp.concatenate([v, jnp.zeros((1, n), F32)], axis=1))
        results[9][...] = jnp.concatenate(rows + [jnp.zeros((3, 128), F32)], axis=0)
        for s in (w4, wup, wdn):
            s.finish()
        o4, o_out, o_wup, o_wdn, o_pj, o_up, o_dn, o_qkv, o_cout = results[:9]
        for c in range(2):
            o_wup[:, 256 * c : 256 * c + 256] = wup.done[c].astype(F32)
            o_wdn[256 * c : 256 * c + 256, :] = wdn.done[c].astype(F32)
        o4[0] = w4.done[0, 0].astype(F32)
        o4[1] = w4.done[0, 1].astype(F32)
        o4[2] = w4.done[1, 0].astype(F32)
        o_out[...] = jnp.transpose(w4.done[1, 1].astype(F32))
        qo.over_fsdp()
        for s in (pj, up, dn):
            s.finish()
        for t in range(at.T):
            for c in range(2):
                lanes = slice(256 * t + 128 * c, 256 * t + 128 * c + 128)
                o_pj[32 * c : 32 * c + 32, 128 * t : 128 * t + 128] = pj.done[c, t].astype(F32)
                o_up[:, lanes] = up.done[c, t].astype(F32)
        o_dn[...] = jnp.transpose(dn.done[...].astype(F32).reshape(256, 256))
        qo.pass_on()
        qo.finish()
        for t in range(at.T):
            for c in range(2):
                i = 2 * t + c
                ref = o_qkv if i < 6 else o_cout
                i = i % 6
                ref[:, 128 * i : 128 * i + 128] = qo.done[c, t].astype(F32)
        for s in sums:
            s.drain()


def reduce_backward(x, cnt, saved, gpool, weights, sources, d_vec):
    total = x.shape[0]
    tiles = total // ROWS
    F, T = lax.axis_size("fsdp"), lax.axis_size("tp")
    ins, out = back_specs(tiles, gpool, weights)
    any_ = pl.BlockSpec(memory_space=pl.ANY)
    scratch = [pltpu.VMEM((total, 256), F32)] + [pltpu.VMEM(s, F32) for s in ACCS]
    for half, block, piece, _, _, wide in SUMS:
        scratch += Sum.buffers(half, block, piece, F, T, wide)
    count = len(SUMS) * Sum.slots(F, T)
    vecs = 1 + (T - 1) + (F - 1)
    scratch += [pltpu.VMEM((vecs, 8, 512), F32)]
    scratch += [pltpu.SemaphoreType.DMA((n,)) for n in (count, count, vecs, vecs)] + [pltpu.SemaphoreType.DMA((len(SUMS), 2))]
    return pl.pallas_call(
        functools.partial(reduce_bwd_kernel, tiles),
        grid=(2 * tiles,),
        in_specs=ins + [any_] * len(sources) + [full_spec((8, 512))],
        out_specs=[out] + [full_spec(s) for s in RESULTS],
        out_shape=[jax.ShapeDtypeStruct((total, 256), F32)] + [jax.ShapeDtypeStruct(s, F32) for s in RESULTS],
        scratch_shapes=scratch,
        compiler_params=pltpu.CompilerParams(vmem_limit_bytes=VMEM_LIMIT, collective_id=2, has_side_effects=True, dimension_semantics=("arbitrary",)),
        name="reduce_backward",
    )(x, cnt, *saved, gpool, *weights, *sources, d_vec)


def gather(x, name, axis):
    return lax.all_gather(x, name, axis=axis, tiled=True)


def scatter(x, name, axis):
    return lax.psum_scatter(x, name, scatter_dimension=axis, tiled=True)


def fits(rows):
    return lax.axis_size("fsdp") == 4 and lax.axis_size("tp") == 4 and rows == 64


def local(characters, counts, words_in, cotangent, char_prenorm, char_qkv, char_out, char_midnorm, char_up, char_down,
          pool_query, char_proj, word_prenorm, word_qkv, word_out, word_midnorm, word_up, word_down):
    words, slots, cdim = characters.shape
    x = characters.reshape(words * slots, cdim)
    cnt = jnp.repeat(counts.astype(F32), slots).reshape(words * slots // ROWS, ROWS // GROUP, GROUP)
    vectors_in = (char_prenorm, char_midnorm, pool_query, word_prenorm, word_midnorm)
    qo = jnp.concatenate([char_qkv, char_out], axis=1)
    w4 = jnp.concatenate([jnp.moveaxis(word_qkv, 1, 0), word_out.T[None]], axis=0)
    direct = fits(char_prenorm.shape[0])
    if direct:
        pad = lambda v: jnp.pad(v.astype(F32), (0, 128 - v.shape[0]))
        small = jnp.stack([pad(v) for v in vectors_in] + [jnp.zeros((128,), F32)] * 3)
        *saved, pooled_low, qo, up, dn, proj, _, w4, wup, wdown, vec = gather_forward(x, cnt, [qo, char_up, char_down, char_proj, small, w4, word_up, word_down])
        dn = dn.reshape(1024, 256)
    else:
        wide = [gather(v.astype(F32), "fsdp", 0) for v in vectors_in]
        vec = jnp.stack([jnp.pad(v, (0, 512 - v.shape[0])) for v in wide] + [jnp.zeros((512,), F32)] * 3)
        qo, up, dn, proj = (gather(w, "fsdp", 0) for w in (qo, char_up, char_down, char_proj))
        w4 = gather(gather(w4, "fsdp", 1), "tp", 2)
        wup = gather(gather(word_up, "fsdp", 0), "tp", 1)
        wdown = gather(gather(word_down, "fsdp", 1), "tp", 0)
        *saved, pooled_low = char_forward(x, cnt, vec, qo, up, dn)
    (block_out, rms, words_grad, gpool, d_proj, d_vec, d_w4, d_wup, d_wdown) = word_section(pooled_low, proj, words_in, cotangent, vec, w4, wup, wdown)
    if direct:
        cg, g_qkv4, g_wout, g_wup, g_wdown, g_proj, g_up, g_down, g_qkv, g_out, g_vec = reduce_backward(
            x, cnt, saved, gpool, [vec, qo, up, dn], [d_w4, d_wup, d_wdown, d_proj], d_vec
        )
        vecs = [g_vec[i, :n] for i, n in ((0, 64), (1, 64), (2, 64), (3, 128), (4, 128))]
    else:
        cg, a_qo, a_up, a_dn, a_vec = char_backward(x, cnt, saved, gpool, vec, qo, up, dn)

        def reduce_char(g):
            g = lax.psum(g.astype(BF16), ("ctx", "tp"))
            return scatter(g, "fsdp", 0).astype(F32)

        def reduce_word(g, tp_axis, fsdp_axis):
            g = scatter(g, "tp", tp_axis)
            g = lax.psum(g, "ctx")
            return scatter(g, "fsdp", fsdp_axis).astype(F32)

        lanes = lambda g, n: jnp.moveaxis(g.reshape(2, g.shape[1], -1, n), 0, 2).reshape(g.shape[1], -1)
        hr = char_proj.shape[0] // 2
        ff = word_up.shape[1] // 2
        g_qo = reduce_char(lanes(a_qo, 128))
        g_qkv, g_out = g_qo[:, :768], g_qo[:, 768:]
        g_up = reduce_char(lanes(a_up, 128))
        g_down = reduce_char(a_dn.reshape(256, 1024).T)
        g_proj = reduce_char(jnp.moveaxis(d_proj.reshape(2, -1, hr, 512), 0, 1).reshape(256, 512))
        g_w4 = reduce_word(d_w4.reshape(4, 512, 512), 2, 1)
        g_qkv4, g_wout = g_w4[:3], g_w4[3].T
        g_wup = reduce_word(lanes(d_wup, ff), 1, 0)
        g_wdown = reduce_word(jnp.moveaxis(d_wdown.reshape(2, -1, ff, 512), 0, 1).reshape(2048, 512), 0, 1)
        vecs = [reduce_char(v) for v in (a_vec[0, :256], a_vec[1, :256], a_vec[2, :256], d_vec[0], d_vec[1])]
    return (
        block_out,
        cg.reshape(words, slots, cdim),
        words_grad,
        rms,
        vecs[0],
        g_qkv,
        g_out,
        vecs[1],
        g_up,
        g_down,
        vecs[2],
        g_proj,
        vecs[3],
        jnp.moveaxis(g_qkv4, 0, 1),
        g_wout,
        vecs[4],
        g_wup,
        g_wdown,
    )


def solution(mesh):
    rows = ("fsdp", "ctx", "tp")
    v, m = P("fsdp"), P("fsdp", None)
    return jax.shard_map(
        local,
        mesh=mesh,
        in_specs=(
            P(rows, None, None), P(rows), P(rows, None), P(rows, None),
            v, m, m, v, m, m, v, m, v, P("fsdp", None, "tp"), P("tp", "fsdp"), v, P("fsdp", "tp"), P("tp", "fsdp"),
        ),
        out_specs=(
            P(rows, None), P(rows, None, None), P(rows, None), P(None, rows),
            v, m, m, v, m, m, v, m, v, P("fsdp", None, "tp"), P("tp", "fsdp"), v, P("fsdp", "tp"), P("tp", "fsdp"),
        ),
        check_vma=False,
    )
```

```python
import functools

import jax
import jax.numpy as jnp
from jax import lax
from jax.experimental import pallas as pl
from jax.experimental.pallas import tpu as pltpu
from jax.sharding import PartitionSpec as P

CHEADS = 4
HEADS = 8
HEAD = 64
EPSILON = 1e-05
MASKED = -1e30
CGELU = 0.7978845608028654
AGELU = 0.044715
ROWS = 512
GROUP = 128
F32 = jnp.float32
BF16 = jnp.bfloat16
VMEM_LIMIT = 66_000_000


def mm(a, b):
    return lax.dot_general(a, b, (((1,), (0,)), ((), ())), preferred_element_type=F32)


def mm_nt(a, b):
    return lax.dot_general(a, b, (((1,), (1,)), ((), ())), preferred_element_type=F32)


def mm_tn(a, b):
    return lax.dot_general(a, b, (((0,), (0,)), ((), ())), preferred_element_type=F32)


def ln_parts(x):
    c = x - jnp.mean(x, axis=-1, keepdims=True)
    r = lax.rsqrt(jnp.mean(c * c, axis=-1, keepdims=True) + EPSILON)
    return c * r, r


def ln_back(xhat, r, gain, g):
    gg = g * gain
    a = jnp.mean(gg, axis=-1, keepdims=True)
    b = jnp.mean(gg * xhat, axis=-1, keepdims=True)
    return r * (gg - a - xhat * b)


def gelu_both(x):
    x2 = x * x
    y = (CGELU * AGELU) * x2 + CGELU
    hp = 0.5 * jnp.tanh(x * y) + 0.5
    g = x * hp
    d = hp + (g - g * hp) * (6.0 * y - 4.0 * CGELU)
    return g, d


def pair_masks(rows):
    lane = lax.broadcasted_iota(jnp.int32, (rows, 128), 1)
    return lane < HEAD


def split_heads(x, low_lanes):
    zero = jnp.zeros_like(x)
    return jnp.where(low_lanes, x, zero), jnp.where(low_lanes, zero, x)


def stack_heads(x, low_lanes):
    a, b = split_heads(x, low_lanes)
    return jnp.concatenate([a, b], axis=0)


def word_of_lane(width):
    return (lax.broadcasted_iota(jnp.int32, (16, width), 1) % GROUP) // 16


def compress(blocks, lane_word):
    out = blocks[0:16, :]
    for w in range(1, GROUP // 16):
        out = jnp.where(lane_word == w, blocks[16 * w : 16 * w + 16, :], out)
    return out


def expand(dense, lane_word):
    zero = jnp.zeros_like(dense)
    return jnp.concatenate(
        [jnp.where(lane_word == w, dense, zero) for w in range(GROUP // 16)], axis=0
    )


def pool_weights(am, q_row, cnt_col):
    words = am.shape[0] // 16
    am3 = am.reshape(words, 16, am.shape[1])
    logits = jnp.sum(am * q_row, axis=-1, keepdims=True)
    slot = (lax.broadcasted_iota(jnp.int32, (am.shape[0], 1), 0) % 16).astype(F32)
    logits = jnp.where(slot < cnt_col, logits, MASKED).reshape(words, 16, 1)
    e = jnp.exp(logits - jnp.max(logits, axis=1, keepdims=True))
    w = e / jnp.sum(e, axis=1, keepdims=True)
    return am3, w


def count_column(cnt_row):
    return jnp.transpose(jnp.broadcast_to(cnt_row, (GROUP, GROUP)))[:, 0:1]


def char_attn_tile(x, cnt, weights):
    g1, wqkv, wout = weights[:3]
    groups = x.shape[0] // GROUP
    xf = x.astype(F32)
    xhat, _ = ln_parts(xf)
    normed = (xhat * g1).astype(BF16)
    packed = mm(normed, wqkv).astype(BF16)
    low = pair_masks(GROUP)
    lw = word_of_lane(2 * GROUP)
    slot = lax.broadcasted_iota(jnp.int32, (16, 2 * GROUP), 0).astype(F32)
    raw, values, scores = [], [], []
    for g in range(groups):
        r = slice(g * GROUP, (g + 1) * GROUP)
        for p in range(CHEADS // 2):
            q = packed[r, 128 * p : 128 * p + 128] * BF16(0.125)
            values.append(packed[r, 512 + 128 * p : 640 + 128 * p])
            raw.append(mm_nt(packed[r, 256 + 128 * p : 384 + 128 * p], stack_heads(q, low)))
    pairs = len(raw)
    for i, st in enumerate(raw):
        cnt_row = cnt[i // 2 : i // 2 + 1, :]
        scores.append(jnp.where(slot < jnp.concatenate([cnt_row, cnt_row], axis=1), compress(st, lw), MASKED))
    scores = jnp.concatenate(scores, axis=0).reshape(pairs, 16, 2 * GROUP)
    e = jnp.exp(scores - jnp.max(scores, axis=1, keepdims=True))
    probs = e / jnp.sum(e, axis=1, keepdims=True)
    low_probs = probs.astype(BF16)
    spread = [expand(low_probs[i], lw) for i in range(pairs)]
    mixed = [mm_tn(pt, v) for pt, v in zip(spread, values)]
    mixed = [jnp.where(low, o[:GROUP], o[GROUP:]) for o in mixed]
    probs = jnp.concatenate([jnp.concatenate([probs[2 * g], probs[2 * g + 1]], axis=1) for g in range(groups)], axis=0)
    mixed = jnp.concatenate([jnp.concatenate(mixed[2 * g : 2 * g + 2], axis=1) for g in range(groups)], axis=0).astype(BF16)
    return packed, probs, mixed, xf + mm(mixed, wout)


def char_mlp_tile(aa, cnt, weights):
    _, _, _, g2, wup, wdown, pq = weights
    ahat, _ = ln_parts(aa)
    middle = (ahat * g2).astype(BF16)
    upper, dgelu = gelu_both(mm(middle, wup))
    upper = upper.astype(BF16)
    am = aa + mm(upper, wdown)
    cols = jnp.concatenate([count_column(cnt[g : g + 1, :]) for g in range(aa.shape[0] // GROUP)], axis=0)
    am3, w = pool_weights(am, pq, cols)
    pooled = jnp.sum(w * am3, axis=1)
    return upper, dgelu.astype(BF16), am, pooled.astype(BF16)


def count_lanes(counts):
    take = GROUP // 16
    w = lax.broadcasted_iota(jnp.int32, (128, GROUP), 0)
    l = lax.broadcasted_iota(jnp.int32, (128, GROUP), 1)
    spread = (lax.rem(w, take) == l // 16).astype(BF16)
    g = lax.broadcasted_iota(jnp.int32, (128 // take, 128), 0)
    lane = lax.broadcasted_iota(jnp.int32, (128 // take, 128), 1)
    rows = []
    for r in range(counts.shape[0]):
        one = jnp.where(lane // take == g, counts[r : r + 1, :].astype(F32), 0.0).astype(BF16)
        rows.append(mm(one, spread))
    return jnp.concatenate(rows, axis=0)


def full_spec(shape):
    return pl.BlockSpec(shape, lambda i: (0,) * len(shape))


def rows_spec(rows, width):
    return pl.BlockSpec((rows, width), lambda i: (i, 0))


def char_mlp_back(cnt, aa, upper, dgelu, am, gpool_ref, base, weights):
    _, _, _, g2, wup, wdown, pq = weights
    rows = aa.shape[0]
    words = rows // 16
    cols = jnp.concatenate([count_column(cnt[g : g + 1, :]) for g in range(rows // GROUP)], axis=0)
    _, w = pool_weights(am, pq, cols)
    gp = jnp.concatenate(
        [jnp.broadcast_to(gpool_ref[pl.ds(base + i, 1), :], (16, 256)) for i in range(words)], axis=0
    )
    dw = jnp.sum(gp * am, axis=-1, keepdims=True).reshape(words, 16, 1)
    dlog = (w * (dw - jnp.sum(w * dw, axis=1, keepdims=True))).reshape(rows, 1)
    gm = w.reshape(rows, 1) * gp + dlog * pq
    d_pq = jnp.sum(dlog * am, axis=0, keepdims=True)
    gdl = gm.astype(BF16)
    d_down_t = mm_tn(gdl, upper)
    ghid = (dgelu.astype(F32) * mm_nt(gdl, wdown)).astype(BF16)
    ahat, ar = ln_parts(aa)
    middle = (ahat * g2).astype(BF16)
    d_up = mm_tn(middle, ghid)
    gmid = mm_nt(ghid, wup)
    gca = gm + ln_back(ahat, ar, g2, gmid)
    d_g2 = jnp.sum(gmid * ahat, axis=0, keepdims=True)
    return gca, d_up, d_down_t, d_g2, d_pq


def char_attn_back(x, packed, probs, mixed, gca, weights):
    g1, wqkv, wout = weights[:3]
    groups = x.shape[0] // GROUP
    low = pair_masks(GROUP)
    lw = word_of_lane(2 * GROUP)
    gcl = gca.astype(BF16)
    d_out = mm_tn(mixed, gcl)
    gcm = mm_nt(gcl, wout).astype(BF16)
    keys, queries, grads, raw, prs = [], [], [], [], []
    for g in range(groups):
        r = slice(g * GROUP, (g + 1) * GROUP)
        for p in range(CHEADS // 2):
            queries.append(stack_heads(packed[r, 128 * p : 128 * p + 128] * BF16(0.125), low))
            keys.append(packed[r, 256 + 128 * p : 384 + 128 * p])
            grads.append(stack_heads(gcm[r, 128 * p : 128 * p + 128], low))
            raw.append(mm_nt(packed[r, 512 + 128 * p : 640 + 128 * p], grads[-1]))
            prs.append(probs[16 * g : 16 * g + 16, 256 * p : 256 * p + 256])
    pairs = len(raw)
    dp = jnp.concatenate([compress(v, lw) for v in raw], axis=0).reshape(pairs, 16, 2 * GROUP)
    pr = jnp.concatenate(prs, axis=0).reshape(pairs, 16, 2 * GROUP)
    ds = (pr * (dp - jnp.sum(pr * dp, axis=1, keepdims=True))).astype(BF16)
    pr = pr.astype(BF16)
    dst = [expand(ds[i], lw) for i in range(pairs)]
    pt = [expand(pr[i], lw) for i in range(pairs)]
    dq = [mm_tn(dst[i], keys[i]) for i in range(pairs)]
    dq = [jnp.where(low, o[:GROUP], o[GROUP:]) * 0.125 for o in dq]
    dk = [mm(dst[i], queries[i]) for i in range(pairs)]
    dv = [mm(pt[i], grads[i]) for i in range(pairs)]
    dqkv = [jnp.concatenate([v[2 * g + p] for v in (dq, dk, dv) for p in range(2)], axis=1) for g in range(groups)]
    dqkv = jnp.concatenate(dqkv, axis=0).astype(BF16)
    xhat, xr = ln_parts(x.astype(F32))
    normed = (xhat * g1).astype(BF16)
    gn = mm_nt(dqkv, wqkv)
    grad = gca + ln_back(xhat, xr, g1, gn)
    return grad, mm_tn(normed, dqkv), d_out, gn * xhat


def char_back_step(step, tiles, ins, cg, gca, accs, gains):
    x, cnt, packed, probs, mixed, aa, upper, dgelu, am, gpool, vec, qo, up, dn = ins
    a_qo, a_up, a_dn, a_vec = accs
    weights = char_weights(vec, qo, up, dn)

    @pl.when(step == 0)
    def _():
        for acc in accs:
            acc[...] = jnp.zeros_like(acc)

    @pl.when(step < tiles)
    def _():
        grad, d_up, d_dn, d_g2, d_pq = char_mlp_back(cnt[0], aa[...], upper[...], dgelu[...], am[...], gpool, step * (ROWS // 16), weights)
        gca[span(step * ROWS, ROWS), :] = grad
        if gains:
            a_vec[1:2, :256] += d_g2
        a_vec[2:3, :256] += d_pq
        for i in range(8):
            t, c = i // 2, i % 2
            a_up[c, :, 128 * t : 128 * t + 128] += d_up[:, 128 * i : 128 * i + 128]
        for c in range(2):
            a_dn[c] += d_dn[128 * c : 128 * c + 128, :]

    @pl.when(step >= tiles)
    def _():
        r = span((step - tiles) * ROWS, ROWS)
        grad, d_qkv, d_out, terms = char_attn_back(x[...], packed[...], probs[...], mixed[...], gca[r, :], weights)
        cg[...] = grad
        if gains:
            a_vec[0:1, :256] += jnp.sum(terms, axis=0, keepdims=True)
        for i in range(8):
            t, c = i // 2, i % 2
            val = d_qkv[:, 128 * i : 128 * i + 128] if i < 6 else d_out[:, 128 * (i - 6) : 128 * (i - 6) + 128]
            a_qo[c, :, 128 * t : 128 * t + 128] += val


ACCS = [(2, 256, 512), (2, 256, 512), (2, 128, 1024), (8, 512)]


def back_specs(tiles, gpool, weights):
    one = lambda i: jnp.minimum(i, tiles - 1)
    two = lambda i: jnp.maximum(i - tiles, 0)

    def rows_at(where, r, w):
        return pl.BlockSpec((r, w), lambda i: (where(i), 0))

    once = lambda sh: pl.BlockSpec(sh, lambda i: (0,) * len(sh), pipeline_mode=pl.Buffered(1))
    ins = [rows_at(two, ROWS, 256), pl.BlockSpec((1, ROWS // GROUP, GROUP), lambda i: (one(i), 0, 0))]
    ins += [rows_at(two, ROWS, 768), rows_at(two, ROWS // 8, 512), rows_at(two, ROWS, 256)]
    ins += [rows_at(one, ROWS, 256), rows_at(one, ROWS, 1024), rows_at(one, ROWS, 1024), rows_at(one, ROWS, 256)]
    ins += [once(gpool.shape)] + [once(w.shape) for w in weights]
    return ins, rows_at(two, ROWS, 256)


def char_bwd_kernel(tiles, *refs):
    ins, (cg, *accs), gca = refs[:14], refs[14:19], refs[19]
    char_back_step(pl.program_id(0), tiles, ins, cg, gca, accs, True)


def char_backward(x, cnt, saved, gpool, *weights):
    total = x.shape[0]
    tiles = total // ROWS
    ins, out = back_specs(tiles, gpool, weights)
    return pl.pallas_call(
        functools.partial(char_bwd_kernel, tiles),
        grid=(2 * tiles,),
        in_specs=ins,
        out_specs=[out] + [full_spec(s) for s in ACCS],
        out_shape=[jax.ShapeDtypeStruct((total, 256), F32)] + [jax.ShapeDtypeStruct(s, F32) for s in ACCS],
        scratch_shapes=[pltpu.VMEM((total, 256), F32)],
        compiler_params=pltpu.CompilerParams(vmem_limit_bytes=VMEM_LIMIT, dimension_semantics=("arbitrary",)),
        name="char_backward",
    )(x, cnt, *saved, gpool, *weights)


MESH = pl.DeviceIdType.MESH


def remote(src, dst, sems, index, where):
    return pltpu.make_async_remote_copy(
        src_ref=src, dst_ref=dst,
        send_sem=sems[0] if index is None else sems[0].at[index],
        recv_sem=sems[1] if index is None else sems[1].at[index],
        device_id=where, device_id_type=MESH,
    )


def span(start, size):
    return pl.ds(pl.multiple_of(start, size), size)


class Place:
    def __init__(self):
        self.f, self.c, self.t = lax.axis_index("fsdp"), lax.axis_index("ctx"), lax.axis_index("tp")
        self.F, self.T = lax.axis_size("fsdp"), lax.axis_size("tp")

    def fs(self, k):
        return lax.rem(self.f + k + self.F, self.F)

    def tp(self, k):
        return lax.rem(self.t + k + self.T, self.T)

    def peers(self):
        out = [{"fsdp": self.fs(k)} for k in range(1, self.F)]
        out += [{"tp": self.tp(k)} for k in range(1, self.T)]
        out += [{"ctx": 1 - self.c, "tp": self.tp(k)} for k in range(1, self.T)]
        return out + [{"ctx": 1 - self.c}]


def call(peers):
    for where in peers:
        pl.semaphore_signal(pltpu.get_barrier_semaphore(), inc=1, device_id=where, device_id_type=MESH)


def meet(peers):
    pl.semaphore_wait(pltpu.get_barrier_semaphore(), len(peers))


def greet(peers):
    call(peers)
    meet(peers)


class Piece:
    def __init__(self, at, shard, whole, mine, landing, region, sems, local_sem, first, side=True, core=None, source=None):
        self.at, self.shard, self.whole = at, shard, whole
        self.mine, self.landing, self.region = mine, landing, region
        self.sems, self.local_sem, self.first = sems, local_sem, first
        self.cores, self.core, self.source = side, core, source

    @staticmethod
    def slots(F, T):
        return (F - 1) + (T - 1) + T

    def held(self, act, other=False):
        if self.core is None:
            act()
        else:
            pl.when(self.at.c == (1 - self.core if other else self.core))(act)

    def local(self, src):
        at = self.at
        return pltpu.make_async_copy(src, self.whole.at[self.landing(at.f, at.c, at.t)], self.local_sem)

    def z(self, k, src=None):
        at = self.at
        f = at.fs(-k) if src is None else at.f
        dst = self.whole.at[self.landing(f, at.c, at.t)]
        return remote(dst if src is None else src, dst, self.sems, self.first + k - 1, {"fsdp": at.fs(k)})

    def plane(self, k, incoming=False):
        at = self.at
        r = self.whole.at[self.region(at.c, at.tp(-k) if incoming else at.t)]
        return remote(r, r, self.sems, self.first + at.F - 1 + k - 1, {"tp": at.tp(k)})

    def side(self, k, incoming=False):
        at = self.at
        c = at.c if self.core is not None else (1 - at.c if incoming else at.c)
        r = self.whole.at[self.region(c, at.tp(-k))]
        return remote(r, r, self.sems, self.first + at.F + at.T - 2 + k, {"ctx": 1 - at.c})

    def begin(self):
        at = self.at

        def go(src):
            self.local(src).start()
            for k in range(1, at.F):
                self.z(k, src).start()

        if self.source is not None:
            for cond, src in self.source:
                pl.when(cond)(functools.partial(go, src))
        else:
            self.held(lambda: go(self.shard.at[self.mine(at.c, at.t)]))

    def landed(self):
        at = self.at
        dst = self.whole.at[self.landing(at.f, at.c, at.t)]
        pltpu.make_async_copy(dst, dst, self.local_sem).wait()
        for k in range(1, at.F):
            self.z(k).wait_recv()

    def spread(self):
        def go():
            self.landed()
            if self.region is not None:
                for k in range(1, self.at.T):
                    self.plane(k).start()
                if self.cores:
                    self.side(0).start()

        self.held(go)

    def pass_on(self):
        def go():
            for k in range(1, self.at.T):
                self.plane(k, True).wait_recv()
                if self.cores:
                    self.side(k).start()

        if self.region is not None:
            self.held(go)

    def arrive(self):
        def go():
            for k in range(self.at.T):
                self.side(k, True).wait_recv()

        if self.region is not None and self.cores:
            self.held(go, True)

    def drain(self):
        def go():
            for k in range(1, self.at.F):
                self.z(k).wait_send()
            if self.region is not None:
                for k in range(1, self.at.T):
                    self.plane(k).wait_send()
                if self.cores:
                    for k in range(self.at.T):
                        self.side(k).wait_send()

        self.held(go)


ALL = slice(None)
GATHERED = [((256, 1024), BF16), ((256, 1024), BF16), ((4, 256, 256), BF16), ((256, 512), BF16), ((4, 8, 128), F32), ((3, 512, 512), BF16), ((512, 512), BF16), ((512, 256), BF16), ((256, 512), BF16)]


def gather_pieces(at, shards, wholes, sems, local_sems):
    F, T = at.F, at.T
    qkv, out, up, dn, pj, sm, w3, wo, wu, wd = shards
    rq, rd, rw = up.shape[0], dn.shape[0], w3.shape[1]
    cu = wu.shape[1] // 2
    lanes = lambda c, t: span(256 * t + 128 * c, 128)
    cols = (lambda c, t: (ALL, lanes(c, t)), lambda f, c, t: (span(f * rq, rq), lanes(c, t)), lambda c, t: (ALL, lanes(c, t)))
    n = qkv.shape[1] // 256
    inside = lax.rem(at.t, n)
    qo_source = [(at.t < n, qkv.at[:, span(256 * inside + 128 * at.c, 128)]), (at.t == n, out.at[:, span(128 * at.c, 128)])]
    quarter = rd // T
    slots = Piece.slots(F, T)
    specs = [
        (None, wholes[0], *cols, dict(source=qo_source)),
        (up, wholes[1], *cols, {}),
        (dn, wholes[2], lambda c, t: (span(quarter * t, quarter), span(128 * c, 128)), lambda f, c, t: (f, span(quarter * t, quarter), span(128 * c, 128)), lambda c, t: (ALL, span(quarter * t, quarter), span(128 * c, 128)), {}),
        (pj, wholes[3], lambda c, t: (ALL, span(128 * t, 128)), lambda f, c, t: (span(f * rq, rq), span(128 * t, 128)), lambda c, t: (ALL, span(128 * t, 128)), dict(side=False)),
        (sm, wholes[4], lambda c, t: (ALL, ALL), lambda f, c, t: (f,), None, dict(side=False)),
        (w3, wholes[5], lambda c, t: (span(0, 2),), lambda f, c, t: (span(0, 2), span(f * rw, rw), span(128 * t, 128)), lambda c, t: (span(0, 2), ALL, span(128 * t, 128)), dict(core=0)),
        (w3, wholes[5], lambda c, t: (pl.ds(2, 1),), lambda f, c, t: (pl.ds(2, 1), span(f * rw, rw), span(128 * t, 128)), lambda c, t: (pl.ds(2, 1), ALL, span(128 * t, 128)), dict(core=1)),
        (wo, wholes[6], lambda c, t: (ALL, ALL), lambda f, c, t: (span(t * rw, rw), span(128 * f, 128)), lambda c, t: (span(t * rw, rw), ALL), dict(core=1)),
        (wu, wholes[7], lambda c, t: (ALL, span(cu * c, cu)), lambda f, c, t: (span(f * rw, rw), ALL), None, {}),
        (wd, wholes[8], lambda c, t: (span(cu * c, cu), ALL), lambda f, c, t: (ALL, span(f * rw, rw)), None, {}),
    ]
    return [
        Piece(at, shard, whole, mine, landing, region, sems, local_sems.at[i], i * slots, **more)
        for i, (shard, whole, mine, landing, region, more) in enumerate(specs)
    ]


PIECES = 10


FWD_OUTS = [(ROWS, 768, BF16), (ROWS // 8, 512, F32), (ROWS, 256, BF16), (ROWS, 256, F32), (ROWS, 1024, BF16), (ROWS, 1024, BF16), (ROWS, 256, F32), (ROWS // 16, 256, BF16)]


def char_weights(vec, qo, up, dn):
    return (vec[0:1, :256], qo[:, :768], qo[:, 768:], vec[1:2, :256], up[...], dn[...], vec[2:3, :256])


def char_fwd_kernel(x, cnt, vec, qo, up, dn, *outs):
    w = char_weights(vec, qo, up, dn)
    first = char_attn_tile(x[...], cnt[0], w)
    for ref, val in zip(outs, first + char_mlp_tile(first[3], cnt[0], w)):
        ref[...] = val


def char_forward(x, cnt, *weights):
    tiles = x.shape[0] // ROWS
    return pl.pallas_call(
        char_fwd_kernel,
        grid=(tiles,),
        in_specs=[rows_spec(ROWS, 256), pl.BlockSpec((1, ROWS // GROUP, GROUP), lambda i: (i, 0, 0))] + [full_spec(w.shape) for w in weights],
        out_specs=[rows_spec(r, w) for r, w, _ in FWD_OUTS],
        out_shape=[jax.ShapeDtypeStruct((r * tiles, w), d) for r, w, d in FWD_OUTS],
        compiler_params=pltpu.CompilerParams(vmem_limit_bytes=VMEM_LIMIT, dimension_semantics=("arbitrary",)),
        name="char_forward",
    )(x, cnt, *weights)


def vectors(sm):
    rows = []
    for i, n in enumerate((64, 64, 64, 128, 128)):
        v = jnp.concatenate([sm[f, i : i + 1, :n] for f in range(sm.shape[0])], axis=1)
        rows.append(v if n == 128 else jnp.concatenate([v, jnp.zeros_like(v)], axis=1))
    return jnp.concatenate(rows + [jnp.zeros((3, 512), F32)], axis=0)


CHUNKS = ((0, 4), (4, 6), (6, 8))
LAG = 5


def gather_fwd_kernel(*refs):
    refs = list(refs)
    take = lambda n: [refs.pop(0) for _ in range(n)]
    x, counts, words_in = take(3)
    small_in = take(5)
    shards = take(PIECES - 1)
    outs = take(len(FWD_OUTS))
    full_out = take(len(GATHERED))
    vec_out, cnt_out, xall = take(3)
    wholes = take(len(GATHERED))
    vec, cnt, xown, pool, kept, small, send, recv, xsend, xrecv, local_sems = refs
    shards.insert(5, small)
    at = Place()
    T = at.T
    own = at.c * T + at.t
    part = ROWS // 16
    pieces = gather_pieces(at, shards, wholes, (send, recv), local_sems)
    qo, up, dn, pj, sm, wa, wb, wo, zu, zd = pieces
    step = pl.program_id(0)
    last = pl.num_programs(0) - 1

    def out(i):
        return pltpu.make_async_copy(wholes[i], full_out[i], local_sems.at[PIECES + i])

    def chunk(i):
        lo, hi = CHUNKS[i]
        return span(lo * part, (hi - lo) * part) if lo % (hi - lo) == 0 else pl.ds(lo * part, (hi - lo) * part)

    def row_copy(i, k, incoming=False):
        dst = xall.at[at.c * T + (at.tp(-k) if incoming else at.t), chunk(i)]
        return remote(dst if incoming else xown.at[chunk(i)], dst, (xsend, xrecv), i * 2 * T + k - 1, {"tp": at.tp(k)})

    def side_copy(i, k):
        dst = xall.at[at.tp(-k), chunk(i)]
        return remote(xown.at[chunk(i)] if k == 0 else dst, dst, (xsend, xrecv), i * 2 * T + T - 1 + k, {"ctx": 1 - at.c})

    def keep(i):
        return pltpu.make_async_copy(xown.at[chunk(i)], xall.at[own, chunk(i)], local_sems.at[PIECES + len(GATHERED) + i])

    def cross_copy(k):
        dst = xall.at[own, chunk(1)]
        return remote(xown.at[chunk(1)], dst, (xsend, xrecv), 2 * T + T - 1 + k, {"ctx": 1, "tp": at.tp(k)})

    def crossed(k):
        dst = xall.at[at.tp(-k), chunk(1)]
        return remote(dst, dst, (xsend, xrecv), 2 * T + T - 1 + k, {"ctx": 1 - at.c})

    def send_rows(i):
        keep(i).start()
        for k in range(1, T):
            pl.when(((at.c == 0) & (i == 0)) | (at.t + k < T))(lambda k=k: row_copy(i, k).start())

        @pl.when(at.c == 0)
        def _():
            for k in range(T if i else 1):
                (cross_copy(k) if i else side_copy(0, 0)).start()

    def pass_rows(i):
        @pl.when(at.c == 0)
        def _():
            for k in range(1, T):
                row_copy(i, k, True).wait_recv()
                side_copy(i, k).start()

    def take_rows(i):
        for k in range(T):
            pl.when(at.c == 1)(lambda k=k: (crossed(k) if i else side_copy(i, k)).wait_recv())
        for k in range(1, T):
            pl.when((at.t >= k) & ((at.c == 1) | (i == 1)))(lambda k=k: row_copy(i, k, True).wait_recv())

    def drain_rows(i):
        keep(i).wait()
        for k in range(1, T):
            pl.when(((at.c == 0) & (i == 0)) | (at.t + k < T))(lambda k=k: row_copy(i, k).wait_send())

        @pl.when(at.c == 0)
        def _():
            for k in range(T):
                (cross_copy(k) if i else side_copy(0, k)).wait_send()

    tiles = pl.num_programs(0) - LAG

    def when(i, *acts):
        @pl.when(step == i)
        def _():
            for act in acts:
                act()

    def open_():
        small[...] = jnp.zeros_like(small)
        for i, v in enumerate(small_in):
            small[i : i + 1, : v.shape[1]] = v[...].astype(F32)
        greet(at.peers())
        for p in (qo, sm):
            p.begin()
        cnt[...] = count_lanes(counts[...])
        cnt_out[...] = cnt[...]
        qo.spread()
        for p in (up, dn):
            p.begin()
        sm.spread()
        vec[...] = vectors(wholes[4])
        vec_out[...] = vec[...]
        qo.pass_on()
        qo.arrive()
        for p in (up, dn):
            p.spread()
        for p in (pj, wa, wb, wo):
            p.begin()

    def copy_out(*which):
        for i in which:
            out(i).start()

    groups = ROWS // GROUP

    def count_rows(i):
        return jnp.concatenate([cnt[pl.ds(i * groups + g, 1), :] for g in range(groups)], axis=0)

    def rows_of(i):
        r = chunk(i)
        start = words_in[r, :].astype(F32) + mm(pool[r, :], wholes[3][...])
        xown[r, :] = (ln_parts(start)[0] * vec[3:4, :]).astype(BF16)

    when(0, open_)
    when(6, *[p.spread for p in (pj, wa, wb, wo)])
    when(7, zu.begin, zd.begin)
    when(8, pj.pass_on, lambda: copy_out(0, 1, 2))
    when(9, lambda: send_rows(0))
    when(11, wa.pass_on, wb.pass_on, wo.pass_on, lambda: send_rows(1), lambda: copy_out(3))
    when(12, lambda: pass_rows(0), wa.arrive, wb.arrive, wo.arrive, lambda: copy_out(5, 6), zu.spread, zd.spread, lambda: copy_out(7, 8))

    @pl.when(step < tiles)
    def _():
        first = char_attn_tile(x[...], count_rows(step), (vec[0:1, :256], wholes[0][:, :768], wholes[0][:, 768:]))
        for ref, val in zip(outs[:4], first):
            ref[...] = val
        kept[lax.rem(step, LAG + 1)] = first[3]

    when(LAG, *[p.pass_on for p in (up, dn)], *[p.arrive for p in (up, dn)])

    @pl.when(step >= LAG)
    def _():
        i = step - LAG
        second = char_mlp_tile(kept[lax.rem(i, LAG + 1)], count_rows(i), (None, None, None, vec[1:2, :256], wholes[1][...], wholes[2][...].reshape(1024, 256), vec[2:3, :256]))
        for ref, val in zip(outs[4:], second):
            ref[...] = val
        pool[span(i * part, part), :] = second[3]

    when(3 + LAG, lambda: rows_of(0))
    when(5 + LAG, lambda: rows_of(1))

    @pl.when(step == last)
    def _():
        rows_of(2)
        keep(2).start()
        for p in pieces:
            p.drain()
        for i in (0, 1, 2, 3, 5, 6, 7, 8):
            out(i).wait()
        for i in range(2):
            take_rows(i)
            drain_rows(i)
        keep(2).wait()


def gather_forward(x, counts, words_in, small, shards):
    tiles = x.shape[0] // ROWS
    F, T = lax.axis_size("fsdp"), lax.axis_size("tp")
    any_ = pl.BlockSpec(memory_space=pl.ANY)
    count = PIECES * Piece.slots(F, T)
    words, width = words_in.shape
    nchunk = len(CHUNKS) * 2 * T

    def early(r, w):
        return pl.BlockSpec((r, w), lambda i: (jnp.minimum(i, tiles - 1), 0))

    def late(r, w):
        return pl.BlockSpec((r, w), lambda i: (jnp.maximum(i - LAG, 0), 0))

    return pl.pallas_call(
        gather_fwd_kernel,
        grid=(tiles + LAG,),
        in_specs=[early(ROWS, 256), full_spec(counts.shape), full_spec(words_in.shape)] + [full_spec(v.shape) for v in small] + [any_] * len(shards),
        out_specs=[early(r, w) for r, w, _ in FWD_OUTS[:4]] + [late(r, w) for r, w, _ in FWD_OUTS[4:]] + [any_] * len(GATHERED) + [full_spec((8, 512)), full_spec((x.shape[0] // GROUP, GROUP)), any_],
        out_shape=[jax.ShapeDtypeStruct((r * tiles, w), d) for r, w, d in FWD_OUTS]
        + [jax.ShapeDtypeStruct(sh, d) for sh, d in GATHERED]
        + [jax.ShapeDtypeStruct((8, 512), F32), jax.ShapeDtypeStruct((x.shape[0] // GROUP, GROUP), F32), jax.ShapeDtypeStruct((2 * T, words, width), BF16)],
        scratch_shapes=[pltpu.VMEM(sh, d) for sh, d in GATHERED]
        + [pltpu.VMEM((8, 512), F32), pltpu.VMEM((x.shape[0] // GROUP, GROUP), F32), pltpu.VMEM((words, width), BF16), pltpu.VMEM((words, 256), BF16), pltpu.VMEM((LAG + 1, ROWS, 256), F32), pltpu.VMEM((8, 128), F32)]
        + [pltpu.SemaphoreType.DMA((n,)) for n in (count, count, nchunk, nchunk, PIECES + len(GATHERED) + len(CHUNKS))],
        compiler_params=pltpu.CompilerParams(vmem_limit_bytes=VMEM_LIMIT, collective_id=0, has_side_effects=True, dimension_semantics=("arbitrary",)),
        name="gather_forward",
    )(x, counts, words_in, *small, *shards)


def word_kernel(
    pooled, proj, words_in, cot, vec, xin, w3_in, wo_in, zu, zd,
    block_out, rms, words_grad, gpool, d_proj, d_vec, h_w4, h_up, h_down,
    xall, kk, vv, kt, vt, ss, ee, qm, dom, mx, ll, ot, dqt, wkt, wvt, w3, wout, wup, wdown, dk_acc, dv_acc, dlt, dk_sum, dv_sum,
    dx_in, dx_own, g_up, g_down, g_w4, in_up, in_down, in_w4,
    xlast, w_send, w_recv, g_send, g_recv, rs_send, rs_recv, x_send, x_recv, local_sems,
):
    at = Place()
    T = at.T
    own = at.c * T + at.t
    nblk, blk, width = xall.shape
    dx = kk
    half = HEADS // 2
    low = pair_masks(blk)
    first, second = range(half), range(half, HEADS)
    cu = zu.shape[1]
    loads = [pltpu.make_async_copy(src, dst, local_sems.at[i]) for i, (src, dst) in enumerate(((w3_in, w3), (xin, xall), (wo_in, wout)))]
    for load in loads:
        load.start()

    near = (at.t + 1 - 2 * lax.rem(at.t, 2), lax.rem(at.t + 2, T))
    far = T - 1 - at.t

    def area(c, t, i, part=None):
        r = span(2 * cu * t + cu * c, cu)
        if part is None:
            return wup.at[:, r] if i == 0 else wdown.at[r, :]
        if i == 0:
            return wup.at[pl.ds(part * width // 2, width // 2), r]
        return wdown.at[span(2 * cu * t + cu * c + part * (cu // 2), cu // 2), :]

    def wide(n, i, incoming=False):
        dst = area(at.c, near[n] if incoming else at.t, i)
        return remote(dst if incoming else (zu, zd)[i], dst, (w_send, w_recv), 2 * n + i, {"tp": near[n]})

    def onward(n, i, incoming=False):
        dst = area(at.c, far if incoming else near[1 - n], i, n)
        return remote(dst, dst, (w_send, w_recv), 4 + 2 * n + i, {"tp": near[n]})

    def side(k, i, incoming=False):
        t = (at.t, near[0], near[1], far)[k]
        dst = area(1 - at.c if incoming else at.c, t, i)
        return remote((zu, zd)[i] if k == 0 and not incoming else dst, dst, (w_send, w_recv), 8 + 2 * k + i, {"ctx": 1 - at.c})

    def mine(i):
        return pltpu.make_async_copy((zu, zd)[i], area(at.c, at.t, i), local_sems.at[3 + i])

    plane = [{"ctx": i, "tp": at.tp(k)} for i in (at.c, 1 - at.c) for k in range(T) if k > 0] + [{"ctx": 1 - at.c}]
    call(plane)
    tail = xlast.shape[1]
    lead = blk - tail

    start = words_in[...].astype(F32) + mm(pooled[...], proj[...])
    shat, sr = ln_parts(start)
    g1v = vec[3:4, :]
    wq, wk, wv = w3.at[0], w3.at[1], w3.at[2]
    loads[0].wait()
    wkt[...] = jnp.transpose(wk[...])
    wvt[...] = jnp.transpose(wv[...])
    loads[1].wait()
    xown = xall[own]
    q = mm(xown, wq[...]).astype(BF16) * BF16(0.125)
    for p in range(HEADS // 2):
        a, b = split_heads(q[:, 128 * p : 128 * p + 128], low)
        qm[2 * p] = a
        qm[2 * p + 1] = b
    mx[...] = jnp.full(mx.shape, MASKED, F32)
    ll[...] = jnp.zeros(ll.shape, F32)
    ot[...] = jnp.zeros(ot.shape, F32)
    dqt[...] = jnp.zeros(dqt.shape, F32)
    dk_sum[...] = jnp.zeros(dk_sum.shape, F32)
    dv_sum[...] = jnp.zeros(dv_sum.shape, F32)

    def scores_of(j, heads):
        for h in heads:
            p = h // 2
            s = mm_nt(kk[j, :, 128 * p : 128 * p + 128], qm[h])
            ss[j, h % half] = s
            mx[h] = jnp.maximum(mx[h], jnp.max(s.reshape(blk // 8, 8, blk), axis=0))

    def mix_of(j, heads):
        for h in heads:
            e = jnp.exp(ss[j, h % half] - mx[h, 0:1, :])
            ll[h] += jnp.sum(e.reshape(blk // 8, 8, blk), axis=0)
            eb = e.astype(BF16)
            ee[j, h] = eb
            ot[64 * h : 64 * h + 64, :] += mm(vt[j, 64 * h : 64 * h + 64, :], eb)

    def top_of(heads):
        for h in heads:
            mx[h] = jnp.broadcast_to(jnp.max(mx[h], axis=0, keepdims=True), (8, blk))

    meet(plane)

    def got_rows(j, sem):
        pltpu.make_async_remote_copy(
            src_ref=xlast.at[j], dst_ref=xlast.at[j], send_sem=x_send.at[0], recv_sem=x_recv.at[sem],
            device_id={"ctx": 1 - at.c}, device_id_type=MESH,
        ).wait_recv()
        xall[j, lead:, :] = xlast[j]

    for k in range(T):

        @pl.when((at.c == 0) & (at.t + k < T) & (k > 0))
        def _():
            if k:
                remote(xin.at[own, pl.ds(lead, tail)], xlast.at[own], (x_send.at[2 * k], x_recv.at[2 * k]), None, {"ctx": 0, "tp": at.tp(k)}).start()

        @pl.when((at.c == 0) | ((at.t + k < T) & (k > 0)))
        def _():
            remote(xin.at[own, pl.ds(lead, tail)], xlast.at[own], (x_send.at[2 * k + 1], x_recv.at[2 * k + 1 + 2 * T * at.c]), None, {"ctx": 1, "tp": at.tp(k)}).start()


    def others():
        for k in range(T):
            pl.when((at.c == 0) & (at.t >= k) & (k > 0))(lambda k=k: got_rows(at.t - k, 2 * k))
            pl.when(at.c == 1)(lambda k=k: got_rows(at.tp(-k), 2 * k + 1))
            pl.when((at.c == 1) & (at.t >= k) & (k > 0))(lambda k=k: got_rows(T + at.t - k, 2 * k + 1 + 2 * T))
        for i in range(2):
            for n in range(2):
                wide(n, i).start()
            side(0, i).start()
            mine(i).start()

    pl.when(own == 0)(others)

    @pl.loop(0, own + 1)
    def _(m):
        pl.when(m == 1)(others)
        j = own - m
        xj = xall[j]
        kk[j] = mm(xj, wk[...]).astype(BF16)
        vv[j] = mm(xj, wv[...]).astype(BF16)
        kt[j] = mm_nt(wkt[...], xj).astype(BF16)
        vt[j] = mm_nt(wvt[...], xj).astype(BF16)
        scores_of(j, first)

    top_of(first)

    @pl.loop(0, own + 1)
    def _(j):
        mix_of(j, first)
        scores_of(j, second)

    top_of(second)
    for i in range(2):
        for n in range(2):
            wide(n, i, True).wait_recv()
        for n in range(2):
            onward(n, i).start()
            side(1 + n, i).start()

    @pl.loop(0, own + 1)
    def _(j):
        mix_of(j, second)

    for h in range(HEADS):
        linv = 1.0 / jnp.sum(ll[h], axis=0, keepdims=True)
        ll[h] = jnp.broadcast_to(linv, (8, blk))
        ot[64 * h : 64 * h + 64, :] = ot[64 * h : 64 * h + 64, :] * linv
    mixed_t = ot[...].astype(BF16)
    mixed = jnp.transpose(mixed_t)
    loads[2].wait()
    attn = mm(mixed, wout[...])
    awa = start + attn
    ahat, ar = ln_parts(awa)
    g2v = vec[4:5, :]
    n2 = (ahat * g2v).astype(BF16)
    for i in range(2):
        for n in range(2):
            onward(n, i, True).wait_recv()
        side(3, i).start()
    for i in range(2):
        mine(i).wait()
        for k in range(4):
            side(k, i, True).wait_recv()
    upper, dgelu = gelu_both(mm(n2, wup[...]))
    upper = upper.astype(BF16)
    mlp = mm(upper, wdown[...])
    final = awa + mlp
    block_out[...] = final.astype(BF16)
    lane = lax.broadcasted_iota(jnp.int32, (blk, 128), 1)
    cols = [jnp.sqrt(jnp.mean(v * v, axis=-1, keepdims=True)) for v in (attn, mlp, final)]
    rms[...] = jnp.transpose(jnp.where(lane == 0, cols[0], jnp.where(lane == 1, cols[1], cols[2])))[0:3, :]
    cotv = cot[...]
    gdown = mm_tn(upper, cotv).astype(BF16)
    ghid = (dgelu * mm_nt(cotv, wdown[...])).astype(BF16)
    gup = mm_tn(n2, ghid).astype(BF16)
    for c in range(2):
        for t in range(T):
            g_down[c, cu * t : cu * t + cu, :] = gdown[cu * (2 * t + c) : cu * (2 * t + c) + cu, :]
            g_up[c, :, cu * t : cu * t + cu] = gup[:, cu * (2 * t + c) : cu * (2 * t + c) + cu]
    grads = ((g_down, in_down, h_down), (g_up, in_up, h_up), (g_w4, in_w4, h_w4))

    def swap(i):
        return remote(grads[i][0].at[1 - at.c], grads[i][1], (g_send, g_recv), i, {"ctx": 1 - at.c})

    def store(i):
        return pltpu.make_async_copy(grads[i][0].at[at.c], grads[i][2], local_sems.at[5 + i])

    def add_halves(i):
        g, other, _ = grads[i]
        swap(i).wait_recv()
        g[at.c] = (g[at.c].astype(F32) + other[...].astype(F32)).astype(BF16)
        store(i).start()

    gn2 = mm_nt(ghid, wup[...])
    d_g2 = jnp.sum(gn2 * ahat, axis=0, keepdims=True)
    ga = cotv.astype(F32) + ln_back(ahat, ar, g2v, gn2)
    gal = ga.astype(BF16)
    g_w4[1, 1] = mm_tn(gal, mixed).astype(BF16)
    swap(0).start()
    swap(1).start()
    do_t = mm_nt(wout[...], gal).astype(BF16)
    do_s = []
    for h in range(HEADS):
        r = slice(64 * h, 64 * h + 64)
        d = do_t[r, :].astype(F32)
        linv = ll[h, 0:1, :]
        dlt[h] = jnp.broadcast_to(jnp.sum(d * ot[r, :], axis=0, keepdims=True) * linv, (8, blk))
        do_s.append((d * linv).astype(BF16))
    do = jnp.transpose(jnp.concatenate(do_s, axis=0))
    for p in range(HEADS // 2):
        a, b = split_heads(do[:, 128 * p : 128 * p + 128], low)
        dom[2 * p] = a
        dom[2 * p + 1] = b

    add_halves(0)
    add_halves(1)

    def grad_copy(j):
        return remote(dx.at[j], dx_in.at[own], (rs_send.at[j], rs_recv.at[own]), None, {"ctx": j // T, "tp": lax.rem(j, T)})

    @pl.loop(0, own + 1)
    def _(j):
        @pl.when(j > 0)
        def _():
            grad_copy(j - 1).start()

        for p in range(HEADS // 2):
            c = slice(128 * p, 128 * p + 128)
            vp = vv[j, :, c]
            dk = None
            for h in (2 * p, 2 * p + 1):
                e = ee[j, h]
                dp = mm_nt(vp, dom[h])
                ds = (e.astype(F32) * (dp - dlt[h, 0:1, :])).astype(BF16)
                dvh = mm(e, dom[h])
                dkh = mm(ds, qm[h])
                dk, dv = (dkh, dvh) if dk is None else (dk + dkh, dv + dvh)
                dqt[64 * h : 64 * h + 64, :] += mm(kt[j, 64 * h : 64 * h + 64, :], ds)
            dk_acc[:, c] = dk.astype(BF16)
            dv_acc[:, c] = dv.astype(BF16)
        dk = dk_acc[...]
        dv = dv_acc[...]
        dxj = mm_nt(dk, wk[...]) + mm_nt(dv, wv[...])
        dx[j] = dxj.astype(BF16)
        dx_own[...] = dxj
        xt = jnp.transpose(xall[j])
        dk_sum[...] += mm(xt, dk)
        dv_sum[...] += mm(xt, dv)

    dq = jnp.transpose((dqt[...] * 0.125).astype(BF16))
    g_w4[0, 0] = mm_tn(xown, dq).astype(BF16)
    g_w4[0, 1] = dk_sum[...].astype(BF16)
    g_w4[1, 0] = dv_sum[...].astype(BF16)
    swap(2).start()
    dx_own[...] += mm_nt(dq, wq[...])

    @pl.loop(own + 1, nblk)
    def _(b):
        remote(dx.at[own], dx_in.at[b], (rs_send.at[b], rs_recv.at[b]), None, {"ctx": 1 - at.c}).wait_recv()
        dx_own[...] += dx_in[b].astype(F32)

    gnf = dx_own[...]
    grad = ga + ln_back(shat, sr, g1v, gnf)
    words_grad[...] = grad
    d_vec[...] = jnp.concatenate([jnp.sum(gnf * shat, axis=0, keepdims=True), d_g2, jnp.zeros((6, width), F32)], axis=0)
    gproj = grad.astype(BF16)
    gproj_w = mm_tn(pooled[...], gproj).astype(BF16)
    hr = gproj_w.shape[0] // (2 * at.F)
    for i in range(at.F):
        for c in range(2):
            d_proj[c, hr * i : hr * i + hr, :] = gproj_w[hr * (2 * i + c) : hr * (2 * i + c) + hr, :]
    gpool[...] = mm_nt(gproj, proj[...])

    add_halves(2)
    for k in range(T):
        pl.when((at.c == 0) & (at.t + k < T) & (k > 0))(lambda k=k: remote(xin.at[own, pl.ds(lead, tail)], xlast.at[own], (x_send.at[2 * k], x_recv.at[2 * k]), None, {"ctx": 0, "tp": at.tp(k)}).wait_send() if k else None)
        pl.when((at.c == 0) | ((at.t + k < T) & (k > 0)))(lambda k=k: remote(xin.at[own, pl.ds(lead, tail)], xlast.at[own], (x_send.at[2 * k + 1], x_recv.at[2 * k + 1]), None, {"ctx": 1 - at.c}).wait_send())
    for i in range(2):
        for n in range(2):
            wide(n, i).wait_send()
            onward(n, i).wait_send()
        for k in range(4):
            side(k, i).wait_send()
    for i in range(3):
        swap(i).wait_send()
        store(i).wait()

    @pl.loop(0, own)
    def _(j):
        grad_copy(j).wait_send()


def word_section(pooled, proj, words_in, cot, vec, xall, w3, wo, zu, zd):
    blk, width = words_in.shape
    T = lax.axis_size("tp")
    nblk = 2 * T
    cu = zu.shape[1]
    ff = 2 * T * cu
    vm = pl.BlockSpec(memory_space=pltpu.VMEM)
    any_ = pl.BlockSpec(memory_space=pl.ANY)
    out_shapes = [((blk, width), BF16), ((3, blk), F32), ((blk, width), F32), ((blk, pooled.shape[1]), F32), ((2, proj.shape[0] // 2, width), BF16), ((8, width), F32)]
    halves = [((2, width, width), BF16), ((width, ff // 2), BF16), ((ff // 2, width), BF16)]
    bufs = [
        ((nblk, blk, width), BF16), ((nblk, blk, width), BF16), ((nblk, blk, width), BF16), ((nblk, width, blk), BF16), ((nblk, width, blk), BF16),
        ((nblk, HEADS // 2, blk, blk), F32), ((nblk, HEADS, blk, blk), BF16), ((HEADS, blk, 128), BF16), ((HEADS, blk, 128), BF16),
        ((HEADS, 8, blk), F32), ((HEADS, 8, blk), F32), ((width, blk), F32), ((width, blk), F32), ((width, width), BF16), ((width, width), BF16),
        ((3, width, width), BF16), ((width, width), BF16), ((width, ff), BF16), ((ff, width), BF16), ((blk, width), BF16), ((blk, width), BF16), ((HEADS, 8, blk), F32),
        ((width, width), F32), ((width, width), F32), ((nblk, blk, width), BF16), ((blk, width), F32),
        ((2, width, ff // 2), BF16), ((2, ff // 2, width), BF16), ((2, 2, width, width), BF16), ((width, ff // 2), BF16), ((ff // 2, width), BF16), ((2, width, width), BF16),
    ]
    nw = 16
    rows = (CHUNKS[-1][1] - CHUNKS[-1][0]) * (ROWS // 16)
    return pl.pallas_call(
        word_kernel,
        in_specs=[vm] * 5 + [any_] * 5,
        out_specs=[vm] * len(out_shapes) + [any_] * len(halves),
        out_shape=[jax.ShapeDtypeStruct(s, d) for s, d in out_shapes + halves],
        scratch_shapes=[pltpu.VMEM(s, d) for s, d in bufs] + [pltpu.VMEM((nblk, rows, width), BF16)] + [pltpu.SemaphoreType.DMA((n,)) for n in (nw, nw, 3, 3, nblk, nblk, 2 * T, 4 * T, 8)],
        compiler_params=pltpu.CompilerParams(vmem_limit_bytes=VMEM_LIMIT, collective_id=1, has_side_effects=True),
        name="word_section",
    )(pooled, proj, words_in, cot, vec, xall, w3, wo, zu, zd)


class Sum:
    def __init__(self, at, source, bufs, tp_cut, fs_cut, sems, first, wide, halved):
        self.at, self.source, self.sems, self.first, self.wide, self.halved = at, source, sems, first, wide, halved
        self.own, self.away, self.got, self.blocks, self.block, self.pieces, self.done = bufs
        self.hold, self.came = self.away, self.got
        self.near = (at.t + 1 - 2 * lax.rem(at.t, 2), lax.rem(at.t + 2, at.T))
        self.far = at.T - 1 - at.t
        self.fs_base = 5 if halved else at.T - 1
        self.tp_cut, self.fs_cut = tp_cut, fs_cut

    @staticmethod
    def slots(F, T):
        return 6 + (F - 1) + 2 * T

    @staticmethod
    def buffers(half, block, piece, F, T, wide, halved):
        quarter = (block[0] // 2,) + block[1:]
        first = [block, (4,) + quarter, (6,) + quarter, (1, 8, 128)] if halved else [half, half, half, (T - 1,) + block]
        shapes = first + [block, (F - 1,) + piece, ((2, T) if wide else (2,)) + piece]
        return [pltpu.VMEM(sh, BF16) for sh in shapes]

    def swap(self):
        at = self.at
        return remote(self.away, self.got, self.sems, self.first, {"ctx": 1 - at.c})

    def to_tp(self, k):
        src = self.source if self.halved else self.own
        return remote(src.at[self.tp_cut(self.at.tp(k))], self.blocks.at[k - 1], self.sems, self.first + k, {"tp": self.at.tp(k)})

    def to_fs(self, k):
        return remote(self.block.at[self.fs_cut(self.at.fs(k))], self.pieces.at[k - 1], self.sems, self.first + self.fs_base + k, {"fsdp": self.at.fs(k)})

    def share(self, k, x, incoming=False):
        at = self.at
        there = 1 - at.c if x else at.c
        c = there if incoming else at.c
        r = self.done.at[c, at.tp(-k) if incoming else at.t] if self.wide else self.done.at[c]
        return remote(r, r, self.sems, self.first + self.fs_base + at.F + 2 * k + x, {"ctx": there, "tp": at.tp(k)} if k else {"ctx": there})

    def shares(self):
        if not self.wide:
            return [(0, 1)]
        return [(k, x) for k in range(self.at.T) for x in range(2) if k or x]

    def local(self, i):
        src = self.source.at[self.at.c if i == 0 else 1 - self.at.c]
        return pltpu.make_async_copy(src, self.own if i == 0 else self.away, self.loc.at[i])

    def fetch(self, loc):
        self.loc = loc
        for i in range(2):
            self.local(i).start()

    def begin_fetched(self):
        for i in range(2):
            self.local(i).wait()
        self.swap().start()

    def begin(self):
        self.own[...] = self.source[self.at.c].astype(BF16)
        self.away[...] = self.source[1 - self.at.c].astype(BF16)
        self.swap().start()

    def halves(self):
        self.swap().wait_recv()
        self.own[...] = (self.own[...].astype(F32) + self.got[...].astype(F32)).astype(BF16)
        for k in range(1, self.at.T):
            self.to_tp(k).start()

    def part(self, t, i):
        cut = list(self.tp_cut(t))
        n = self.own.shape[0] // 2
        if cut[0] == ALL:
            cut[0] = pl.ds(i * n, n)
        else:
            cut[0] = span(t * 2 * n + i * n, n)
        return self.source.at[tuple(cut)]

    def mine(self, i):
        t, j = ((self.at.t, 0), (self.at.t, 1), (self.near[1], 0), (self.near[0], 1))[i]
        return pltpu.make_async_copy(self.part(t, j), self.hold.at[i], self.loc.at[i])

    def near_send(self, n, far):
        at = self.at
        src = self.part(self.far if far else self.near[n], n)
        return remote(src, self.came.at[2 * n + far], self.sems, self.first + 2 * n + far, {"tp": self.near[n]})

    def onward(self, n):
        return remote(self.hold.at[2 + n], self.came.at[4 + n], self.sems, self.first + 4 + n, {"tp": self.near[1 - n]})

    def begin_halved(self):
        for i in range(4):
            self.mine(i).start()
        for n in range(2):
            for far in (1, 0):
                self.near_send(n, far).start()

    def pass_halved(self):
        for i in range(4):
            self.mine(i).wait()
        for n in range(2):
            self.near_send(n, 1).wait_recv()
            self.hold[2 + n] = (self.hold[2 + n].astype(F32) + self.came[2 * n + 1].astype(F32)).astype(BF16)
        for n in range(2):
            self.onward(n).start()

    def over_near(self):
        n = self.own.shape[0] // 2
        for i in range(2):
            self.near_send(i, 0).wait_recv()
            self.onward(i).wait_recv()
            total = self.hold[i].astype(F32) + self.came[2 * i].astype(F32) + self.came[4 + i].astype(F32)
            self.block[i * n : i * n + n] = total.astype(BF16)
        for k in range(1, self.at.F):
            self.to_fs(k).start()

    def over_tp(self):
        total = self.own[self.tp_cut(self.at.t)].astype(F32)
        for k in range(1, self.at.T):
            self.to_tp(k).wait_recv()
            total += self.blocks[k - 1].astype(F32)
        self.block[...] = total.astype(BF16)
        for k in range(1, self.at.F):
            self.to_fs(k).start()

    def over_fsdp(self):
        at = self.at
        total = self.block[self.fs_cut(at.f)].astype(F32)
        for k in range(1, at.F):
            self.to_fs(k).wait_recv()
            total += self.pieces[k - 1].astype(F32)
        if self.wide:
            self.done[at.c, at.t] = total.astype(BF16)
        else:
            self.done[at.c] = total.astype(BF16)
        for k, x in self.shares():
            self.share(k, x).start()

    def finish(self):
        for k, x in self.shares():
            self.share(k, x, True).wait_recv()

    def drain(self):
        at = self.at
        if self.halved:
            for n in range(2):
                for far in range(2):
                    self.near_send(n, far).wait_send()
                self.onward(n).wait_send()
        else:
            self.swap().wait_send()
            for k in range(1, at.T):
                self.to_tp(k).wait_send()
        for k in range(1, at.F):
            self.to_fs(k).wait_send()
        for k, x in self.shares():
            self.share(k, x).wait_send()


SUMS = [
    ((2, 512, 512), (2, 512, 128), (2, 128, 128), 2, 1, False, True),
    ((512, 1024), (512, 256), (128, 256), 1, 0, False, True),
    ((1024, 512), (256, 512), (256, 128), 0, 1, False, True),
    ((128, 512), (128, 128), (32, 128), 1, 0, True, False),
    ((256, 512), (256, 128), (64, 128), 1, 0, True, False),
    ((128, 1024), (32, 1024), (32, 256), 0, 1, True, False),
    ((256, 512), (256, 128), (64, 128), 1, 0, True, False),
]


def cutter(shape, axis, size):
    def cut(i):
        return tuple(span(i * size, size) if d == axis else ALL for d in range(len(shape)))

    return cut


def reduce_bwd_kernel(tiles, *refs):
    refs = list(refs)
    take = lambda n: [refs.pop(0) for _ in range(n)]
    ins = take(14)
    sources = take(4)
    (d_vec,) = take(1)
    (cg,) = take(1)
    results = take(len(SUMS))
    (vec_out,) = take(1)
    (gca,) = take(1)
    accs = take(len(ACCS))
    at = Place()
    bufs = [take(7) for _ in SUMS]
    vec_in, send, recv, vsend, vrecv, local_sems = refs
    slots = Sum.slots(at.F, at.T)
    a_qo, a_up, a_dn, a_vec = accs
    origin = list(sources) + [a_up, a_dn, a_qo]
    sums = []
    for i, (half, block, piece, ta, fa, wide, halved) in enumerate(SUMS):
        sums.append(Sum(at, origin[i], bufs[i], cutter(half, ta, block[ta]), cutter(block, fa, piece[fa]), (send, recv), i * slots, wide, halved))
        sums[i].loc = local_sems.at[i]
    w4, wup, wdn, pj, up, dn, qo = sums
    step = pl.program_id(0)
    last = 2 * tiles - 1

    def when(i, *acts):
        @pl.when(step == i)
        def _():
            for act in acts:
                act()

    def open_():
        meet(at.peers())
        w4.begin_halved()
        wup.begin_halved()
        pj.begin_fetched()

    when(0, lambda: call(at.peers()), lambda: pj.fetch(pj.loc))
    when(1, open_)
    when(3, pj.halves)
    when(6, w4.pass_halved, wup.pass_halved, wdn.begin_halved)
    when(8, up.begin, dn.begin, pj.over_tp)
    when(11, w4.over_near, wup.over_near, wdn.pass_halved, up.halves, dn.halves, pj.over_fsdp)
    when(15, wdn.over_near, up.over_tp, dn.over_tp)
    def vec_copy(i, where):
        return remote(a_vec, vec_in.at[i], (vsend, vrecv), i, where)

    def vec_begin():
        a_vec[3:5, :] = d_vec[0:2, :]
        vec_copy(0, {"ctx": 1 - at.c}).start()

    def vec_plane():
        vec_copy(0, {"ctx": 1 - at.c}).wait()
        a_vec[...] += vec_in[0]
        for k in range(1, at.T):
            vec_copy(k, {"tp": at.tp(k)}).start()

    def vec_depth():
        for k in range(1, at.T):
            vec_copy(k, {"tp": at.tp(k)}).wait()
        a_vec[...] += vec_in[1] + vec_in[2] + vec_in[3]
        for k in range(1, at.F):
            vec_copy(at.T - 1 + k, {"fsdp": at.fs(k)}).start()

    def vec_end():
        for k in range(1, at.F):
            vec_copy(at.T - 1 + k, {"fsdp": at.fs(k)}).wait()
        total = a_vec[...] + (vec_in[4] + vec_in[5] + vec_in[6])
        rows = [jnp.zeros((2, 128), F32)]
        for i, n in ((2, 64), (3, 128), (4, 128)):
            v = jnp.zeros((1, n), F32)
            for f in range(at.F):
                v = jnp.where(at.f == f, total[i : i + 1, f * n : f * n + n], v)
            rows.append(v if n == 128 else jnp.concatenate([v, jnp.zeros((1, n), F32)], axis=1))
        vec_out[...] = jnp.concatenate(rows + [jnp.zeros((3, 128), F32)], axis=0)

    when(8, vec_begin)
    when(10, vec_plane)
    when(12, vec_depth)
    when(14, vec_end)
    char_back_step(step, tiles, ins, cg, gca, accs, False)

    @pl.when(step == last)
    def _():
        qo.begin()
        w4.over_fsdp()
        wup.over_fsdp()
        qo.halves()

        def keep(*which):
            for i in which:
                sums[i].finish()
                results[i][...] = sums[i].done[...]

        keep(0, 1, 3)
        qo.over_tp()
        up.over_fsdp()
        dn.over_fsdp()
        wdn.over_fsdp()
        qo.over_fsdp()
        keep(4, 5, 2)
        for s in sums[:6]:
            s.drain()
        keep(6)
        qo.drain()


def reduce_backward(x, cnt, saved, gpool, weights, sources, d_vec):
    total = x.shape[0]
    tiles = total // ROWS
    F, T = lax.axis_size("fsdp"), lax.axis_size("tp")
    ins, out = back_specs(tiles, gpool, weights)
    any_ = pl.BlockSpec(memory_space=pl.ANY)
    scratch = [pltpu.VMEM((total, 256), F32)] + [pltpu.VMEM(s, F32) for s in ACCS]
    results = []
    for half, block, piece, _, _, wide, halved in SUMS:
        scratch += Sum.buffers(half, block, piece, F, T, wide, halved)
        results.append(((2, T) if wide else (2,)) + piece)
    count = len(SUMS) * Sum.slots(F, T)
    vecs = 1 + (T - 1) + (F - 1)
    scratch += [pltpu.VMEM((vecs, 8, 512), F32)]
    scratch += [pltpu.SemaphoreType.DMA((n,)) for n in (count, count, vecs, vecs)] + [pltpu.SemaphoreType.DMA((len(SUMS), 4))]
    return pl.pallas_call(
        functools.partial(reduce_bwd_kernel, tiles),
        grid=(2 * tiles,),
        in_specs=ins + [any_] * len(sources) + [full_spec((8, 512))],
        out_specs=[out] + [full_spec(s) for s in results] + [full_spec((8, 128))],
        out_shape=[jax.ShapeDtypeStruct((total, 256), F32)] + [jax.ShapeDtypeStruct(s, BF16) for s in results] + [jax.ShapeDtypeStruct((8, 128), F32)],
        scratch_shapes=scratch,
        compiler_params=pltpu.CompilerParams(vmem_limit_bytes=VMEM_LIMIT, collective_id=2, has_side_effects=True, dimension_semantics=("arbitrary",)),
        name="reduce_backward",
    )(x, cnt, *saved, gpool, *weights, *sources, d_vec)


FINAL = [(3, 128, 128), (128, 128), (128, 512), (512, 128), (64, 512), (64, 1024), (256, 256), (64, 768), (64, 256), (1, 64), (1, 64), (1, 64), (1, 128), (1, 128)]


def final_kernel(cg, block, grad, rms, w4, wup, wdn, pj, up, dn, qo, vec, w_qkv, w_up, g1, g2, cg_out, block_out, grad_out, rms_out, *outs):
    cg_out[...] = cg[...]

    @pl.when(pl.program_id(0) == 0)
    def _():
        block_out[...] = block[...]
        grad_out[...] = grad[...]
        rms_out[...] = rms[...]
        o3, o_out, o_wup, o_wdn, o_pj, o_up, o_dn, o_qkv, o_cout = outs[:9]
        o3[0] = w4[0, 0].astype(F32)
        o3[1] = w4[0, 1].astype(F32)
        o3[2] = w4[1, 0].astype(F32)
        o_out[...] = jnp.transpose(w4[1, 1].astype(F32))
        for c in range(2):
            o_wup[:, 256 * c : 256 * c + 256] = wup[c].astype(F32)
            o_wdn[256 * c : 256 * c + 256, :] = wdn[c].astype(F32)
            for t in range(pj.shape[1]):
                i = 2 * t + c
                o_pj[32 * c : 32 * c + 32, 128 * t : 128 * t + 128] = pj[c, t].astype(F32)
                o_up[:, 128 * i : 128 * i + 128] = up[c, t].astype(F32)
                ref, i = (o_qkv, i) if i < 6 else (o_cout, i - 6)
                ref[:, 128 * i : 128 * i + 128] = qo[c, t].astype(F32)
        o_dn[...] = jnp.transpose(dn[...].astype(F32).reshape(256, 256))
        for i, n in enumerate((64, 64, 64, 128, 128)):
            if i > 1:
                outs[9 + i][...] = vec[i : i + 1, :n]
        for i, (w, d, gain) in enumerate(((w_qkv, o_qkv, g1), (w_up, o_up, g2))):
            col = jnp.sum(w[...].astype(F32) * d[...], axis=-1, keepdims=True)
            row = jnp.transpose(jnp.broadcast_to(col, (64, 128)))[0:1, :]
            outs[9 + i][...] = row / gain[...].astype(F32)


def finish(cg, block, grad, rms, parts):
    tiles = 4
    rows = cg.shape[0] // tiles
    small = [block, grad, rms] + list(parts)
    return pl.pallas_call(
        final_kernel,
        grid=(tiles,),
        in_specs=[rows_spec(rows, cg.shape[1])] + [full_spec(v.shape) for v in small],
        out_specs=[rows_spec(rows, cg.shape[1])] + [full_spec(v.shape) for v in small[:3]] + [full_spec(v) for v in FINAL],
        out_shape=[jax.ShapeDtypeStruct(v.shape, v.dtype) for v in [cg] + small[:3]] + [jax.ShapeDtypeStruct(v, F32) for v in FINAL],
        compiler_params=pltpu.CompilerParams(vmem_limit_bytes=VMEM_LIMIT, dimension_semantics=("arbitrary",)),
        name="finish",
    )(cg, block, grad, rms, *parts)


def gather(x, name, axis):
    return lax.all_gather(x, name, axis=axis, tiled=True)


def scatter(x, name, axis):
    return lax.psum_scatter(x, name, scatter_dimension=axis, tiled=True)


def fits(rows):
    return lax.axis_size("fsdp") == 4 and lax.axis_size("tp") == 4 and rows == 64


def local(characters, counts, words_in, cotangent, char_prenorm, char_qkv, char_out, char_midnorm, char_up, char_down,
          pool_query, char_proj, word_prenorm, word_qkv, word_out, word_midnorm, word_up, word_down):
    words, slots, cdim = characters.shape
    x = characters.reshape(words * slots, cdim)
    vectors_in = (char_prenorm, char_midnorm, pool_query, word_prenorm, word_midnorm)
    w3 = jnp.moveaxis(word_qkv, 1, 0)
    direct = fits(char_prenorm.shape[0])
    group_rows = (words * slots // ROWS, ROWS // GROUP, GROUP)
    if direct:
        shards = [char_qkv, char_out, char_up, char_down, char_proj, w3, word_out, word_up, word_down]
        *saved, pooled_low, qo, up, dn, proj, _, w3, wo, zu, zd, vec, cnt, xall = gather_forward(x, counts.reshape(words // 128, 128), words_in, [v.reshape(1, -1) for v in vectors_in], shards)
        dn = dn.reshape(1024, 256)
        cnt = cnt.reshape(group_rows)
    else:
        cnt = jnp.repeat(counts.astype(F32), slots).reshape(group_rows)
        wide = [gather(v.astype(F32), "fsdp", 0) for v in vectors_in]
        vec = jnp.stack([jnp.pad(v, (0, 512 - v.shape[0])) for v in wide] + [jnp.zeros((512,), F32)] * 3)
        qo = jnp.concatenate([gather(char_qkv, "fsdp", 0), gather(char_out, "fsdp", 0)], axis=1)
        up, dn, proj = (gather(w, "fsdp", 0) for w in (char_up, char_down, char_proj))
        w3 = gather(gather(w3, "fsdp", 1), "tp", 2)
        wo = gather(gather(word_out, "fsdp", 1), "tp", 0)
        cu = word_up.shape[1] // 2
        zu = lax.dynamic_slice_in_dim(gather(word_up, "fsdp", 0), lax.axis_index("ctx") * cu, cu, 1)
        zd = lax.dynamic_slice_in_dim(gather(word_down, "fsdp", 1), lax.axis_index("ctx") * cu, cu, 0)
        *saved, pooled_low = char_forward(x, cnt, vec, qo, up, dn)
        start, _ = ln_parts(words_in.astype(F32) + mm(pooled_low, proj))
        xall = gather((start * vec[3:4]).astype(BF16), ("ctx", "tp"), 0).reshape(-1, words, words_in.shape[1])
    (block_out, rms, words_grad, gpool, d_proj, d_vec, h_w4, h_up, h_down) = word_section(pooled_low, proj, words_in, cotangent, vec, xall, w3, wo, zu, zd)
    if direct:
        cg, *parts = reduce_backward(x, cnt, saved, gpool, [vec, qo, up, dn], [h_w4, h_up, h_down, d_proj], d_vec)
        cg, block_out, words_grad, rms, g_qkv4, g_wout, g_wup, g_wdown, g_proj, g_up, g_down, g_qkv, g_out, *vecs = finish(cg, block_out, words_grad, rms, parts + [char_qkv, char_up, char_prenorm.reshape(1, -1), char_midnorm.reshape(1, -1)])
        vecs = [v.reshape(-1) for v in vecs]
    else:
        cg, a_qo, a_up, a_dn, a_vec = char_backward(x, cnt, saved, gpool, vec, qo, up, dn)

        def reduce_char(g):
            g = lax.psum(g.astype(BF16), ("ctx", "tp"))
            return scatter(g, "fsdp", 0).astype(F32)

        def reduce_word(g, tp_axis, fsdp_axis, ctx_axis):
            g = scatter(scatter(g, "tp", tp_axis), "fsdp", fsdp_axis)
            return gather(g, "ctx", ctx_axis).astype(F32)

        lanes = lambda g, n: jnp.moveaxis(g.reshape(2, g.shape[1], -1, n), 0, 2).reshape(g.shape[1], -1)
        hr = char_proj.shape[0] // 2
        g_qo = reduce_char(lanes(a_qo, 128))
        g_qkv, g_out = g_qo[:, :768], g_qo[:, 768:]
        g_up = reduce_char(lanes(a_up, 128))
        g_down = reduce_char(a_dn.reshape(256, 1024).T)
        g_proj = reduce_char(jnp.moveaxis(d_proj.reshape(2, -1, hr, 512), 0, 1).reshape(256, 512))
        g_w4 = reduce_word(h_w4, 2, 1, 0)
        g_qkv4, g_wout = g_w4[:3], g_w4[3].T
        g_wup = reduce_word(h_up, 1, 0, 1)
        g_wdown = reduce_word(h_down, 0, 1, 0)
        vecs = [reduce_char(v) for v in (a_vec[0, :256], a_vec[1, :256], a_vec[2, :256], d_vec[0], d_vec[1])]
    return (
        block_out,
        cg.reshape(words, slots, cdim),
        words_grad,
        rms,
        vecs[0],
        g_qkv,
        g_out,
        vecs[1],
        g_up,
        g_down,
        vecs[2],
        g_proj,
        vecs[3],
        jnp.moveaxis(g_qkv4, 0, 1),
        g_wout,
        vecs[4],
        g_wup,
        g_wdown,
    )


def solution(mesh):
    rows = ("fsdp", "ctx", "tp")
    v, m = P("fsdp"), P("fsdp", None)
    return jax.shard_map(
        local,
        mesh=mesh,
        in_specs=(
            P(rows, None, None), P(rows), P(rows, None), P(rows, None),
            v, m, m, v, m, m, v, m, v, P("fsdp", None, "tp"), P("tp", "fsdp"), v, P("fsdp", "tp"), P("tp", "fsdp"),
        ),
        out_specs=(
            P(rows, None), P(rows, None, None), P(rows, None), P(None, rows),
            v, m, m, v, m, m, v, m, v, P("fsdp", None, "tp"), P("tp", "fsdp"), v, P("fsdp", "tp"), P("tp", "fsdp"),
        ),
        check_vma=False,
    )
```

```python
import functools

import jax
import jax.numpy as jnp
from jax import lax
from jax.experimental import pallas as pl
from jax.experimental.pallas import tpu as pltpu
from jax.sharding import PartitionSpec as P

CHEADS = 4
HEADS = 8
HEAD = 64
EPSILON = 1e-05
MASKED = -1e30
CGELU = 0.7978845608028654
AGELU = 0.044715
ROWS = 512
GROUP = 128
F32 = jnp.float32
BF16 = jnp.bfloat16
VMEM_LIMIT = 66_000_000


def mm(a, b):
    return lax.dot_general(a, b, (((1,), (0,)), ((), ())), preferred_element_type=F32)


def mm_nt(a, b):
    return lax.dot_general(a, b, (((1,), (1,)), ((), ())), preferred_element_type=F32)


def mm_tn(a, b):
    return lax.dot_general(a, b, (((0,), (0,)), ((), ())), preferred_element_type=F32)


def ln_parts(x):
    c = x - jnp.mean(x, axis=-1, keepdims=True)
    r = lax.rsqrt(jnp.mean(c * c, axis=-1, keepdims=True) + EPSILON)
    return c * r, r


def ln_back(xhat, r, gain, g):
    gg = g * gain
    a = jnp.mean(gg, axis=-1, keepdims=True)
    b = jnp.mean(gg * xhat, axis=-1, keepdims=True)
    return r * (gg - a - xhat * b)


def gelu_both(x):
    x2 = x * x
    y = (CGELU * AGELU) * x2 + CGELU
    hp = 0.5 * jnp.tanh(x * y) + 0.5
    g = x * hp
    d = hp + (g - g * hp) * (6.0 * y - 4.0 * CGELU)
    return g, d


def pair_masks(rows):
    lane = lax.broadcasted_iota(jnp.int32, (rows, 128), 1)
    return lane < HEAD


def split_heads(x, low_lanes):
    zero = jnp.zeros_like(x)
    return jnp.where(low_lanes, x, zero), jnp.where(low_lanes, zero, x)


def stack_heads(x, low_lanes):
    a, b = split_heads(x, low_lanes)
    return jnp.concatenate([a, b], axis=0)


def word_of_lane(width):
    return (lax.broadcasted_iota(jnp.int32, (16, width), 1) % GROUP) // 16


def compress(blocks, lane_word):
    out = blocks[0:16, :]
    for w in range(1, GROUP // 16):
        out = jnp.where(lane_word == w, blocks[16 * w : 16 * w + 16, :], out)
    return out


def expand(dense, lane_word):
    zero = jnp.zeros_like(dense)
    return jnp.concatenate(
        [jnp.where(lane_word == w, dense, zero) for w in range(GROUP // 16)], axis=0
    )


def pool_weights(am, q_row, cnt_col):
    words = am.shape[0] // 16
    am3 = am.reshape(words, 16, am.shape[1])
    logits = jnp.sum(am * q_row, axis=-1, keepdims=True)
    slot = (lax.broadcasted_iota(jnp.int32, (am.shape[0], 1), 0) % 16).astype(F32)
    logits = jnp.where(slot < cnt_col, logits, MASKED).reshape(words, 16, 1)
    e = jnp.exp(logits - jnp.max(logits, axis=1, keepdims=True))
    w = e / jnp.sum(e, axis=1, keepdims=True)
    return am3, w


def count_column(cnt_row):
    return jnp.transpose(jnp.broadcast_to(cnt_row, (GROUP, GROUP)))[:, 0:1]


def char_attn_tile(x, cnt, weights):
    g1, wqkv, wout = weights[:3]
    groups = x.shape[0] // GROUP
    xf = x.astype(F32)
    xhat, _ = ln_parts(xf)
    normed = (xhat * g1).astype(BF16)
    packed = mm(normed, wqkv).astype(BF16)
    low = pair_masks(GROUP)
    lw = word_of_lane(2 * GROUP)
    slot = lax.broadcasted_iota(jnp.int32, (16, 2 * GROUP), 0).astype(F32)
    raw, values, scores = [], [], []
    for g in range(groups):
        r = slice(g * GROUP, (g + 1) * GROUP)
        for p in range(CHEADS // 2):
            q = packed[r, 128 * p : 128 * p + 128] * BF16(0.125)
            values.append(packed[r, 512 + 128 * p : 640 + 128 * p])
            raw.append(mm_nt(packed[r, 256 + 128 * p : 384 + 128 * p], stack_heads(q, low)))
    pairs = len(raw)
    for i, st in enumerate(raw):
        cnt_row = cnt[i // 2 : i // 2 + 1, :]
        scores.append(jnp.where(slot < jnp.concatenate([cnt_row, cnt_row], axis=1), compress(st, lw), MASKED))
    scores = jnp.concatenate(scores, axis=0).reshape(pairs, 16, 2 * GROUP)
    e = jnp.exp(scores - jnp.max(scores, axis=1, keepdims=True))
    probs = e / jnp.sum(e, axis=1, keepdims=True)
    low_probs = probs.astype(BF16)
    spread = [expand(low_probs[i], lw) for i in range(pairs)]
    mixed = [mm_tn(pt, v) for pt, v in zip(spread, values)]
    mixed = [jnp.where(low, o[:GROUP], o[GROUP:]) for o in mixed]
    probs = jnp.concatenate([jnp.concatenate([probs[2 * g], probs[2 * g + 1]], axis=1) for g in range(groups)], axis=0)
    mixed = jnp.concatenate([jnp.concatenate(mixed[2 * g : 2 * g + 2], axis=1) for g in range(groups)], axis=0).astype(BF16)
    return packed, probs, mixed, xf + mm(mixed, wout)


def char_mlp_tile(aa, cnt, weights):
    _, _, _, g2, wup, wdown, pq = weights
    ahat, _ = ln_parts(aa)
    middle = (ahat * g2).astype(BF16)
    upper, dgelu = gelu_both(mm(middle, wup))
    upper = upper.astype(BF16)
    am = aa + mm(upper, wdown)
    cols = jnp.concatenate([count_column(cnt[g : g + 1, :]) for g in range(aa.shape[0] // GROUP)], axis=0)
    am3, w = pool_weights(am, pq, cols)
    pooled = jnp.sum(w * am3, axis=1)
    return upper, dgelu.astype(BF16), am, pooled.astype(BF16)


def count_lanes(counts):
    take = GROUP // 16
    w = lax.broadcasted_iota(jnp.int32, (128, GROUP), 0)
    l = lax.broadcasted_iota(jnp.int32, (128, GROUP), 1)
    spread = (lax.rem(w, take) == l // 16).astype(BF16)
    g = lax.broadcasted_iota(jnp.int32, (128 // take, 128), 0)
    lane = lax.broadcasted_iota(jnp.int32, (128 // take, 128), 1)
    rows = []
    for r in range(counts.shape[0]):
        one = jnp.where(lane // take == g, counts[r : r + 1, :].astype(F32), 0.0).astype(BF16)
        rows.append(mm(one, spread))
    return jnp.concatenate(rows, axis=0)


def full_spec(shape):
    return pl.BlockSpec(shape, lambda i: (0,) * len(shape))


def rows_spec(rows, width):
    return pl.BlockSpec((rows, width), lambda i: (i, 0))


def char_mlp_back(cnt, aa, upper, dgelu, am, gpool_ref, base, weights):
    _, _, _, g2, wup, wdown, pq = weights
    rows = aa.shape[0]
    words = rows // 16
    cols = jnp.concatenate([count_column(cnt[g : g + 1, :]) for g in range(rows // GROUP)], axis=0)
    _, w = pool_weights(am, pq, cols)
    gp = jnp.concatenate(
        [jnp.broadcast_to(gpool_ref[pl.ds(base + i, 1), :], (16, 256)) for i in range(words)], axis=0
    )
    dw = jnp.sum(gp * am, axis=-1, keepdims=True).reshape(words, 16, 1)
    dlog = (w * (dw - jnp.sum(w * dw, axis=1, keepdims=True))).reshape(rows, 1)
    gm = w.reshape(rows, 1) * gp + dlog * pq
    d_pq = jnp.sum(dlog * am, axis=0, keepdims=True)
    gdl = gm.astype(BF16)
    d_down_t = mm_tn(gdl, upper)
    ghid = (dgelu.astype(F32) * mm_nt(gdl, wdown)).astype(BF16)
    ahat, ar = ln_parts(aa)
    middle = (ahat * g2).astype(BF16)
    d_up = mm_tn(middle, ghid)
    gmid = mm_nt(ghid, wup)
    gca = gm + ln_back(ahat, ar, g2, gmid)
    d_g2 = jnp.sum(gmid * ahat, axis=0, keepdims=True)
    return gca, d_up, d_down_t, d_g2, d_pq


def char_attn_back(x, packed, probs, mixed, gca, weights):
    g1, wqkv, wout = weights[:3]
    groups = x.shape[0] // GROUP
    low = pair_masks(GROUP)
    lw = word_of_lane(2 * GROUP)
    gcl = gca.astype(BF16)
    d_out = mm_tn(mixed, gcl)
    gcm = mm_nt(gcl, wout).astype(BF16)
    keys, queries, grads, raw, prs = [], [], [], [], []
    for g in range(groups):
        r = slice(g * GROUP, (g + 1) * GROUP)
        for p in range(CHEADS // 2):
            queries.append(stack_heads(packed[r, 128 * p : 128 * p + 128] * BF16(0.125), low))
            keys.append(packed[r, 256 + 128 * p : 384 + 128 * p])
            grads.append(stack_heads(gcm[r, 128 * p : 128 * p + 128], low))
            raw.append(mm_nt(packed[r, 512 + 128 * p : 640 + 128 * p], grads[-1]))
            prs.append(probs[16 * g : 16 * g + 16, 256 * p : 256 * p + 256])
    pairs = len(raw)
    dp = jnp.concatenate([compress(v, lw) for v in raw], axis=0).reshape(pairs, 16, 2 * GROUP)
    pr = jnp.concatenate(prs, axis=0).reshape(pairs, 16, 2 * GROUP)
    ds = (pr * (dp - jnp.sum(pr * dp, axis=1, keepdims=True))).astype(BF16)
    pr = pr.astype(BF16)
    dst = [expand(ds[i], lw) for i in range(pairs)]
    pt = [expand(pr[i], lw) for i in range(pairs)]
    dq = [mm_tn(dst[i], keys[i]) for i in range(pairs)]
    dq = [jnp.where(low, o[:GROUP], o[GROUP:]) * 0.125 for o in dq]
    dk = [mm(dst[i], queries[i]) for i in range(pairs)]
    dv = [mm(pt[i], grads[i]) for i in range(pairs)]
    dqkv = [jnp.concatenate([v[2 * g + p] for v in (dq, dk, dv) for p in range(2)], axis=1) for g in range(groups)]
    dqkv = jnp.concatenate(dqkv, axis=0).astype(BF16)
    xhat, xr = ln_parts(x.astype(F32))
    normed = (xhat * g1).astype(BF16)
    gn = mm_nt(dqkv, wqkv)
    grad = gca + ln_back(xhat, xr, g1, gn)
    return grad, mm_tn(normed, dqkv), d_out, gn * xhat


def char_back_step(step, tiles, ins, cg, gca, accs, gains):
    x, cnt, packed, probs, mixed, aa, upper, dgelu, am, gpool, vec, qo, up, dn = ins
    a_qo, a_up, a_dn, a_vec = accs
    weights = char_weights(vec, qo, up, dn)

    @pl.when(step == 0)
    def _():
        for acc in accs:
            acc[...] = jnp.zeros_like(acc)

    @pl.when(step < tiles)
    def _():
        grad, d_up, d_dn, d_g2, d_pq = char_mlp_back(cnt[0], aa[...], upper[...], dgelu[...], am[...], gpool, step * (ROWS // 16), weights)
        gca[span(step * ROWS, ROWS), :] = grad
        if gains:
            a_vec[1:2, :256] += d_g2
        a_vec[2:3, :256] += d_pq
        for i in range(8):
            t, c = i // 2, i % 2
            a_up[c, :, 128 * t : 128 * t + 128] += d_up[:, 128 * i : 128 * i + 128]
        for c in range(2):
            a_dn[c] += d_dn[128 * c : 128 * c + 128, :]

    @pl.when(step >= tiles)
    def _():
        r = span((step - tiles) * ROWS, ROWS)
        grad, d_qkv, d_out, terms = char_attn_back(x[...], packed[...], probs[...], mixed[...], gca[r, :], weights)
        cg[...] = grad
        if gains:
            a_vec[0:1, :256] += jnp.sum(terms, axis=0, keepdims=True)
        for i in range(8):
            t, c = i // 2, i % 2
            val = d_qkv[:, 128 * i : 128 * i + 128] if i < 6 else d_out[:, 128 * (i - 6) : 128 * (i - 6) + 128]
            a_qo[c, :, 128 * t : 128 * t + 128] += val


ACCS = [(2, 256, 512), (2, 256, 512), (2, 128, 1024), (8, 512)]


def back_specs(tiles, gpool, weights):
    one = lambda i: jnp.minimum(i, tiles - 1)
    two = lambda i: jnp.maximum(i - tiles, 0)

    def rows_at(where, r, w):
        return pl.BlockSpec((r, w), lambda i: (where(i), 0))

    once = lambda sh: pl.BlockSpec(sh, lambda i: (0,) * len(sh), pipeline_mode=pl.Buffered(1))
    ins = [rows_at(two, ROWS, 256), pl.BlockSpec((1, ROWS // GROUP, GROUP), lambda i: (one(i), 0, 0))]
    ins += [rows_at(two, ROWS, 768), rows_at(two, ROWS // 8, 512), rows_at(two, ROWS, 256)]
    ins += [rows_at(one, ROWS, 256), rows_at(one, ROWS, 1024), rows_at(one, ROWS, 1024), rows_at(one, ROWS, 256)]
    ins += [once(gpool.shape)] + [once(w.shape) for w in weights]
    return ins, rows_at(two, ROWS, 256)


def char_bwd_kernel(tiles, *refs):
    ins, (cg, *accs), gca = refs[:14], refs[14:19], refs[19]
    char_back_step(pl.program_id(0), tiles, ins, cg, gca, accs, True)


def char_backward(x, cnt, saved, gpool, *weights):
    total = x.shape[0]
    tiles = total // ROWS
    ins, out = back_specs(tiles, gpool, weights)
    return pl.pallas_call(
        functools.partial(char_bwd_kernel, tiles),
        grid=(2 * tiles,),
        in_specs=ins,
        out_specs=[out] + [full_spec(s) for s in ACCS],
        out_shape=[jax.ShapeDtypeStruct((total, 256), F32)] + [jax.ShapeDtypeStruct(s, F32) for s in ACCS],
        scratch_shapes=[pltpu.VMEM((total, 256), F32)],
        compiler_params=pltpu.CompilerParams(vmem_limit_bytes=VMEM_LIMIT, dimension_semantics=("arbitrary",)),
        name="char_backward",
    )(x, cnt, *saved, gpool, *weights)


MESH = pl.DeviceIdType.MESH


def remote(src, dst, sems, index, where):
    return pltpu.make_async_remote_copy(
        src_ref=src, dst_ref=dst,
        send_sem=sems[0] if index is None else sems[0].at[index],
        recv_sem=sems[1] if index is None else sems[1].at[index],
        device_id=where, device_id_type=MESH,
    )


def span(start, size):
    return pl.ds(pl.multiple_of(start, size), size)


class Place:
    def __init__(self):
        self.f, self.c, self.t = lax.axis_index("fsdp"), lax.axis_index("ctx"), lax.axis_index("tp")
        self.F, self.T = lax.axis_size("fsdp"), lax.axis_size("tp")

    def fs(self, k):
        return lax.rem(self.f + k + self.F, self.F)

    def tp(self, k):
        return lax.rem(self.t + k + self.T, self.T)

    def peers(self):
        out = [{"fsdp": self.fs(k)} for k in range(1, self.F)]
        out += [{"tp": self.tp(k)} for k in range(1, self.T)]
        out += [{"ctx": 1 - self.c, "tp": self.tp(k)} for k in range(1, self.T)]
        return out + [{"ctx": 1 - self.c}]


def call(peers):
    for where in peers:
        pl.semaphore_signal(pltpu.get_barrier_semaphore(), inc=1, device_id=where, device_id_type=MESH)


def meet(peers):
    pl.semaphore_wait(pltpu.get_barrier_semaphore(), len(peers))


def greet(peers):
    call(peers)
    meet(peers)


class Piece:
    def __init__(self, at, shard, whole, mine, landing, region, sems, local_sem, first, side=True, core=None, source=None):
        self.at, self.shard, self.whole = at, shard, whole
        self.mine, self.landing, self.region = mine, landing, region
        self.sems, self.local_sem, self.first = sems, local_sem, first
        self.cores, self.core, self.source = side, core, source

    @staticmethod
    def slots(F, T):
        return (F - 1) + (T - 1) + T

    def held(self, act, other=False):
        if self.core is None:
            act()
        else:
            pl.when(self.at.c == (1 - self.core if other else self.core))(act)

    def local(self, src):
        at = self.at
        return pltpu.make_async_copy(src, self.whole.at[self.landing(at.f, at.c, at.t)], self.local_sem)

    def z(self, k, src=None):
        at = self.at
        f = at.fs(-k) if src is None else at.f
        dst = self.whole.at[self.landing(f, at.c, at.t)]
        return remote(dst if src is None else src, dst, self.sems, self.first + k - 1, {"fsdp": at.fs(k)})

    def plane(self, k, incoming=False):
        at = self.at
        r = self.whole.at[self.region(at.c, at.tp(-k) if incoming else at.t)]
        return remote(r, r, self.sems, self.first + at.F - 1 + k - 1, {"tp": at.tp(k)})

    def side(self, k, incoming=False):
        at = self.at
        c = at.c if self.core is not None else (1 - at.c if incoming else at.c)
        r = self.whole.at[self.region(c, at.tp(-k))]
        return remote(r, r, self.sems, self.first + at.F + at.T - 2 + k, {"ctx": 1 - at.c})

    def begin(self):
        at = self.at

        def go(src):
            self.local(src).start()
            for k in range(1, at.F):
                self.z(k, src).start()

        if self.source is not None:
            for cond, src in self.source:
                pl.when(cond)(functools.partial(go, src))
        else:
            self.held(lambda: go(self.shard.at[self.mine(at.c, at.t)]))

    def landed(self):
        at = self.at
        dst = self.whole.at[self.landing(at.f, at.c, at.t)]
        pltpu.make_async_copy(dst, dst, self.local_sem).wait()
        for k in range(1, at.F):
            self.z(k).wait_recv()

    def spread(self):
        def go():
            self.landed()
            if self.region is not None:
                for k in range(1, self.at.T):
                    self.plane(k).start()
                if self.cores:
                    self.side(0).start()

        self.held(go)

    def pass_on(self):
        def go():
            for k in range(1, self.at.T):
                self.plane(k, True).wait_recv()
                if self.cores:
                    self.side(k).start()

        if self.region is not None:
            self.held(go)

    def arrive(self):
        def go():
            for k in range(self.at.T):
                self.side(k, True).wait_recv()

        if self.region is not None and self.cores:
            self.held(go, True)

    def drain(self):
        def go():
            for k in range(1, self.at.F):
                self.z(k).wait_send()
            if self.region is not None:
                for k in range(1, self.at.T):
                    self.plane(k).wait_send()
                if self.cores:
                    for k in range(self.at.T):
                        self.side(k).wait_send()

        self.held(go)


ALL = slice(None)
GATHERED = [((256, 1024), BF16), ((256, 1024), BF16), ((4, 256, 256), BF16), ((256, 512), BF16), ((4, 8, 128), F32), ((3, 512, 512), BF16), ((512, 512), BF16), ((512, 256), BF16), ((256, 512), BF16)]


def gather_pieces(at, shards, wholes, sems, local_sems):
    F, T = at.F, at.T
    qkv, out, up, dn, pj, sm, w3, wo, wu, wd = shards
    rq, rd, rw = up.shape[0], dn.shape[0], w3.shape[1]
    cu = wu.shape[1] // 2
    lanes = lambda c, t: span(256 * t + 128 * c, 128)
    cols = (lambda c, t: (ALL, lanes(c, t)), lambda f, c, t: (span(f * rq, rq), lanes(c, t)), lambda c, t: (ALL, lanes(c, t)))
    n = qkv.shape[1] // 256
    inside = lax.rem(at.t, n)
    qo_source = [(at.t < n, qkv.at[:, span(256 * inside + 128 * at.c, 128)]), (at.t == n, out.at[:, span(128 * at.c, 128)])]
    quarter = rd // T
    slots = Piece.slots(F, T)
    specs = [
        (None, wholes[0], *cols, dict(source=qo_source)),
        (up, wholes[1], *cols, {}),
        (dn, wholes[2], lambda c, t: (span(quarter * t, quarter), span(128 * c, 128)), lambda f, c, t: (f, span(quarter * t, quarter), span(128 * c, 128)), lambda c, t: (ALL, span(quarter * t, quarter), span(128 * c, 128)), {}),
        (pj, wholes[3], lambda c, t: (ALL, span(128 * t, 128)), lambda f, c, t: (span(f * rq, rq), span(128 * t, 128)), lambda c, t: (ALL, span(128 * t, 128)), dict(side=False)),
        (sm, wholes[4], lambda c, t: (ALL, ALL), lambda f, c, t: (f,), None, dict(side=False)),
        (w3, wholes[5], lambda c, t: (span(0, 2),), lambda f, c, t: (span(0, 2), span(f * rw, rw), span(128 * t, 128)), lambda c, t: (span(0, 2), ALL, span(128 * t, 128)), dict(core=0)),
        (w3, wholes[5], lambda c, t: (pl.ds(2, 1),), lambda f, c, t: (pl.ds(2, 1), span(f * rw, rw), span(128 * t, 128)), lambda c, t: (pl.ds(2, 1), ALL, span(128 * t, 128)), dict(core=1)),
        (wo, wholes[6], lambda c, t: (ALL, ALL), lambda f, c, t: (span(t * rw, rw), span(128 * f, 128)), lambda c, t: (span(t * rw, rw), ALL), dict(core=1)),
        (wu, wholes[7], lambda c, t: (ALL, span(cu * c, cu)), lambda f, c, t: (span(f * rw, rw), ALL), None, {}),
        (wd, wholes[8], lambda c, t: (span(cu * c, cu), ALL), lambda f, c, t: (ALL, span(f * rw, rw)), None, {}),
    ]
    return [
        Piece(at, shard, whole, mine, landing, region, sems, local_sems.at[i], i * slots, **more)
        for i, (shard, whole, mine, landing, region, more) in enumerate(specs)
    ]


PIECES = 10


FWD_OUTS = [(ROWS, 768, BF16), (ROWS // 8, 512, F32), (ROWS, 256, BF16), (ROWS, 256, F32), (ROWS, 1024, BF16), (ROWS, 1024, BF16), (ROWS, 256, F32), (ROWS // 16, 256, BF16)]


def char_weights(vec, qo, up, dn):
    return (vec[0:1, :256], qo[:, :768], qo[:, 768:], vec[1:2, :256], up[...], dn[...], vec[2:3, :256])


def char_fwd_kernel(x, cnt, vec, qo, up, dn, *outs):
    w = char_weights(vec, qo, up, dn)
    first = char_attn_tile(x[...], cnt[0], w)
    for ref, val in zip(outs, first + char_mlp_tile(first[3], cnt[0], w)):
        ref[...] = val


def char_forward(x, cnt, *weights):
    tiles = x.shape[0] // ROWS
    return pl.pallas_call(
        char_fwd_kernel,
        grid=(tiles,),
        in_specs=[rows_spec(ROWS, 256), pl.BlockSpec((1, ROWS // GROUP, GROUP), lambda i: (i, 0, 0))] + [full_spec(w.shape) for w in weights],
        out_specs=[rows_spec(r, w) for r, w, _ in FWD_OUTS],
        out_shape=[jax.ShapeDtypeStruct((r * tiles, w), d) for r, w, d in FWD_OUTS],
        compiler_params=pltpu.CompilerParams(vmem_limit_bytes=VMEM_LIMIT, dimension_semantics=("arbitrary",)),
        name="char_forward",
    )(x, cnt, *weights)


def vectors(sm):
    rows = []
    for i, n in enumerate((64, 64, 64, 128, 128)):
        v = jnp.concatenate([sm[f, i : i + 1, :n] for f in range(sm.shape[0])], axis=1)
        rows.append(v if n == 128 else jnp.concatenate([v, jnp.zeros_like(v)], axis=1))
    return jnp.concatenate(rows + [jnp.zeros((3, 512), F32)], axis=0)


CHUNKS = ((0, 4), (4, 6), (6, 8))
LAG = 6


def gather_fwd_kernel(*refs):
    refs = list(refs)
    take = lambda n: [refs.pop(0) for _ in range(n)]
    x, counts, words_in = take(3)
    small_in = take(5)
    shards = take(PIECES - 1)
    outs = take(len(FWD_OUTS))
    full_out = take(len(GATHERED))
    vec_out, cnt_out, xall = take(3)
    wholes = take(len(GATHERED))
    vec, cnt, xown, pool, kept, small, send, recv, xsend, xrecv, local_sems = refs
    shards.insert(5, small)
    at = Place()
    T = at.T
    own = at.c * T + at.t
    part = ROWS // 16
    pieces = gather_pieces(at, shards, wholes, (send, recv), local_sems)
    qo, up, dn, pj, sm, wa, wb, wo, zu, zd = pieces
    step = pl.program_id(0)
    last = pl.num_programs(0) - 1

    def out(i):
        return pltpu.make_async_copy(wholes[i], full_out[i], local_sems.at[PIECES + i])

    def chunk(i):
        lo, hi = CHUNKS[i]
        return span(lo * part, (hi - lo) * part) if lo % (hi - lo) == 0 else pl.ds(lo * part, (hi - lo) * part)

    def row_copy(i, k, incoming=False):
        dst = xall.at[at.c * T + (at.tp(-k) if incoming else at.t), chunk(i)]
        return remote(dst if incoming else xown.at[chunk(i)], dst, (xsend, xrecv), i * 2 * T + k - 1, {"tp": at.tp(k)})

    def side_copy(i, k):
        dst = xall.at[at.tp(-k), chunk(i)]
        return remote(xown.at[chunk(i)] if k == 0 else dst, dst, (xsend, xrecv), i * 2 * T + T - 1 + k, {"ctx": 1 - at.c})

    def keep(i):
        return pltpu.make_async_copy(xown.at[chunk(i)], xall.at[own, chunk(i)], local_sems.at[PIECES + len(GATHERED) + i])

    def cross_copy(k):
        dst = xall.at[own, chunk(1)]
        return remote(xown.at[chunk(1)], dst, (xsend, xrecv), 2 * T + T - 1 + k, {"ctx": 1, "tp": at.tp(k)})

    def crossed(k):
        dst = xall.at[at.tp(-k), chunk(1)]
        return remote(dst, dst, (xsend, xrecv), 2 * T + T - 1 + k, {"ctx": 1 - at.c})

    def send_rows(i):
        keep(i).start()
        for k in range(1, T):
            pl.when(((at.c == 0) & (i == 0)) | (at.t + k < T))(lambda k=k: row_copy(i, k).start())

        @pl.when(at.c == 0)
        def _():
            for k in range(T if i else 1):
                (cross_copy(k) if i else side_copy(0, 0)).start()

    def pass_rows(i):
        @pl.when(at.c == 0)
        def _():
            for k in range(1, T):
                row_copy(i, k, True).wait_recv()
                side_copy(i, k).start()

    def take_rows(i):
        for k in range(T):
            pl.when(at.c == 1)(lambda k=k: (crossed(k) if i else side_copy(i, k)).wait_recv())
        for k in range(1, T):
            pl.when((at.t >= k) & ((at.c == 1) | (i == 1)))(lambda k=k: row_copy(i, k, True).wait_recv())

    def drain_rows(i):
        keep(i).wait()
        for k in range(1, T):
            pl.when(((at.c == 0) & (i == 0)) | (at.t + k < T))(lambda k=k: row_copy(i, k).wait_send())

        @pl.when(at.c == 0)
        def _():
            for k in range(T):
                (cross_copy(k) if i else side_copy(0, k)).wait_send()

    tiles = pl.num_programs(0) - LAG

    def when(i, *acts):
        @pl.when(step == i)
        def _():
            for act in acts:
                act()

    def open_():
        small[...] = jnp.zeros_like(small)
        for i, v in enumerate(small_in):
            small[i : i + 1, : v.shape[1]] = v[...].astype(F32)
        greet(at.peers())
        for p in (qo, sm):
            p.begin()
        cnt[...] = count_lanes(counts[...])
        cnt_out[...] = cnt[...]
        qo.spread()
        for p in (up, dn):
            p.begin()
        sm.spread()
        vec[...] = vectors(wholes[4])
        vec_out[...] = vec[...]
        qo.pass_on()
        qo.arrive()
        for p in (up, dn):
            p.spread()
        for p in (pj, wa, wb, wo):
            p.begin()

    def copy_out(*which):
        for i in which:
            out(i).start()

    groups = ROWS // GROUP

    def count_rows(i):
        return jnp.concatenate([cnt[pl.ds(i * groups + g, 1), :] for g in range(groups)], axis=0)

    def rows_of(i):
        r = chunk(i)
        start = words_in[r, :].astype(F32) + mm(pool[r, :], wholes[3][...])
        xown[r, :] = (ln_parts(start)[0] * vec[3:4, :]).astype(BF16)

    when(0, open_)
    when(6, *[p.spread for p in (pj, wa, wb, wo)])
    when(7, zu.begin, zd.begin)
    when(9, pj.pass_on, lambda: copy_out(0, 1, 2))
    when(10, lambda: send_rows(0))
    when(12, wa.pass_on, wb.pass_on, wo.pass_on, lambda: send_rows(1), lambda: copy_out(3))
    when(13, lambda: pass_rows(0), wa.arrive, wb.arrive, wo.arrive, lambda: copy_out(5, 6), zu.spread, zd.spread, lambda: copy_out(7, 8))

    @pl.when(step < tiles)
    def _():
        first = char_attn_tile(x[...], count_rows(step), (vec[0:1, :256], wholes[0][:, :768], wholes[0][:, 768:]))
        for ref, val in zip(outs[:4], first):
            ref[...] = val
        kept[lax.rem(step, LAG + 1)] = first[3]

    when(LAG, *[p.pass_on for p in (up, dn)], *[p.arrive for p in (up, dn)])

    @pl.when(step >= LAG)
    def _():
        i = step - LAG
        second = char_mlp_tile(kept[lax.rem(i, LAG + 1)], count_rows(i), (None, None, None, vec[1:2, :256], wholes[1][...], wholes[2][...].reshape(1024, 256), vec[2:3, :256]))
        for ref, val in zip(outs[4:], second):
            ref[...] = val
        pool[span(i * part, part), :] = second[3]

    when(3 + LAG, lambda: rows_of(0))
    when(5 + LAG, lambda: rows_of(1))

    @pl.when(step == last)
    def _():
        rows_of(2)
        keep(2).start()
        for p in pieces:
            p.drain()
        for i in (0, 1, 2, 3, 5, 6, 7, 8):
            out(i).wait()
        for i in range(2):
            take_rows(i)
            drain_rows(i)
        keep(2).wait()


def gather_forward(x, counts, words_in, small, shards):
    tiles = x.shape[0] // ROWS
    F, T = lax.axis_size("fsdp"), lax.axis_size("tp")
    any_ = pl.BlockSpec(memory_space=pl.ANY)
    count = PIECES * Piece.slots(F, T)
    words, width = words_in.shape
    nchunk = len(CHUNKS) * 2 * T

    def early(r, w):
        return pl.BlockSpec((r, w), lambda i: (jnp.minimum(i, tiles - 1), 0))

    def late(r, w):
        return pl.BlockSpec((r, w), lambda i: (jnp.maximum(i - LAG, 0), 0))

    return pl.pallas_call(
        gather_fwd_kernel,
        grid=(tiles + LAG,),
        in_specs=[early(ROWS, 256), full_spec(counts.shape), full_spec(words_in.shape)] + [full_spec(v.shape) for v in small] + [any_] * len(shards),
        out_specs=[early(r, w) for r, w, _ in FWD_OUTS[:4]] + [late(r, w) for r, w, _ in FWD_OUTS[4:]] + [any_] * len(GATHERED) + [full_spec((8, 512)), full_spec((x.shape[0] // GROUP, GROUP)), any_],
        out_shape=[jax.ShapeDtypeStruct((r * tiles, w), d) for r, w, d in FWD_OUTS]
        + [jax.ShapeDtypeStruct(sh, d) for sh, d in GATHERED]
        + [jax.ShapeDtypeStruct((8, 512), F32), jax.ShapeDtypeStruct((x.shape[0] // GROUP, GROUP), F32), jax.ShapeDtypeStruct((2 * T, words, width), BF16)],
        scratch_shapes=[pltpu.VMEM(sh, d) for sh, d in GATHERED]
        + [pltpu.VMEM((8, 512), F32), pltpu.VMEM((x.shape[0] // GROUP, GROUP), F32), pltpu.VMEM((words, width), BF16), pltpu.VMEM((words, 256), BF16), pltpu.VMEM((LAG + 1, ROWS, 256), F32), pltpu.VMEM((8, 128), F32)]
        + [pltpu.SemaphoreType.DMA((n,)) for n in (count, count, nchunk, nchunk, PIECES + len(GATHERED) + len(CHUNKS))],
        compiler_params=pltpu.CompilerParams(vmem_limit_bytes=VMEM_LIMIT, collective_id=0, has_side_effects=True, dimension_semantics=("arbitrary",)),
        name="gather_forward",
    )(x, counts, words_in, *small, *shards)


def word_kernel(
    pooled, proj, words_in, cot, vec, xin, w3_in, wo_in, zu, zd,
    block_out, rms, words_grad, gpool, d_proj, d_vec, h_w4, h_up, h_down,
    xall, kk, vv, kt, vt, ss, ee, qm, dom, mx, ll, ot, dqt, w3, wout, wup, wdown, dk_acc, dv_acc, dlt, dk_sum, dv_sum,
    dx_in, dx_own, g_up, g_down, g_w4, in_up, in_down, in_w4,
    xlast, w_send, w_recv, g_send, g_recv, rs_send, rs_recv, x_send, x_recv, local_sems,
):
    at = Place()
    T = at.T
    own = at.c * T + at.t
    nblk, blk, width = xall.shape
    dx = kk
    half = HEADS // 2
    low = pair_masks(blk)
    first, second = range(half), range(half, HEADS)
    cu = zu.shape[1]
    loads = [pltpu.make_async_copy(src, dst, local_sems.at[i]) for i, (src, dst) in enumerate(((w3_in, w3), (xin, xall), (wo_in, wout)))]
    for load in loads:
        load.start()

    near = (at.t + 1 - 2 * lax.rem(at.t, 2), lax.rem(at.t + 2, T))
    far = T - 1 - at.t

    def area(c, t, i, part=None):
        r = span(2 * cu * t + cu * c, cu)
        if part is None:
            return wup.at[:, r] if i == 0 else wdown.at[r, :]
        if i == 0:
            return wup.at[pl.ds(part * width // 2, width // 2), r]
        return wdown.at[span(2 * cu * t + cu * c + part * (cu // 2), cu // 2), :]

    def wide(n, i, incoming=False):
        dst = area(at.c, near[n] if incoming else at.t, i)
        return remote(dst if incoming else (zu, zd)[i], dst, (w_send, w_recv), 2 * n + i, {"tp": near[n]})

    def onward(n, i, incoming=False):
        dst = area(at.c, far if incoming else near[1 - n], i, n)
        return remote(dst, dst, (w_send, w_recv), 4 + 2 * n + i, {"tp": near[n]})

    def side(k, i, incoming=False):
        t = (at.t, near[0], near[1], far)[k]
        dst = area(1 - at.c if incoming else at.c, t, i)
        return remote((zu, zd)[i] if k == 0 and not incoming else dst, dst, (w_send, w_recv), 8 + 2 * k + i, {"ctx": 1 - at.c})

    def mine(i):
        return pltpu.make_async_copy((zu, zd)[i], area(at.c, at.t, i), local_sems.at[3 + i])

    plane = [{"ctx": i, "tp": at.tp(k)} for i in (at.c, 1 - at.c) for k in range(T) if k > 0] + [{"ctx": 1 - at.c}]
    call(plane)
    tail = xlast.shape[1]
    lead = blk - tail

    start = words_in[...].astype(F32) + mm(pooled[...], proj[...])
    shat, sr = ln_parts(start)
    g1v = vec[3:4, :]
    wq, wk, wv = w3.at[0], w3.at[1], w3.at[2]
    loads[0].wait()
    loads[1].wait()
    xown = xall[own]
    q = mm(xown, wq[...]).astype(BF16) * BF16(0.125)
    for p in range(HEADS // 2):
        a, b = split_heads(q[:, 128 * p : 128 * p + 128], low)
        qm[2 * p] = a
        qm[2 * p + 1] = b
    mx[...] = jnp.full(mx.shape, MASKED, F32)
    ll[...] = jnp.zeros(ll.shape, F32)
    ot[...] = jnp.zeros(ot.shape, F32)
    dqt[...] = jnp.zeros(dqt.shape, F32)
    dk_sum[...] = jnp.zeros(dk_sum.shape, F32)
    dv_sum[...] = jnp.zeros(dv_sum.shape, F32)

    def scores_of(j, heads):
        for h in heads:
            p = h // 2
            s = mm_nt(kk[j, :, 128 * p : 128 * p + 128], qm[h])
            ss[j, h % half] = s
            mx[h] = jnp.maximum(mx[h], jnp.max(s.reshape(blk // 8, 8, blk), axis=0))

    def mix_of(j, heads):
        for h in heads:
            e = jnp.exp(ss[j, h % half] - mx[h, 0:1, :])
            ll[h] += jnp.sum(e.reshape(blk // 8, 8, blk), axis=0)
            eb = e.astype(BF16)
            ee[j, h] = eb
            ot[64 * h : 64 * h + 64, :] += mm(vt[j, 64 * h : 64 * h + 64, :], eb)

    def top_of(heads):
        for h in heads:
            mx[h] = jnp.broadcast_to(jnp.max(mx[h], axis=0, keepdims=True), (8, blk))

    meet(plane)

    def got_rows(j, sem):
        pltpu.make_async_remote_copy(
            src_ref=xlast.at[j], dst_ref=xlast.at[j], send_sem=x_send.at[0], recv_sem=x_recv.at[sem],
            device_id={"ctx": 1 - at.c}, device_id_type=MESH,
        ).wait_recv()
        xall[j, lead:, :] = xlast[j]

    for k in range(T):

        @pl.when((at.c == 0) & (at.t + k < T) & (k > 0))
        def _():
            if k:
                remote(xin.at[own, pl.ds(lead, tail)], xlast.at[own], (x_send.at[2 * k], x_recv.at[2 * k]), None, {"ctx": 0, "tp": at.tp(k)}).start()

        @pl.when((at.c == 0) | ((at.t + k < T) & (k > 0)))
        def _():
            remote(xin.at[own, pl.ds(lead, tail)], xlast.at[own], (x_send.at[2 * k + 1], x_recv.at[2 * k + 1 + 2 * T * at.c]), None, {"ctx": 1, "tp": at.tp(k)}).start()


    for i in range(2):
        for n in range(2):
            wide(n, i).start()
        side(0, i).start()
        mine(i).start()

    def others():
        for k in range(T):
            pl.when((at.c == 0) & (at.t >= k) & (k > 0))(lambda k=k: got_rows(at.t - k, 2 * k))
            pl.when(at.c == 1)(lambda k=k: got_rows(at.tp(-k), 2 * k + 1))
            pl.when((at.c == 1) & (at.t >= k) & (k > 0))(lambda k=k: got_rows(T + at.t - k, 2 * k + 1 + 2 * T))

    @pl.loop(0, own + 1)
    def _(m):
        pl.when(m == 1)(others)
        j = own - m
        xj = xall[j]
        kj = mm(xj, wk[...]).astype(BF16)
        vj = mm(xj, wv[...]).astype(BF16)
        kk[j] = kj
        vv[j] = vj
        kt[j] = jnp.transpose(kj)
        vt[j] = jnp.transpose(vj)
        scores_of(j, first)

    top_of(first)
    for i in range(2):
        for n in range(2):
            wide(n, i, True).wait_recv()
        for n in range(2):
            onward(n, i).start()
            side(1 + n, i).start()

    @pl.loop(0, own + 1)
    def _(j):
        mix_of(j, first)
        scores_of(j, second)

    top_of(second)

    @pl.loop(0, own + 1)
    def _(j):
        mix_of(j, second)

    for h in range(HEADS):
        linv = 1.0 / jnp.sum(ll[h], axis=0, keepdims=True)
        ll[h] = jnp.broadcast_to(linv, (8, blk))
        ot[64 * h : 64 * h + 64, :] = ot[64 * h : 64 * h + 64, :] * linv
    mixed_t = ot[...].astype(BF16)
    mixed = jnp.transpose(mixed_t)
    loads[2].wait()
    attn = mm(mixed, wout[...])
    awa = start + attn
    ahat, ar = ln_parts(awa)
    g2v = vec[4:5, :]
    n2 = (ahat * g2v).astype(BF16)
    for i in range(2):
        for n in range(2):
            onward(n, i, True).wait_recv()
        side(3, i).start()
    for i in range(2):
        mine(i).wait()
        for k in range(4):
            side(k, i, True).wait_recv()
    upper, dgelu = gelu_both(mm(n2, wup[...]))
    upper = upper.astype(BF16)
    mlp = mm(upper, wdown[...])
    final = awa + mlp
    block_out[...] = final.astype(BF16)
    lane = lax.broadcasted_iota(jnp.int32, (blk, 128), 1)
    cols = [jnp.sqrt(jnp.mean(v * v, axis=-1, keepdims=True)) for v in (attn, mlp, final)]
    rms[...] = jnp.transpose(jnp.where(lane == 0, cols[0], jnp.where(lane == 1, cols[1], cols[2])))[0:3, :]
    cotv = cot[...]
    gdown = mm_tn(upper, cotv).astype(BF16)
    ghid = (dgelu * mm_nt(cotv, wdown[...])).astype(BF16)
    gup = mm_tn(n2, ghid).astype(BF16)
    for c in range(2):
        for t in range(T):
            g_down[c, cu * t : cu * t + cu, :] = gdown[cu * (2 * t + c) : cu * (2 * t + c) + cu, :]
            g_up[c, :, cu * t : cu * t + cu] = gup[:, cu * (2 * t + c) : cu * (2 * t + c) + cu]
    grads = ((g_down, in_down, h_down), (g_up, in_up, h_up), (g_w4, in_w4, h_w4))

    def swap(i):
        return remote(grads[i][0].at[1 - at.c], grads[i][1], (g_send, g_recv), i, {"ctx": 1 - at.c})

    def store(i):
        return pltpu.make_async_copy(grads[i][0].at[at.c], grads[i][2], local_sems.at[5 + i])

    def add_halves(i):
        g, other, _ = grads[i]
        swap(i).wait_recv()
        g[at.c] = (g[at.c].astype(F32) + other[...].astype(F32)).astype(BF16)
        store(i).start()

    gn2 = mm_nt(ghid, wup[...])
    d_g2 = jnp.sum(gn2 * ahat, axis=0, keepdims=True)
    ga = cotv.astype(F32) + ln_back(ahat, ar, g2v, gn2)
    gal = ga.astype(BF16)
    g_w4[1, 1] = mm_tn(gal, mixed).astype(BF16)
    swap(0).start()
    swap(1).start()
    do_t = mm_nt(wout[...], gal).astype(BF16)
    do_s = []
    for h in range(HEADS):
        r = slice(64 * h, 64 * h + 64)
        d = do_t[r, :].astype(F32)
        linv = ll[h, 0:1, :]
        dlt[h] = jnp.broadcast_to(jnp.sum(d * ot[r, :], axis=0, keepdims=True) * linv, (8, blk))
        do_s.append((d * linv).astype(BF16))
    do = jnp.transpose(jnp.concatenate(do_s, axis=0))
    for p in range(HEADS // 2):
        a, b = split_heads(do[:, 128 * p : 128 * p + 128], low)
        dom[2 * p] = a
        dom[2 * p + 1] = b

    add_halves(0)
    add_halves(1)

    def grad_copy(j):
        return remote(dx.at[j], dx_in.at[own], (rs_send.at[j], rs_recv.at[own]), None, {"ctx": j // T, "tp": lax.rem(j, T)})

    @pl.loop(0, own + 1)
    def _(j):
        @pl.when(j > 0)
        def _():
            grad_copy(j - 1).start()

        for p in range(HEADS // 2):
            c = slice(128 * p, 128 * p + 128)
            vp = vv[j, :, c]
            dk = None
            for h in (2 * p, 2 * p + 1):
                e = ee[j, h]
                dp = mm_nt(vp, dom[h])
                ds = (e.astype(F32) * (dp - dlt[h, 0:1, :])).astype(BF16)
                dvh = mm(e, dom[h])
                dkh = mm(ds, qm[h])
                dk, dv = (dkh, dvh) if dk is None else (dk + dkh, dv + dvh)
                dqt[64 * h : 64 * h + 64, :] += mm(kt[j, 64 * h : 64 * h + 64, :], ds)
            dk_acc[:, c] = dk.astype(BF16)
            dv_acc[:, c] = dv.astype(BF16)
        dk = dk_acc[...]
        dv = dv_acc[...]
        dxj = mm_nt(dk, wk[...]) + mm_nt(dv, wv[...])
        dx[j] = dxj.astype(BF16)
        dx_own[...] = dxj
        xt = jnp.transpose(xall[j])
        dk_sum[...] += mm(xt, dk)
        dv_sum[...] += mm(xt, dv)

    dq = jnp.transpose((dqt[...] * 0.125).astype(BF16))
    g_w4[0, 0] = mm_tn(xown, dq).astype(BF16)
    g_w4[0, 1] = dk_sum[...].astype(BF16)
    g_w4[1, 0] = dv_sum[...].astype(BF16)
    swap(2).start()
    dx_own[...] += mm_nt(dq, wq[...])

    @pl.loop(own + 1, nblk)
    def _(b):
        remote(dx.at[own], dx_in.at[b], (rs_send.at[b], rs_recv.at[b]), None, {"ctx": 1 - at.c}).wait_recv()
        dx_own[...] += dx_in[b].astype(F32)

    gnf = dx_own[...]
    grad = ga + ln_back(shat, sr, g1v, gnf)
    words_grad[...] = grad
    d_vec[...] = jnp.concatenate([jnp.sum(gnf * shat, axis=0, keepdims=True), d_g2, jnp.zeros((6, width), F32)], axis=0)
    gproj = grad.astype(BF16)
    gproj_w = mm_tn(pooled[...], gproj).astype(BF16)
    hr = gproj_w.shape[0] // (2 * at.F)
    for i in range(at.F):
        for c in range(2):
            d_proj[c, hr * i : hr * i + hr, :] = gproj_w[hr * (2 * i + c) : hr * (2 * i + c) + hr, :]
    gpool[...] = mm_nt(gproj, proj[...])

    add_halves(2)
    for k in range(T):
        pl.when((at.c == 0) & (at.t + k < T) & (k > 0))(lambda k=k: remote(xin.at[own, pl.ds(lead, tail)], xlast.at[own], (x_send.at[2 * k], x_recv.at[2 * k]), None, {"ctx": 0, "tp": at.tp(k)}).wait_send() if k else None)
        pl.when((at.c == 0) | ((at.t + k < T) & (k > 0)))(lambda k=k: remote(xin.at[own, pl.ds(lead, tail)], xlast.at[own], (x_send.at[2 * k + 1], x_recv.at[2 * k + 1]), None, {"ctx": 1 - at.c}).wait_send())
    for i in range(2):
        for n in range(2):
            wide(n, i).wait_send()
            onward(n, i).wait_send()
        for k in range(4):
            side(k, i).wait_send()
    for i in range(3):
        swap(i).wait_send()
        store(i).wait()

    @pl.loop(0, own)
    def _(j):
        grad_copy(j).wait_send()


def word_section(pooled, proj, words_in, cot, vec, xall, w3, wo, zu, zd):
    blk, width = words_in.shape
    T = lax.axis_size("tp")
    nblk = 2 * T
    cu = zu.shape[1]
    ff = 2 * T * cu
    vm = pl.BlockSpec(memory_space=pltpu.VMEM)
    any_ = pl.BlockSpec(memory_space=pl.ANY)
    out_shapes = [((blk, width), BF16), ((3, blk), F32), ((blk, width), F32), ((blk, pooled.shape[1]), F32), ((2, proj.shape[0] // 2, width), BF16), ((8, width), F32)]
    halves = [((2, width, width), BF16), ((width, ff // 2), BF16), ((ff // 2, width), BF16)]
    bufs = [
        ((nblk, blk, width), BF16), ((nblk, blk, width), BF16), ((nblk, blk, width), BF16), ((nblk, width, blk), BF16), ((nblk, width, blk), BF16),
        ((nblk, HEADS // 2, blk, blk), F32), ((nblk, HEADS, blk, blk), BF16), ((HEADS, blk, 128), BF16), ((HEADS, blk, 128), BF16),
        ((HEADS, 8, blk), F32), ((HEADS, 8, blk), F32), ((width, blk), F32), ((width, blk), F32),
        ((3, width, width), BF16), ((width, width), BF16), ((width, ff), BF16), ((ff, width), BF16), ((blk, width), BF16), ((blk, width), BF16), ((HEADS, 8, blk), F32),
        ((width, width), F32), ((width, width), F32), ((nblk, blk, width), BF16), ((blk, width), F32),
        ((2, width, ff // 2), BF16), ((2, ff // 2, width), BF16), ((2, 2, width, width), BF16), ((width, ff // 2), BF16), ((ff // 2, width), BF16), ((2, width, width), BF16),
    ]
    nw = 16
    rows = (CHUNKS[-1][1] - CHUNKS[-1][0]) * (ROWS // 16)
    return pl.pallas_call(
        word_kernel,
        in_specs=[vm] * 5 + [any_] * 5,
        out_specs=[vm] * len(out_shapes) + [any_] * len(halves),
        out_shape=[jax.ShapeDtypeStruct(s, d) for s, d in out_shapes + halves],
        scratch_shapes=[pltpu.VMEM(s, d) for s, d in bufs] + [pltpu.VMEM((nblk, rows, width), BF16)] + [pltpu.SemaphoreType.DMA((n,)) for n in (nw, nw, 3, 3, nblk, nblk, 2 * T, 4 * T, 8)],
        compiler_params=pltpu.CompilerParams(vmem_limit_bytes=VMEM_LIMIT, collective_id=1, has_side_effects=True),
        name="word_section",
    )(pooled, proj, words_in, cot, vec, xall, w3, wo, zu, zd)


def sweep(shape, act, rows=32):
    rows = min(rows, shape[-2])

    @pl.loop(0, shape[-2] // rows)
    def _(i):
        act((ALL,) * (len(shape) - 2) + (span(i * rows, rows), ALL))


class Sum:
    def __init__(self, at, source, bufs, tp_cut, fs_cut, sems, first, wide, halved):
        self.at, self.source, self.sems, self.first, self.wide, self.halved = at, source, sems, first, wide, halved
        self.own, self.away, self.got, self.blocks, self.block, self.pieces, self.done = bufs
        self.hold, self.came = self.away, self.got
        self.near = (at.t + 1 - 2 * lax.rem(at.t, 2), lax.rem(at.t + 2, at.T))
        self.far = at.T - 1 - at.t
        self.fs_base = 5 if halved else at.T - 1
        self.tp_cut, self.fs_cut = tp_cut, fs_cut

    @staticmethod
    def slots(F, T):
        return 6 + (F - 1) + 2 * T

    @staticmethod
    def buffers(half, block, piece, F, T, wide, halved):
        quarter = (block[0] // 2,) + block[1:]
        first = [block, (4,) + quarter, (6,) + quarter, (1, 8, 128)] if halved else [half, half, half, (T - 1,) + block]
        shapes = first + [block, (F - 1,) + piece, ((2, T) if wide else (2,)) + piece]
        return [pltpu.VMEM(sh, BF16) for sh in shapes]

    def swap(self):
        at = self.at
        return remote(self.away, self.got, self.sems, self.first, {"ctx": 1 - at.c})

    def to_tp(self, k):
        src = self.source if self.halved else self.own
        return remote(src.at[self.tp_cut(self.at.tp(k))], self.blocks.at[k - 1], self.sems, self.first + k, {"tp": self.at.tp(k)})

    def to_fs(self, k):
        return remote(self.block.at[self.fs_cut(self.at.fs(k))], self.pieces.at[k - 1], self.sems, self.first + self.fs_base + k, {"fsdp": self.at.fs(k)})

    def share(self, k, x, incoming=False):
        at = self.at
        there = 1 - at.c if x else at.c
        c = there if incoming else at.c
        r = self.done.at[c, at.tp(-k) if incoming else at.t] if self.wide else self.done.at[c]
        return remote(r, r, self.sems, self.first + self.fs_base + at.F + 2 * k + x, {"ctx": there, "tp": at.tp(k)} if k else {"ctx": there})

    def shares(self):
        if not self.wide:
            return [(0, 1)]
        return [(k, x) for k in range(self.at.T) for x in range(2) if k or x]

    def local(self, i):
        src = self.source.at[self.at.c if i == 0 else 1 - self.at.c]
        return pltpu.make_async_copy(src, self.own if i == 0 else self.away, self.loc.at[i])

    def fetch(self, loc):
        self.loc = loc
        for i in range(2):
            self.local(i).start()

    def begin_fetched(self):
        for i in range(2):
            self.local(i).wait()
        self.swap().start()

    def begin(self):
        near, there = self.source.at[self.at.c], self.source.at[1 - self.at.c]

        def act(r):
            self.own[r] = near[r].astype(BF16)
            self.away[r] = there[r].astype(BF16)

        sweep(self.own.shape, act)
        self.swap().start()

    def halves(self):
        self.swap().wait_recv()

        def act(r):
            self.own[r] = (self.own[r].astype(F32) + self.got[r].astype(F32)).astype(BF16)

        sweep(self.own.shape, act)
        for k in range(1, self.at.T):
            self.to_tp(k).start()

    def part(self, t, i):
        cut = list(self.tp_cut(t))
        n = self.own.shape[0] // 2
        if cut[0] == ALL:
            cut[0] = pl.ds(i * n, n)
        else:
            cut[0] = span(t * 2 * n + i * n, n)
        return self.source.at[tuple(cut)]

    def mine(self, i):
        t, j = ((self.at.t, 0), (self.at.t, 1), (self.near[1], 0), (self.near[0], 1))[i]
        return pltpu.make_async_copy(self.part(t, j), self.hold.at[i], self.loc.at[i])

    def near_send(self, n, far):
        at = self.at
        src = self.part(self.far if far else self.near[n], n)
        return remote(src, self.came.at[2 * n + far], self.sems, self.first + 2 * n + far, {"tp": self.near[n]})

    def onward(self, n):
        return remote(self.hold.at[2 + n], self.came.at[4 + n], self.sems, self.first + 4 + n, {"tp": self.near[1 - n]})

    def begin_halved(self):
        for i in range(4):
            self.mine(i).start()
        for n in range(2):
            for far in (1, 0):
                self.near_send(n, far).start()

    def pass_halved(self):
        for i in range(4):
            self.mine(i).wait()
        for n in range(2):
            self.near_send(n, 1).wait_recv()
            mine, came = self.hold.at[2 + n], self.came.at[2 * n + 1]

            def act(r, mine=mine, came=came):
                mine[r] = (mine[r].astype(F32) + came[r].astype(F32)).astype(BF16)

            sweep(mine.shape, act)
        for n in range(2):
            self.onward(n).start()

    def over_near(self):
        n = self.own.shape[0] // 2
        for i in range(2):
            self.near_send(i, 0).wait_recv()
            self.onward(i).wait_recv()
            terms = (self.hold.at[i], self.came.at[2 * i], self.came.at[4 + i])
            block = self.block.at[pl.ds(i * n, n)]

            def act(r, terms=terms, block=block):
                block[r] = sum(v[r].astype(F32) for v in terms).astype(BF16)

            sweep(block.shape, act)
        for k in range(1, self.at.F):
            self.to_fs(k).start()

    def over_tp(self):
        own = self.own.at[self.tp_cut(self.at.t)]
        for k in range(1, self.at.T):
            self.to_tp(k).wait_recv()
        terms = [own] + [self.blocks.at[k - 1] for k in range(1, self.at.T)]

        def act(r):
            self.block[r] = sum(v[r].astype(F32) for v in terms).astype(BF16)

        sweep(self.block.shape, act)
        for k in range(1, self.at.F):
            self.to_fs(k).start()

    def over_fsdp(self):
        at = self.at
        for k in range(1, at.F):
            self.to_fs(k).wait_recv()
        terms = [self.block.at[self.fs_cut(at.f)]] + [self.pieces.at[k - 1] for k in range(1, at.F)]
        done = self.done.at[at.c, at.t] if self.wide else self.done.at[at.c]

        def act(r):
            done[r] = sum(v[r].astype(F32) for v in terms).astype(BF16)

        sweep(done.shape, act)
        for k, x in self.shares():
            self.share(k, x).start()

    def finish(self):
        for k, x in self.shares():
            self.share(k, x, True).wait_recv()

    def drain(self):
        at = self.at
        if self.halved:
            for n in range(2):
                for far in range(2):
                    self.near_send(n, far).wait_send()
                self.onward(n).wait_send()
        else:
            self.swap().wait_send()
            for k in range(1, at.T):
                self.to_tp(k).wait_send()
        for k in range(1, at.F):
            self.to_fs(k).wait_send()
        for k, x in self.shares():
            self.share(k, x).wait_send()


SUMS = [
    ((2, 512, 512), (2, 512, 128), (2, 128, 128), 2, 1, False, True),
    ((512, 1024), (512, 256), (128, 256), 1, 0, False, True),
    ((1024, 512), (256, 512), (256, 128), 0, 1, False, True),
    ((128, 512), (128, 128), (32, 128), 1, 0, True, False),
    ((256, 512), (256, 128), (64, 128), 1, 0, True, False),
    ((128, 1024), (32, 1024), (32, 256), 0, 1, True, False),
    ((256, 512), (256, 128), (64, 128), 1, 0, True, False),
]


def cutter(shape, axis, size):
    def cut(i):
        return tuple(span(i * size, size) if d == axis else ALL for d in range(len(shape)))

    return cut


def reduce_bwd_kernel(tiles, *refs):
    refs = list(refs)
    take = lambda n: [refs.pop(0) for _ in range(n)]
    ins = take(14)
    sources = take(4)
    (d_vec,) = take(1)
    (cg,) = take(1)
    results = take(len(SUMS))
    (vec_out,) = take(1)
    (gca,) = take(1)
    accs = take(len(ACCS))
    at = Place()
    bufs = [take(7) for _ in SUMS]
    vec_in, send, recv, vsend, vrecv, local_sems = refs
    slots = Sum.slots(at.F, at.T)
    a_qo, a_up, a_dn, a_vec = accs
    origin = list(sources) + [a_up, a_dn, a_qo]
    sums = []
    for i, (half, block, piece, ta, fa, wide, halved) in enumerate(SUMS):
        sums.append(Sum(at, origin[i], bufs[i], cutter(half, ta, block[ta]), cutter(block, fa, piece[fa]), (send, recv), i * slots, wide, halved))
        sums[i].loc = local_sems.at[i]
    w4, wup, wdn, pj, up, dn, qo = sums
    step = pl.program_id(0)
    last = 2 * tiles - 1

    plan = {}

    def when(i, *acts):
        plan.setdefault(i, []).extend(acts)

    def open_():
        meet(at.peers())
        w4.begin_halved()
        wup.begin_halved()
        pj.begin_fetched()

    when(0, lambda: call(at.peers()), lambda: pj.fetch(pj.loc))
    when(1, open_)
    when(3, pj.halves)
    when(6, w4.pass_halved, wup.pass_halved, wdn.begin_halved)
    when(8, lambda: vec_begin(), up.begin, dn.begin, pj.over_tp, w4.over_near)
    when(9, lambda: vec_plane(), wup.over_near)
    when(10, wdn.pass_halved, up.halves, dn.halves, pj.over_fsdp)
    when(11, lambda: vec_depth())
    when(13, w4.over_fsdp)
    when(13, wdn.over_near)
    when(14, up.over_tp, dn.over_tp, wup.over_fsdp)

    def vec_copy(i, where):
        return remote(a_vec, vec_in.at[i], (vsend, vrecv), i, where)

    def vec_begin():
        a_vec[3:5, :] = d_vec[0:2, :]
        vec_copy(0, {"ctx": 1 - at.c}).start()

    def vec_plane():
        vec_copy(0, {"ctx": 1 - at.c}).wait()
        a_vec[...] += vec_in[0]
        for k in range(1, at.T):
            vec_copy(k, {"tp": at.tp(k)}).start()

    def vec_depth():
        for k in range(1, at.T):
            vec_copy(k, {"tp": at.tp(k)}).wait()
        a_vec[...] += vec_in[1] + vec_in[2] + vec_in[3]
        for k in range(1, at.F):
            vec_copy(at.T - 1 + k, {"fsdp": at.fs(k)}).start()

    def vec_end():
        for k in range(1, at.F):
            vec_copy(at.T - 1 + k, {"fsdp": at.fs(k)}).wait()
        total = a_vec[...] + (vec_in[4] + vec_in[5] + vec_in[6])
        rows = [jnp.zeros((2, 128), F32)]
        for i, n in ((2, 64), (3, 128), (4, 128)):
            v = jnp.zeros((1, n), F32)
            for f in range(at.F):
                v = jnp.where(at.f == f, total[i : i + 1, f * n : f * n + n], v)
            rows.append(v if n == 128 else jnp.concatenate([v, jnp.zeros((1, n), F32)], axis=1))
        vec_out[...] = jnp.concatenate(rows + [jnp.zeros((3, 128), F32)], axis=0)

    busy = functools.reduce(lambda a, b: a | b, [step == i for i in plan])

    @pl.when(busy)
    def _():
        for i, acts in plan.items():

            @pl.when(step == i)
            def _():
                for act in acts:
                    act()

    char_back_step(step, tiles, ins, cg, gca, accs, False)

    @pl.when(step == last)
    def _():
        qo.begin()
        qo.halves()

        def result(i):
            return pltpu.make_async_copy(sums[i].done, results[i], local_sems.at[i, 0])

        def keep(*which):
            for i in which:
                sums[i].finish()
                result(i).start()

        vec_end()
        keep(0, 1, 3)
        qo.over_tp()
        up.over_fsdp()
        dn.over_fsdp()
        wdn.over_fsdp()
        qo.over_fsdp()
        keep(4, 5, 2)
        for s in sums[:6]:
            s.drain()
        keep(6)
        qo.drain()
        for i in range(len(sums)):
            result(i).wait()


def reduce_backward(x, cnt, saved, gpool, weights, sources, d_vec):
    total = x.shape[0]
    tiles = total // ROWS
    F, T = lax.axis_size("fsdp"), lax.axis_size("tp")
    ins, out = back_specs(tiles, gpool, weights)
    any_ = pl.BlockSpec(memory_space=pl.ANY)
    scratch = [pltpu.VMEM((total, 256), F32)] + [pltpu.VMEM(s, F32) for s in ACCS]
    results = []
    for half, block, piece, _, _, wide, halved in SUMS:
        scratch += Sum.buffers(half, block, piece, F, T, wide, halved)
        results.append(((2, T) if wide else (2,)) + piece)
    count = len(SUMS) * Sum.slots(F, T)
    vecs = 1 + (T - 1) + (F - 1)
    scratch += [pltpu.VMEM((vecs, 8, 512), F32)]
    scratch += [pltpu.SemaphoreType.DMA((n,)) for n in (count, count, vecs, vecs)] + [pltpu.SemaphoreType.DMA((len(SUMS), 4))]
    return pl.pallas_call(
        functools.partial(reduce_bwd_kernel, tiles),
        grid=(2 * tiles,),
        in_specs=ins + [any_] * len(sources) + [full_spec((8, 512))],
        out_specs=[out] + [any_] * len(results) + [full_spec((8, 128))],
        out_shape=[jax.ShapeDtypeStruct((total, 256), F32)] + [jax.ShapeDtypeStruct(s, BF16) for s in results] + [jax.ShapeDtypeStruct((8, 128), F32)],
        scratch_shapes=scratch,
        compiler_params=pltpu.CompilerParams(vmem_limit_bytes=VMEM_LIMIT, collective_id=2, has_side_effects=True, dimension_semantics=("arbitrary",)),
        name="reduce_backward",
    )(x, cnt, *saved, gpool, *weights, *sources, d_vec)


FINAL = [(3, 128, 128), (128, 128), (128, 512), (512, 128), (64, 512), (64, 1024), (256, 256), (64, 768), (64, 256), (1, 64), (1, 64), (1, 64), (1, 128), (1, 128)]


def final_kernel(cg, block, grad, rms, w4, wup, wdn, pj, up, dn, qo, vec, w_qkv, w_up, g1, g2, cg_out, block_out, grad_out, rms_out, *outs):
    cg_out[...] = cg[...]

    @pl.when(pl.program_id(0) == 0)
    def _():
        block_out[...] = block[...]
        grad_out[...] = grad[...]
        rms_out[...] = rms[...]
        o3, o_out, o_wup, o_wdn, o_pj, o_up, o_dn, o_qkv, o_cout = outs[:9]
        o3[0] = w4[0, 0].astype(F32)
        o3[1] = w4[0, 1].astype(F32)
        o3[2] = w4[1, 0].astype(F32)
        o_out[...] = jnp.transpose(w4[1, 1].astype(F32))
        for c in range(2):
            o_wup[:, 256 * c : 256 * c + 256] = wup[c].astype(F32)
            o_wdn[256 * c : 256 * c + 256, :] = wdn[c].astype(F32)
            for t in range(pj.shape[1]):
                i = 2 * t + c
                o_pj[32 * c : 32 * c + 32, 128 * t : 128 * t + 128] = pj[c, t].astype(F32)
                o_up[:, 128 * i : 128 * i + 128] = up[c, t].astype(F32)
                ref, i = (o_qkv, i) if i < 6 else (o_cout, i - 6)
                ref[:, 128 * i : 128 * i + 128] = qo[c, t].astype(F32)
        o_dn[...] = jnp.transpose(dn[...].astype(F32).reshape(256, 256))
        for i, n in enumerate((64, 64, 64, 128, 128)):
            if i > 1:
                outs[9 + i][...] = vec[i : i + 1, :n]
        for i, (w, d, gain) in enumerate(((w_qkv, o_qkv, g1), (w_up, o_up, g2))):
            col = jnp.sum(w[...].astype(F32) * d[...], axis=-1, keepdims=True)
            row = jnp.transpose(jnp.broadcast_to(col, (64, 128)))[0:1, :]
            outs[9 + i][...] = row / gain[...].astype(F32)


def finish(cg, block, grad, rms, parts):
    tiles = 2
    rows = cg.shape[0] // tiles
    small = [block, grad, rms] + list(parts)
    return pl.pallas_call(
        final_kernel,
        grid=(tiles,),
        in_specs=[rows_spec(rows, cg.shape[1])] + [full_spec(v.shape) for v in small],
        out_specs=[rows_spec(rows, cg.shape[1])] + [full_spec(v.shape) for v in small[:3]] + [full_spec(v) for v in FINAL],
        out_shape=[jax.ShapeDtypeStruct(v.shape, v.dtype) for v in [cg] + small[:3]] + [jax.ShapeDtypeStruct(v, F32) for v in FINAL],
        compiler_params=pltpu.CompilerParams(vmem_limit_bytes=VMEM_LIMIT, dimension_semantics=("arbitrary",)),
        name="finish",
    )(cg, block, grad, rms, *parts)


def gather(x, name, axis):
    return lax.all_gather(x, name, axis=axis, tiled=True)


def scatter(x, name, axis):
    return lax.psum_scatter(x, name, scatter_dimension=axis, tiled=True)


def fits(rows):
    return lax.axis_size("fsdp") == 4 and lax.axis_size("tp") == 4 and rows == 64


def local(characters, counts, words_in, cotangent, char_prenorm, char_qkv, char_out, char_midnorm, char_up, char_down,
          pool_query, char_proj, word_prenorm, word_qkv, word_out, word_midnorm, word_up, word_down):
    words, slots, cdim = characters.shape
    x = characters.reshape(words * slots, cdim)
    vectors_in = (char_prenorm, char_midnorm, pool_query, word_prenorm, word_midnorm)
    w3 = jnp.moveaxis(word_qkv, 1, 0)
    direct = fits(char_prenorm.shape[0])
    group_rows = (words * slots // ROWS, ROWS // GROUP, GROUP)
    if direct:
        shards = [char_qkv, char_out, char_up, char_down, char_proj, w3, word_out, word_up, word_down]
        *saved, pooled_low, qo, up, dn, proj, _, w3, wo, zu, zd, vec, cnt, xall = gather_forward(x, counts.reshape(words // 128, 128), words_in, [v.reshape(1, -1) for v in vectors_in], shards)
        dn = dn.reshape(1024, 256)
        cnt = cnt.reshape(group_rows)
    else:
        cnt = jnp.repeat(counts.astype(F32), slots).reshape(group_rows)
        wide = [gather(v.astype(F32), "fsdp", 0) for v in vectors_in]
        vec = jnp.stack([jnp.pad(v, (0, 512 - v.shape[0])) for v in wide] + [jnp.zeros((512,), F32)] * 3)
        qo = jnp.concatenate([gather(char_qkv, "fsdp", 0), gather(char_out, "fsdp", 0)], axis=1)
        up, dn, proj = (gather(w, "fsdp", 0) for w in (char_up, char_down, char_proj))
        w3 = gather(gather(w3, "fsdp", 1), "tp", 2)
        wo = gather(gather(word_out, "fsdp", 1), "tp", 0)
        cu = word_up.shape[1] // 2
        zu = lax.dynamic_slice_in_dim(gather(word_up, "fsdp", 0), lax.axis_index("ctx") * cu, cu, 1)
        zd = lax.dynamic_slice_in_dim(gather(word_down, "fsdp", 1), lax.axis_index("ctx") * cu, cu, 0)
        *saved, pooled_low = char_forward(x, cnt, vec, qo, up, dn)
        start, _ = ln_parts(words_in.astype(F32) + mm(pooled_low, proj))
        xall = gather((start * vec[3:4]).astype(BF16), ("ctx", "tp"), 0).reshape(-1, words, words_in.shape[1])
    (block_out, rms, words_grad, gpool, d_proj, d_vec, h_w4, h_up, h_down) = word_section(pooled_low, proj, words_in, cotangent, vec, xall, w3, wo, zu, zd)
    if direct:
        cg, *parts = reduce_backward(x, cnt, saved, gpool, [vec, qo, up, dn], [h_w4, h_up, h_down, d_proj], d_vec)
        cg, block_out, words_grad, rms, g_qkv4, g_wout, g_wup, g_wdown, g_proj, g_up, g_down, g_qkv, g_out, *vecs = finish(cg, block_out, words_grad, rms, parts + [char_qkv, char_up, char_prenorm.reshape(1, -1), char_midnorm.reshape(1, -1)])
        vecs = [v.reshape(-1) for v in vecs]
    else:
        cg, a_qo, a_up, a_dn, a_vec = char_backward(x, cnt, saved, gpool, vec, qo, up, dn)

        def reduce_char(g):
            g = lax.psum(g.astype(BF16), ("ctx", "tp"))
            return scatter(g, "fsdp", 0).astype(F32)

        def reduce_word(g, tp_axis, fsdp_axis, ctx_axis):
            g = scatter(scatter(g, "tp", tp_axis), "fsdp", fsdp_axis)
            return gather(g, "ctx", ctx_axis).astype(F32)

        lanes = lambda g, n: jnp.moveaxis(g.reshape(2, g.shape[1], -1, n), 0, 2).reshape(g.shape[1], -1)
        hr = char_proj.shape[0] // 2
        g_qo = reduce_char(lanes(a_qo, 128))
        g_qkv, g_out = g_qo[:, :768], g_qo[:, 768:]
        g_up = reduce_char(lanes(a_up, 128))
        g_down = reduce_char(a_dn.reshape(256, 1024).T)
        g_proj = reduce_char(jnp.moveaxis(d_proj.reshape(2, -1, hr, 512), 0, 1).reshape(256, 512))
        g_w4 = reduce_word(h_w4, 2, 1, 0)
        g_qkv4, g_wout = g_w4[:3], g_w4[3].T
        g_wup = reduce_word(h_up, 1, 0, 1)
        g_wdown = reduce_word(h_down, 0, 1, 0)
        vecs = [reduce_char(v) for v in (a_vec[0, :256], a_vec[1, :256], a_vec[2, :256], d_vec[0], d_vec[1])]
    return (
        block_out,
        cg.reshape(words, slots, cdim),
        words_grad,
        rms,
        vecs[0],
        g_qkv,
        g_out,
        vecs[1],
        g_up,
        g_down,
        vecs[2],
        g_proj,
        vecs[3],
        jnp.moveaxis(g_qkv4, 0, 1),
        g_wout,
        vecs[4],
        g_wup,
        g_wdown,
    )


def solution(mesh):
    rows = ("fsdp", "ctx", "tp")
    v, m = P("fsdp"), P("fsdp", None)
    return jax.shard_map(
        local,
        mesh=mesh,
        in_specs=(
            P(rows, None, None), P(rows), P(rows, None), P(rows, None),
            v, m, m, v, m, m, v, m, v, P("fsdp", None, "tp"), P("tp", "fsdp"), v, P("fsdp", "tp"), P("tp", "fsdp"),
        ),
        out_specs=(
            P(rows, None), P(rows, None, None), P(rows, None), P(None, rows),
            v, m, m, v, m, m, v, m, v, P("fsdp", None, "tp"), P("tp", "fsdp"), v, P("fsdp", "tp"), P("tp", "fsdp"),
        ),
        check_vma=False,
    )
```

```python
import functools

import jax
import jax.numpy as jnp
from jax import lax
from jax.experimental import pallas as pl
from jax.experimental.pallas import tpu as pltpu
from jax.sharding import PartitionSpec as P

CHEADS = 4
HEADS = 8
HEAD = 64
EPSILON = 1e-05
MASKED = -1e30
CGELU = 0.7978845608028654
AGELU = 0.044715
ROWS = 512
GROUP = 128
F32 = jnp.float32
BF16 = jnp.bfloat16
VMEM_LIMIT = 66_000_000


def mm(a, b):
    return lax.dot_general(a, b, (((1,), (0,)), ((), ())), preferred_element_type=F32)


def mm_nt(a, b):
    return lax.dot_general(a, b, (((1,), (1,)), ((), ())), preferred_element_type=F32)


def mm_tn(a, b):
    return lax.dot_general(a, b, (((0,), (0,)), ((), ())), preferred_element_type=F32)


def ln_parts(x):
    c = x - jnp.mean(x, axis=-1, keepdims=True)
    r = lax.rsqrt(jnp.mean(c * c, axis=-1, keepdims=True) + EPSILON)
    return c * r, r


def ln_back(xhat, r, gain, g):
    gg = g * gain
    a = jnp.mean(gg, axis=-1, keepdims=True)
    b = jnp.mean(gg * xhat, axis=-1, keepdims=True)
    return r * (gg - a - xhat * b)


def gelu_both(x):
    x2 = x * x
    y = (CGELU * AGELU) * x2 + CGELU
    hp = 0.5 * jnp.tanh(x * y) + 0.5
    g = x * hp
    d = hp + (g - g * hp) * (6.0 * y - 4.0 * CGELU)
    return g, d


def pair_masks(rows):
    lane = lax.broadcasted_iota(jnp.int32, (rows, 128), 1)
    return lane < HEAD


def split_heads(x, low_lanes):
    zero = jnp.zeros_like(x)
    return jnp.where(low_lanes, x, zero), jnp.where(low_lanes, zero, x)


def stack_heads(x, low_lanes):
    a, b = split_heads(x, low_lanes)
    return jnp.concatenate([a, b], axis=0)


def word_of_lane(width):
    return (lax.broadcasted_iota(jnp.int32, (16, width), 1) % GROUP) // 16


def compress(blocks, lane_word):
    out = blocks[0:16, :]
    for w in range(1, GROUP // 16):
        out = jnp.where(lane_word == w, blocks[16 * w : 16 * w + 16, :], out)
    return out


def expand(dense, lane_word):
    zero = jnp.zeros_like(dense)
    return jnp.concatenate(
        [jnp.where(lane_word == w, dense, zero) for w in range(GROUP // 16)], axis=0
    )


def pool_weights(am, q_row, cnt_col):
    words = am.shape[0] // 16
    am3 = am.reshape(words, 16, am.shape[1])
    logits = jnp.sum(am * q_row, axis=-1, keepdims=True)
    slot = (lax.broadcasted_iota(jnp.int32, (am.shape[0], 1), 0) % 16).astype(F32)
    logits = jnp.where(slot < cnt_col, logits, MASKED).reshape(words, 16, 1)
    e = jnp.exp(logits - jnp.max(logits, axis=1, keepdims=True))
    w = e / jnp.sum(e, axis=1, keepdims=True)
    return am3, w


def count_column(cnt_row):
    return jnp.transpose(jnp.broadcast_to(cnt_row, (GROUP, GROUP)))[:, 0:1]


def char_attn_tile(x, cnt, weights):
    g1, wqkv, wout = weights[:3]
    groups = x.shape[0] // GROUP
    xf = x.astype(F32)
    xhat, _ = ln_parts(xf)
    normed = (xhat * g1).astype(BF16)
    packed = mm(normed, wqkv).astype(BF16)
    low = pair_masks(GROUP)
    lw = word_of_lane(2 * GROUP)
    slot = lax.broadcasted_iota(jnp.int32, (16, 2 * GROUP), 0).astype(F32)
    raw, values, scores = [], [], []
    for g in range(groups):
        r = slice(g * GROUP, (g + 1) * GROUP)
        for p in range(CHEADS // 2):
            q = packed[r, 128 * p : 128 * p + 128] * BF16(0.125)
            values.append(packed[r, 512 + 128 * p : 640 + 128 * p])
            raw.append(mm_nt(packed[r, 256 + 128 * p : 384 + 128 * p], stack_heads(q, low)))
    pairs = len(raw)
    for i, st in enumerate(raw):
        cnt_row = cnt[i // 2 : i // 2 + 1, :]
        scores.append(jnp.where(slot < jnp.concatenate([cnt_row, cnt_row], axis=1), compress(st, lw), MASKED))
    scores = jnp.concatenate(scores, axis=0).reshape(pairs, 16, 2 * GROUP)
    e = jnp.exp(scores - jnp.max(scores, axis=1, keepdims=True))
    probs = e / jnp.sum(e, axis=1, keepdims=True)
    low_probs = probs.astype(BF16)
    spread = [expand(low_probs[i], lw) for i in range(pairs)]
    mixed = [mm_tn(pt, v) for pt, v in zip(spread, values)]
    mixed = [jnp.where(low, o[:GROUP], o[GROUP:]) for o in mixed]
    probs = jnp.concatenate([jnp.concatenate([probs[2 * g], probs[2 * g + 1]], axis=1) for g in range(groups)], axis=0)
    mixed = jnp.concatenate([jnp.concatenate(mixed[2 * g : 2 * g + 2], axis=1) for g in range(groups)], axis=0).astype(BF16)
    return packed, probs, mixed, xf + mm(mixed, wout)


def char_mlp_tile(aa, cnt, weights):
    _, _, _, g2, wup, wdown, pq = weights
    ahat, _ = ln_parts(aa)
    middle = (ahat * g2).astype(BF16)
    upper, dgelu = gelu_both(mm(middle, wup))
    upper = upper.astype(BF16)
    am = aa + mm(upper, wdown)
    cols = jnp.concatenate([count_column(cnt[g : g + 1, :]) for g in range(aa.shape[0] // GROUP)], axis=0)
    am3, w = pool_weights(am, pq, cols)
    pooled = jnp.sum(w * am3, axis=1)
    return upper, dgelu.astype(BF16), am, pooled.astype(BF16)


def count_lanes(counts):
    take = GROUP // 16
    w = lax.broadcasted_iota(jnp.int32, (128, GROUP), 0)
    l = lax.broadcasted_iota(jnp.int32, (128, GROUP), 1)
    spread = (lax.rem(w, take) == l // 16).astype(BF16)
    g = lax.broadcasted_iota(jnp.int32, (128 // take, 128), 0)
    lane = lax.broadcasted_iota(jnp.int32, (128 // take, 128), 1)
    rows = []
    for r in range(counts.shape[0]):
        one = jnp.where(lane // take == g, counts[r : r + 1, :].astype(F32), 0.0).astype(BF16)
        rows.append(mm(one, spread))
    return jnp.concatenate(rows, axis=0)


def full_spec(shape):
    return pl.BlockSpec(shape, lambda i: (0,) * len(shape))


def rows_spec(rows, width):
    return pl.BlockSpec((rows, width), lambda i: (i, 0))


def char_mlp_back(cnt, aa, upper, dgelu, am, gpool_ref, base, weights):
    _, _, _, g2, wup, wdown, pq = weights
    rows = aa.shape[0]
    words = rows // 16
    cols = jnp.concatenate([count_column(cnt[g : g + 1, :]) for g in range(rows // GROUP)], axis=0)
    _, w = pool_weights(am, pq, cols)
    gp = jnp.concatenate(
        [jnp.broadcast_to(gpool_ref[pl.ds(base + i, 1), :], (16, 256)) for i in range(words)], axis=0
    )
    dw = jnp.sum(gp * am, axis=-1, keepdims=True).reshape(words, 16, 1)
    dlog = (w * (dw - jnp.sum(w * dw, axis=1, keepdims=True))).reshape(rows, 1)
    gm = w.reshape(rows, 1) * gp + dlog * pq
    d_pq = jnp.sum(dlog * am, axis=0, keepdims=True)
    gdl = gm.astype(BF16)
    d_down_t = mm_tn(gdl, upper)
    ghid = (dgelu.astype(F32) * mm_nt(gdl, wdown)).astype(BF16)
    ahat, ar = ln_parts(aa)
    middle = (ahat * g2).astype(BF16)
    d_up = mm_tn(middle, ghid)
    gmid = mm_nt(ghid, wup)
    gca = gm + ln_back(ahat, ar, g2, gmid)
    d_g2 = jnp.sum(gmid * ahat, axis=0, keepdims=True)
    return gca, d_up, d_down_t, d_g2, d_pq


def char_attn_back(x, packed, probs, mixed, gca, weights):
    g1, wqkv, wout = weights[:3]
    groups = x.shape[0] // GROUP
    low = pair_masks(GROUP)
    lw = word_of_lane(2 * GROUP)
    gcl = gca.astype(BF16)
    d_out = mm_tn(mixed, gcl)
    gcm = mm_nt(gcl, wout).astype(BF16)
    keys, queries, grads, raw, prs = [], [], [], [], []
    for g in range(groups):
        r = slice(g * GROUP, (g + 1) * GROUP)
        for p in range(CHEADS // 2):
            queries.append(stack_heads(packed[r, 128 * p : 128 * p + 128] * BF16(0.125), low))
            keys.append(packed[r, 256 + 128 * p : 384 + 128 * p])
            grads.append(stack_heads(gcm[r, 128 * p : 128 * p + 128], low))
            raw.append(mm_nt(packed[r, 512 + 128 * p : 640 + 128 * p], grads[-1]))
            prs.append(probs[16 * g : 16 * g + 16, 256 * p : 256 * p + 256])
    pairs = len(raw)
    dp = jnp.concatenate([compress(v, lw) for v in raw], axis=0).reshape(pairs, 16, 2 * GROUP)
    pr = jnp.concatenate(prs, axis=0).reshape(pairs, 16, 2 * GROUP)
    ds = (pr * (dp - jnp.sum(pr * dp, axis=1, keepdims=True))).astype(BF16)
    pr = pr.astype(BF16)
    dst = [expand(ds[i], lw) for i in range(pairs)]
    pt = [expand(pr[i], lw) for i in range(pairs)]
    dq = [mm_tn(dst[i], keys[i]) for i in range(pairs)]
    dq = [jnp.where(low, o[:GROUP], o[GROUP:]) * 0.125 for o in dq]
    dk = [mm(dst[i], queries[i]) for i in range(pairs)]
    dv = [mm(pt[i], grads[i]) for i in range(pairs)]
    dqkv = [jnp.concatenate([v[2 * g + p] for v in (dq, dk, dv) for p in range(2)], axis=1) for g in range(groups)]
    dqkv = jnp.concatenate(dqkv, axis=0).astype(BF16)
    xhat, xr = ln_parts(x.astype(F32))
    normed = (xhat * g1).astype(BF16)
    gn = mm_nt(dqkv, wqkv)
    grad = gca + ln_back(xhat, xr, g1, gn)
    return grad, mm_tn(normed, dqkv), d_out, gn * xhat


def char_back_step(step, tiles, ins, cg, gca, accs, gains):
    x, cnt, packed, probs, mixed, aa, upper, dgelu, am, gpool, vec, qo, up, dn = ins
    a_qo, a_up, a_dn, a_vec = accs
    weights = char_weights(vec, qo, up, dn)

    @pl.when(step == 0)
    def _():
        for acc in accs:
            acc[...] = jnp.zeros_like(acc)

    @pl.when(step < tiles)
    def _():
        grad, d_up, d_dn, d_g2, d_pq = char_mlp_back(cnt[0], aa[...], upper[...], dgelu[...], am[...], gpool, step * (ROWS // 16), weights)
        gca[span(step * ROWS, ROWS), :] = grad
        if gains:
            a_vec[1:2, :256] += d_g2
        a_vec[2:3, :256] += d_pq
        for i in range(8):
            t, c = i // 2, i % 2
            a_up[c, :, 128 * t : 128 * t + 128] += d_up[:, 128 * i : 128 * i + 128]
        for c in range(2):
            a_dn[c] += d_dn[128 * c : 128 * c + 128, :]

    @pl.when(step >= tiles)
    def _():
        r = span((step - tiles) * ROWS, ROWS)
        grad, d_qkv, d_out, terms = char_attn_back(x[...], packed[...], probs[...], mixed[...], gca[r, :], weights)
        cg[...] = grad
        if gains:
            a_vec[0:1, :256] += jnp.sum(terms, axis=0, keepdims=True)
        for i in range(8):
            t, c = i // 2, i % 2
            val = d_qkv[:, 128 * i : 128 * i + 128] if i < 6 else d_out[:, 128 * (i - 6) : 128 * (i - 6) + 128]
            a_qo[c, :, 128 * t : 128 * t + 128] += val


ACCS = [(2, 256, 512), (2, 256, 512), (2, 128, 1024), (8, 512)]


def back_specs(tiles, gpool, weights):
    one = lambda i: jnp.minimum(i, tiles - 1)
    two = lambda i: jnp.maximum(i - tiles, 0)

    def rows_at(where, r, w):
        return pl.BlockSpec((r, w), lambda i: (where(i), 0))

    once = lambda sh: pl.BlockSpec(sh, lambda i: (0,) * len(sh), pipeline_mode=pl.Buffered(1))
    ins = [rows_at(two, ROWS, 256), pl.BlockSpec((1, ROWS // GROUP, GROUP), lambda i: (one(i), 0, 0))]
    ins += [rows_at(two, ROWS, 768), rows_at(two, ROWS // 8, 512), rows_at(two, ROWS, 256)]
    ins += [rows_at(one, ROWS, 256), rows_at(one, ROWS, 1024), rows_at(one, ROWS, 1024), rows_at(one, ROWS, 256)]
    ins += [once(gpool.shape)] + [once(w.shape) for w in weights]
    return ins, rows_at(two, ROWS, 256)


def char_bwd_kernel(tiles, *refs):
    ins, (cg, *accs), gca = refs[:14], refs[14:19], refs[19]
    char_back_step(pl.program_id(0), tiles, ins, cg, gca, accs, True)


def char_backward(x, cnt, saved, gpool, *weights):
    total = x.shape[0]
    tiles = total // ROWS
    ins, out = back_specs(tiles, gpool, weights)
    return pl.pallas_call(
        functools.partial(char_bwd_kernel, tiles),
        grid=(2 * tiles,),
        in_specs=ins,
        out_specs=[out] + [full_spec(s) for s in ACCS],
        out_shape=[jax.ShapeDtypeStruct((total, 256), F32)] + [jax.ShapeDtypeStruct(s, F32) for s in ACCS],
        scratch_shapes=[pltpu.VMEM((total, 256), F32)],
        compiler_params=pltpu.CompilerParams(vmem_limit_bytes=VMEM_LIMIT, dimension_semantics=("arbitrary",)),
        name="char_backward",
    )(x, cnt, *saved, gpool, *weights)


MESH = pl.DeviceIdType.MESH


def remote(src, dst, sems, index, where):
    return pltpu.make_async_remote_copy(
        src_ref=src, dst_ref=dst,
        send_sem=sems[0] if index is None else sems[0].at[index],
        recv_sem=sems[1] if index is None else sems[1].at[index],
        device_id=where, device_id_type=MESH,
    )


def span(start, size):
    return pl.ds(pl.multiple_of(start, size), size)


class Place:
    def __init__(self):
        self.f, self.c, self.t = lax.axis_index("fsdp"), lax.axis_index("ctx"), lax.axis_index("tp")
        self.F, self.T = lax.axis_size("fsdp"), lax.axis_size("tp")

    def fs(self, k):
        return lax.rem(self.f + k + self.F, self.F)

    def tp(self, k):
        return lax.rem(self.t + k + self.T, self.T)

    def peers(self):
        out = [{"fsdp": self.fs(k)} for k in range(1, self.F)]
        out += [{"tp": self.tp(k)} for k in range(1, self.T)]
        out += [{"ctx": 1 - self.c, "tp": self.tp(k)} for k in range(1, self.T)]
        return out + [{"ctx": 1 - self.c}]


def call(peers):
    for where in peers:
        pl.semaphore_signal(pltpu.get_barrier_semaphore(), inc=1, device_id=where, device_id_type=MESH)


def meet(peers):
    pl.semaphore_wait(pltpu.get_barrier_semaphore(), len(peers))


def greet(peers):
    call(peers)
    meet(peers)


class Piece:
    def __init__(self, at, shard, whole, mine, landing, region, sems, local_sem, first, side=True, core=None, source=None):
        self.at, self.shard, self.whole = at, shard, whole
        self.mine, self.landing, self.region = mine, landing, region
        self.sems, self.local_sem, self.first = sems, local_sem, first
        self.cores, self.core, self.source = side, core, source

    @staticmethod
    def slots(F, T):
        return (F - 1) + (T - 1) + T

    def held(self, act, other=False):
        if self.core is None:
            act()
        else:
            pl.when(self.at.c == (1 - self.core if other else self.core))(act)

    def local(self, src):
        at = self.at
        return pltpu.make_async_copy(src, self.whole.at[self.landing(at.f, at.c, at.t)], self.local_sem)

    def z(self, k, src=None):
        at = self.at
        f = at.fs(-k) if src is None else at.f
        dst = self.whole.at[self.landing(f, at.c, at.t)]
        return remote(dst if src is None else src, dst, self.sems, self.first + k - 1, {"fsdp": at.fs(k)})

    def plane(self, k, incoming=False):
        at = self.at
        r = self.whole.at[self.region(at.c, at.tp(-k) if incoming else at.t)]
        return remote(r, r, self.sems, self.first + at.F - 1 + k - 1, {"tp": at.tp(k)})

    def side(self, k, incoming=False):
        at = self.at
        c = at.c if self.core is not None else (1 - at.c if incoming else at.c)
        r = self.whole.at[self.region(c, at.tp(-k))]
        return remote(r, r, self.sems, self.first + at.F + at.T - 2 + k, {"ctx": 1 - at.c})

    def begin(self):
        at = self.at

        def go(src):
            self.local(src).start()
            for k in range(1, at.F):
                self.z(k, src).start()

        if self.source is not None:
            for cond, src in self.source:
                pl.when(cond)(functools.partial(go, src))
        else:
            self.held(lambda: go(self.shard.at[self.mine(at.c, at.t)]))

    def landed(self):
        at = self.at
        dst = self.whole.at[self.landing(at.f, at.c, at.t)]
        pltpu.make_async_copy(dst, dst, self.local_sem).wait()
        for k in range(1, at.F):
            self.z(k).wait_recv()

    def spread(self):
        def go():
            self.landed()
            if self.region is not None:
                for k in range(1, self.at.T):
                    self.plane(k).start()
                if self.cores:
                    self.side(0).start()

        self.held(go)

    def pass_on(self):
        def go():
            for k in range(1, self.at.T):
                self.plane(k, True).wait_recv()
                if self.cores:
                    self.side(k).start()

        if self.region is not None:
            self.held(go)

    def arrive(self):
        def go():
            for k in range(self.at.T):
                self.side(k, True).wait_recv()

        if self.region is not None and self.cores:
            self.held(go, True)

    def drain(self):
        def go():
            for k in range(1, self.at.F):
                self.z(k).wait_send()
            if self.region is not None:
                for k in range(1, self.at.T):
                    self.plane(k).wait_send()
                if self.cores:
                    for k in range(self.at.T):
                        self.side(k).wait_send()

        self.held(go)


ALL = slice(None)
GATHERED = [((256, 1024), BF16), ((256, 1024), BF16), ((4, 256, 256), BF16), ((256, 512), BF16), ((4, 8, 128), F32), ((3, 512, 512), BF16), ((512, 512), BF16), ((512, 256), BF16), ((256, 512), BF16)]


def gather_pieces(at, shards, wholes, sems, local_sems):
    F, T = at.F, at.T
    qkv, out, up, dn, pj, sm, w3, wo, wu, wd = shards
    rq, rd, rw = up.shape[0], dn.shape[0], w3.shape[1]
    cu = wu.shape[1] // 2
    lanes = lambda c, t: span(256 * t + 128 * c, 128)
    cols = (lambda c, t: (ALL, lanes(c, t)), lambda f, c, t: (span(f * rq, rq), lanes(c, t)), lambda c, t: (ALL, lanes(c, t)))
    n = qkv.shape[1] // 256
    inside = lax.rem(at.t, n)
    qo_source = [(at.t < n, qkv.at[:, span(256 * inside + 128 * at.c, 128)]), (at.t == n, out.at[:, span(128 * at.c, 128)])]
    quarter = rd // T
    slots = Piece.slots(F, T)
    specs = [
        (None, wholes[0], *cols, dict(source=qo_source)),
        (up, wholes[1], *cols, {}),
        (dn, wholes[2], lambda c, t: (span(quarter * t, quarter), span(128 * c, 128)), lambda f, c, t: (f, span(quarter * t, quarter), span(128 * c, 128)), lambda c, t: (ALL, span(quarter * t, quarter), span(128 * c, 128)), {}),
        (pj, wholes[3], lambda c, t: (ALL, span(128 * t, 128)), lambda f, c, t: (span(f * rq, rq), span(128 * t, 128)), lambda c, t: (ALL, span(128 * t, 128)), dict(core=0)),
        (sm, wholes[4], lambda c, t: (ALL, ALL), lambda f, c, t: (f,), None, dict(side=False)),
        (w3, wholes[5], lambda c, t: (span(0, 2),), lambda f, c, t: (span(0, 2), span(f * rw, rw), span(128 * t, 128)), lambda c, t: (span(0, 2), ALL, span(128 * t, 128)), dict(core=0)),
        (w3, wholes[5], lambda c, t: (pl.ds(2, 1),), lambda f, c, t: (pl.ds(2, 1), span(f * rw, rw), span(128 * t, 128)), lambda c, t: (pl.ds(2, 1), ALL, span(128 * t, 128)), dict(core=1)),
        (wo, wholes[6], lambda c, t: (ALL, ALL), lambda f, c, t: (span(t * rw, rw), span(128 * f, 128)), lambda c, t: (span(t * rw, rw), ALL), dict(core=1)),
        (wu, wholes[7], lambda c, t: (ALL, span(cu * c, cu)), lambda f, c, t: (span(f * rw, rw), ALL), None, {}),
        (wd, wholes[8], lambda c, t: (span(cu * c, cu), ALL), lambda f, c, t: (ALL, span(f * rw, rw)), None, {}),
    ]
    return [
        Piece(at, shard, whole, mine, landing, region, sems, local_sems.at[i], i * slots, **more)
        for i, (shard, whole, mine, landing, region, more) in enumerate(specs)
    ]


PIECES = 10


FWD_OUTS = [(ROWS, 768, BF16), (ROWS // 8, 512, F32), (ROWS, 256, BF16), (ROWS, 256, F32), (ROWS, 1024, BF16), (ROWS, 1024, BF16), (ROWS, 256, F32), (ROWS // 16, 256, BF16)]


def char_weights(vec, qo, up, dn):
    return (vec[0:1, :256], qo[:, :768], qo[:, 768:], vec[1:2, :256], up[...], dn[...], vec[2:3, :256])


def char_fwd_kernel(x, cnt, vec, qo, up, dn, *outs):
    w = char_weights(vec, qo, up, dn)
    first = char_attn_tile(x[...], cnt[0], w)
    for ref, val in zip(outs, first + char_mlp_tile(first[3], cnt[0], w)):
        ref[...] = val


def char_forward(x, cnt, *weights):
    tiles = x.shape[0] // ROWS
    return pl.pallas_call(
        char_fwd_kernel,
        grid=(tiles,),
        in_specs=[rows_spec(ROWS, 256), pl.BlockSpec((1, ROWS // GROUP, GROUP), lambda i: (i, 0, 0))] + [full_spec(w.shape) for w in weights],
        out_specs=[rows_spec(r, w) for r, w, _ in FWD_OUTS],
        out_shape=[jax.ShapeDtypeStruct((r * tiles, w), d) for r, w, d in FWD_OUTS],
        compiler_params=pltpu.CompilerParams(vmem_limit_bytes=VMEM_LIMIT, dimension_semantics=("arbitrary",)),
        name="char_forward",
    )(x, cnt, *weights)


def vectors(sm):
    rows = []
    for i, n in enumerate((64, 64, 64, 128, 128)):
        v = jnp.concatenate([sm[f, i : i + 1, :n] for f in range(sm.shape[0])], axis=1)
        rows.append(v if n == 128 else jnp.concatenate([v, jnp.zeros_like(v)], axis=1))
    return jnp.concatenate(rows + [jnp.zeros((3, 512), F32)], axis=0)


CHUNKS = ((0, 4), (4, 6), (6, 8))
LAG = 6


def gather_fwd_kernel(*refs):
    refs = list(refs)
    take = lambda n: [refs.pop(0) for _ in range(n)]
    x, counts, words_in = take(3)
    small_in = take(5)
    shards = take(PIECES - 1)
    outs = take(len(FWD_OUTS))
    full_out = take(len(GATHERED))
    vec_out, cnt_out, xall = take(3)
    wholes = take(len(GATHERED))
    vec, cnt, xown, pool, kept, small, send, recv, xsend, xrecv, local_sems = refs
    shards.insert(5, small)
    at = Place()
    T = at.T
    own = at.c * T + at.t
    part = ROWS // 16
    pieces = gather_pieces(at, shards, wholes, (send, recv), local_sems)
    qo, up, dn, pj, sm, wa, wb, wo, zu, zd = pieces
    step = pl.program_id(0)
    last = pl.num_programs(0) - 1

    def out(i):
        return pltpu.make_async_copy(wholes[i], full_out[i], local_sems.at[PIECES + i])

    def chunk(i):
        lo, hi = CHUNKS[i]
        return span(lo * part, (hi - lo) * part) if lo % (hi - lo) == 0 else pl.ds(lo * part, (hi - lo) * part)

    def row_copy(i, k, incoming=False):
        dst = xall.at[at.c * T + (at.tp(-k) if incoming else at.t), chunk(i)]
        return remote(dst if incoming else xown.at[chunk(i)], dst, (xsend, xrecv), i * 2 * T + k - 1, {"tp": at.tp(k)})

    def side_copy(i, k):
        dst = xall.at[at.tp(-k), chunk(i)]
        return remote(xown.at[chunk(i)] if k == 0 else dst, dst, (xsend, xrecv), i * 2 * T + T - 1 + k, {"ctx": 1 - at.c})

    def keep(i):
        return pltpu.make_async_copy(xown.at[chunk(i)], xall.at[own, chunk(i)], local_sems.at[PIECES + len(GATHERED) + i])

    def cross_copy(k):
        dst = xall.at[own, chunk(1)]
        return remote(xown.at[chunk(1)], dst, (xsend, xrecv), 2 * T + T - 1 + k, {"ctx": 1, "tp": at.tp(k)})

    def crossed(k):
        dst = xall.at[at.tp(-k), chunk(1)]
        return remote(dst, dst, (xsend, xrecv), 2 * T + T - 1 + k, {"ctx": 1 - at.c})

    def send_rows(i):
        keep(i).start()
        for k in range(1, T):
            pl.when(((at.c == 0) & (i == 0)) | (at.t + k < T))(lambda k=k: row_copy(i, k).start())

        @pl.when(at.c == 0)
        def _():
            for k in range(T if i else 1):
                (cross_copy(k) if i else side_copy(0, 0)).start()

    def pass_rows(i):
        @pl.when(at.c == 0)
        def _():
            for k in range(1, T):
                row_copy(i, k, True).wait_recv()
                side_copy(i, k).start()

    def take_rows(i):
        for k in range(T):
            pl.when(at.c == 1)(lambda k=k: (crossed(k) if i else side_copy(i, k)).wait_recv())
        for k in range(1, T):
            pl.when((at.t >= k) & ((at.c == 1) | (i == 1)))(lambda k=k: row_copy(i, k, True).wait_recv())

    def drain_rows(i):
        keep(i).wait()
        for k in range(1, T):
            pl.when(((at.c == 0) & (i == 0)) | (at.t + k < T))(lambda k=k: row_copy(i, k).wait_send())

        @pl.when(at.c == 0)
        def _():
            for k in range(T):
                (cross_copy(k) if i else side_copy(0, k)).wait_send()

    tiles = pl.num_programs(0) - LAG

    def when(i, *acts):
        @pl.when(step == i)
        def _():
            for act in acts:
                act()

    def open_():
        small[...] = jnp.zeros_like(small)
        for i, v in enumerate(small_in):
            small[i : i + 1, : v.shape[1]] = v[...].astype(F32)
        greet(at.peers())
        for p in (qo, sm):
            p.begin()
        cnt[...] = count_lanes(counts[...])
        cnt_out[...] = cnt[...]
        qo.spread()
        for p in (up, dn):
            p.begin()
        sm.spread()
        vec[...] = vectors(wholes[4])
        vec_out[...] = vec[...]
        qo.pass_on()
        qo.arrive()
        for p in (up, dn):
            p.spread()
        for p in (pj, wa, wb, wo):
            p.begin()

    def copy_out(*which):
        for i in which:
            out(i).start()

    groups = ROWS // GROUP

    def count_rows(i):
        return jnp.concatenate([cnt[pl.ds(i * groups + g, 1), :] for g in range(groups)], axis=0)

    def rows_of(i):
        r = chunk(i)
        start = words_in[r, :].astype(F32) + mm(pool[r, :], wholes[3][...])
        xown[r, :] = (ln_parts(start)[0] * vec[3:4, :]).astype(BF16)

    when(0, open_)
    when(6, *[p.spread for p in (pj, wa, wb, wo)])
    when(7, zu.begin, zd.begin)
    when(8, pj.pass_on)
    when(9, pj.arrive, lambda: copy_out(0, 1, 2))
    when(10, lambda: send_rows(0))
    when(12, wa.pass_on, wb.pass_on, wo.pass_on, lambda: send_rows(1), lambda: copy_out(3))
    when(13, lambda: pass_rows(0), wa.arrive, wb.arrive, wo.arrive, lambda: copy_out(5, 6), zu.spread, zd.spread, lambda: copy_out(7, 8))

    @pl.when(step < tiles)
    def _():
        first = char_attn_tile(x[...], count_rows(step), (vec[0:1, :256], wholes[0][:, :768], wholes[0][:, 768:]))
        for ref, val in zip(outs[:4], first):
            ref[...] = val
        kept[lax.rem(step, LAG + 1)] = first[3]

    when(LAG, *[p.pass_on for p in (up, dn)], *[p.arrive for p in (up, dn)])

    @pl.when(step >= LAG)
    def _():
        i = step - LAG
        second = char_mlp_tile(kept[lax.rem(i, LAG + 1)], count_rows(i), (None, None, None, vec[1:2, :256], wholes[1][...], wholes[2][...].reshape(1024, 256), vec[2:3, :256]))
        for ref, val in zip(outs[4:], second):
            ref[...] = val
        pool[span(i * part, part), :] = second[3]

    when(3 + LAG, lambda: rows_of(0))
    when(5 + LAG, lambda: rows_of(1))

    @pl.when(step == last)
    def _():
        rows_of(2)
        keep(2).start()
        for p in pieces:
            p.drain()
        for i in (0, 1, 2, 3, 5, 6, 7, 8):
            out(i).wait()
        for i in range(2):
            take_rows(i)
            drain_rows(i)
        keep(2).wait()


def gather_forward(x, counts, words_in, small, shards):
    tiles = x.shape[0] // ROWS
    F, T = lax.axis_size("fsdp"), lax.axis_size("tp")
    any_ = pl.BlockSpec(memory_space=pl.ANY)
    count = PIECES * Piece.slots(F, T)
    words, width = words_in.shape
    nchunk = len(CHUNKS) * 2 * T

    def early(r, w):
        return pl.BlockSpec((r, w), lambda i: (jnp.minimum(i, tiles - 1), 0))

    def late(r, w):
        return pl.BlockSpec((r, w), lambda i: (jnp.maximum(i - LAG, 0), 0))

    return pl.pallas_call(
        gather_fwd_kernel,
        grid=(tiles + LAG,),
        in_specs=[early(ROWS, 256), full_spec(counts.shape), full_spec(words_in.shape)] + [full_spec(v.shape) for v in small] + [any_] * len(shards),
        out_specs=[early(r, w) for r, w, _ in FWD_OUTS[:4]] + [late(r, w) for r, w, _ in FWD_OUTS[4:]] + [any_] * len(GATHERED) + [full_spec((8, 512)), full_spec((x.shape[0] // GROUP, GROUP)), any_],
        out_shape=[jax.ShapeDtypeStruct((r * tiles, w), d) for r, w, d in FWD_OUTS]
        + [jax.ShapeDtypeStruct(sh, d) for sh, d in GATHERED]
        + [jax.ShapeDtypeStruct((8, 512), F32), jax.ShapeDtypeStruct((x.shape[0] // GROUP, GROUP), F32), jax.ShapeDtypeStruct((2 * T, words, width), BF16)],
        scratch_shapes=[pltpu.VMEM(sh, d) for sh, d in GATHERED]
        + [pltpu.VMEM((8, 512), F32), pltpu.VMEM((x.shape[0] // GROUP, GROUP), F32), pltpu.VMEM((words, width), BF16), pltpu.VMEM((words, 256), BF16), pltpu.VMEM((LAG + 1, ROWS, 256), F32), pltpu.VMEM((8, 128), F32)]
        + [pltpu.SemaphoreType.DMA((n,)) for n in (count, count, nchunk, nchunk, PIECES + len(GATHERED) + len(CHUNKS))],
        compiler_params=pltpu.CompilerParams(vmem_limit_bytes=VMEM_LIMIT, collective_id=0, has_side_effects=True, dimension_semantics=("arbitrary",)),
        name="gather_forward",
    )(x, counts, words_in, *small, *shards)


def word_kernel(
    pooled, proj, words_in, cot, vec, xin, w3_in, wo_in, zu, zd,
    block_out, rms, words_grad, gpool, d_proj, d_vec, h_w4, h_up, h_down,
    xall, kk, vv, kt, vt, ss, ee, qm, dom, mx, ll, ot, dqt, w3, wout, wup, wdown, dk_acc, dv_acc, dlt, dk_sum, dv_sum,
    dx_in, dx_own, g_up, g_down, g_w4, in_up, in_down, in_w4,
    xlast, w_send, w_recv, g_send, g_recv, rs_send, rs_recv, x_send, x_recv, local_sems,
):
    at = Place()
    T = at.T
    own = at.c * T + at.t
    nblk, blk, width = xall.shape
    dx = kk
    half = HEADS // 2
    low = pair_masks(blk)
    first, second = range(half), range(half, HEADS)
    cu = zu.shape[1]
    loads = [pltpu.make_async_copy(src, dst, local_sems.at[i]) for i, (src, dst) in enumerate(((w3_in, w3), (xin, xall), (wo_in, wout)))]
    for load in loads:
        load.start()

    near = (at.t + 1 - 2 * lax.rem(at.t, 2), lax.rem(at.t + 2, T))
    far = T - 1 - at.t

    def area(c, t, i, part=None):
        r = span(2 * cu * t + cu * c, cu)
        if part is None:
            return wup.at[:, r] if i == 0 else wdown.at[r, :]
        if i == 0:
            return wup.at[pl.ds(part * width // 2, width // 2), r]
        return wdown.at[span(2 * cu * t + cu * c + part * (cu // 2), cu // 2), :]

    def wide(n, i, incoming=False):
        dst = area(at.c, near[n] if incoming else at.t, i)
        return remote(dst if incoming else (zu, zd)[i], dst, (w_send, w_recv), 2 * n + i, {"tp": near[n]})

    def onward(n, i, incoming=False):
        dst = area(at.c, far if incoming else near[1 - n], i, n)
        return remote(dst, dst, (w_send, w_recv), 4 + 2 * n + i, {"tp": near[n]})

    def side(k, i, incoming=False):
        t = (at.t, near[0], near[1], far)[k]
        dst = area(1 - at.c if incoming else at.c, t, i)
        return remote((zu, zd)[i] if k == 0 and not incoming else dst, dst, (w_send, w_recv), 8 + 2 * k + i, {"ctx": 1 - at.c})

    def mine(i):
        return pltpu.make_async_copy((zu, zd)[i], area(at.c, at.t, i), local_sems.at[3 + i])

    plane = [{"ctx": i, "tp": at.tp(k)} for i in (at.c, 1 - at.c) for k in range(T) if k > 0] + [{"ctx": 1 - at.c}]
    call(plane)
    tail = xlast.shape[1]
    lead = blk - tail

    start = words_in[...].astype(F32) + mm(pooled[...], proj[...])
    shat, sr = ln_parts(start)
    g1v = vec[3:4, :]
    wq, wk, wv = w3.at[0], w3.at[1], w3.at[2]
    loads[0].wait()
    loads[1].wait()
    xown = xall[own]
    q = mm(xown, wq[...]).astype(BF16) * BF16(0.125)
    for p in range(HEADS // 2):
        a, b = split_heads(q[:, 128 * p : 128 * p + 128], low)
        qm[2 * p] = a
        qm[2 * p + 1] = b
    mx[...] = jnp.full(mx.shape, MASKED, F32)
    ll[...] = jnp.zeros(ll.shape, F32)
    ot[...] = jnp.zeros(ot.shape, F32)
    dqt[...] = jnp.zeros(dqt.shape, F32)
    dk_sum[...] = jnp.zeros(dk_sum.shape, F32)
    dv_sum[...] = jnp.zeros(dv_sum.shape, F32)

    def scores_of(j, heads):
        for h in heads:
            p = h // 2
            s = mm_nt(kk[j, :, 128 * p : 128 * p + 128], qm[h])
            ss[j, h % half] = s
            mx[h] = jnp.maximum(mx[h], jnp.max(s.reshape(blk // 8, 8, blk), axis=0))

    def mix_of(j, heads):
        for h in heads:
            e = jnp.exp(ss[j, h % half] - mx[h, 0:1, :])
            ll[h] += jnp.sum(e.reshape(blk // 8, 8, blk), axis=0)
            eb = e.astype(BF16)
            ee[j, h] = eb
            ot[64 * h : 64 * h + 64, :] += mm(vt[j, 64 * h : 64 * h + 64, :], eb)

    def top_of(heads):
        for h in heads:
            mx[h] = jnp.broadcast_to(jnp.max(mx[h], axis=0, keepdims=True), (8, blk))

    meet(plane)

    def got_rows(j, sem):
        pltpu.make_async_remote_copy(
            src_ref=xlast.at[j], dst_ref=xlast.at[j], send_sem=x_send.at[0], recv_sem=x_recv.at[sem],
            device_id={"ctx": 1 - at.c}, device_id_type=MESH,
        ).wait_recv()
        xall[j, lead:, :] = xlast[j]

    for k in range(T):

        @pl.when((at.c == 0) & (at.t + k < T) & (k > 0))
        def _():
            if k:
                remote(xin.at[own, pl.ds(lead, tail)], xlast.at[own], (x_send.at[2 * k], x_recv.at[2 * k]), None, {"ctx": 0, "tp": at.tp(k)}).start()

        @pl.when((at.c == 0) | ((at.t + k < T) & (k > 0)))
        def _():
            remote(xin.at[own, pl.ds(lead, tail)], xlast.at[own], (x_send.at[2 * k + 1], x_recv.at[2 * k + 1 + 2 * T * at.c]), None, {"ctx": 1, "tp": at.tp(k)}).start()


    for i in range(2):
        for n in range(2):
            wide(n, i).start()
        side(0, i).start()
        mine(i).start()

    def others():
        for k in range(T):
            pl.when((at.c == 0) & (at.t >= k) & (k > 0))(lambda k=k: got_rows(at.t - k, 2 * k))
            pl.when(at.c == 1)(lambda k=k: got_rows(at.tp(-k), 2 * k + 1))
            pl.when((at.c == 1) & (at.t >= k) & (k > 0))(lambda k=k: got_rows(T + at.t - k, 2 * k + 1 + 2 * T))

    @pl.loop(0, own + 1)
    def _(m):
        pl.when(m == 1)(others)
        j = own - m
        xj = xall[j]
        kj = mm(xj, wk[...]).astype(BF16)
        vj = mm(xj, wv[...]).astype(BF16)
        kk[j] = kj
        vv[j] = vj
        kt[j] = jnp.transpose(kj)
        vt[j] = jnp.transpose(vj)
        scores_of(j, first)

    top_of(first)
    for i in range(2):
        for n in range(2):
            wide(n, i, True).wait_recv()
        for n in range(2):
            onward(n, i).start()
            side(1 + n, i).start()

    @pl.loop(0, own + 1)
    def _(j):
        mix_of(j, first)
        scores_of(j, second)

    top_of(second)

    @pl.loop(0, own + 1)
    def _(j):
        mix_of(j, second)

    for h in range(HEADS):
        linv = 1.0 / jnp.sum(ll[h], axis=0, keepdims=True)
        ll[h] = jnp.broadcast_to(linv, (8, blk))
        ot[64 * h : 64 * h + 64, :] = ot[64 * h : 64 * h + 64, :] * linv
    mixed_t = ot[...].astype(BF16)
    mixed = jnp.transpose(mixed_t)
    loads[2].wait()
    attn = mm(mixed, wout[...])
    awa = start + attn
    ahat, ar = ln_parts(awa)
    g2v = vec[4:5, :]
    n2 = (ahat * g2v).astype(BF16)
    for i in range(2):
        for n in range(2):
            onward(n, i, True).wait_recv()
        side(3, i).start()
    for i in range(2):
        mine(i).wait()
        for k in range(4):
            side(k, i, True).wait_recv()
    upper, dgelu = gelu_both(mm(n2, wup[...]))
    upper = upper.astype(BF16)
    mlp = mm(upper, wdown[...])
    final = awa + mlp
    block_out[...] = final.astype(BF16)
    lane = lax.broadcasted_iota(jnp.int32, (blk, 128), 1)
    cols = [jnp.sqrt(jnp.mean(v * v, axis=-1, keepdims=True)) for v in (attn, mlp, final)]
    rms[...] = jnp.transpose(jnp.where(lane == 0, cols[0], jnp.where(lane == 1, cols[1], cols[2])))[0:3, :]
    cotv = cot[...]
    gdown = mm_tn(upper, cotv).astype(BF16)
    ghid = (dgelu * mm_nt(cotv, wdown[...])).astype(BF16)
    gup = mm_tn(n2, ghid).astype(BF16)
    for c in range(2):
        for t in range(T):
            g_down[c, cu * t : cu * t + cu, :] = gdown[cu * (2 * t + c) : cu * (2 * t + c) + cu, :]
            g_up[c, :, cu * t : cu * t + cu] = gup[:, cu * (2 * t + c) : cu * (2 * t + c) + cu]
    grads = ((g_down, in_down, h_down), (g_up, in_up, h_up), (g_w4, in_w4, h_w4))

    def swap(i):
        return remote(grads[i][0].at[1 - at.c], grads[i][1], (g_send, g_recv), i, {"ctx": 1 - at.c})

    def store(i):
        return pltpu.make_async_copy(grads[i][0].at[at.c], grads[i][2], local_sems.at[5 + i])

    def add_halves(i):
        g, other, _ = grads[i]
        swap(i).wait_recv()
        g[at.c] = (g[at.c].astype(F32) + other[...].astype(F32)).astype(BF16)
        store(i).start()

    gn2 = mm_nt(ghid, wup[...])
    d_g2 = jnp.sum(gn2 * ahat, axis=0, keepdims=True)
    ga = cotv.astype(F32) + ln_back(ahat, ar, g2v, gn2)
    gal = ga.astype(BF16)
    g_w4[1, 1] = mm_tn(gal, mixed).astype(BF16)
    swap(0).start()
    swap(1).start()
    do_t = mm_nt(wout[...], gal).astype(BF16)
    do_s = []
    for h in range(HEADS):
        r = slice(64 * h, 64 * h + 64)
        d = do_t[r, :].astype(F32)
        linv = ll[h, 0:1, :]
        dlt[h] = jnp.broadcast_to(jnp.sum(d * ot[r, :], axis=0, keepdims=True) * linv, (8, blk))
        do_s.append((d * linv).astype(BF16))
    do = jnp.transpose(jnp.concatenate(do_s, axis=0))
    for p in range(HEADS // 2):
        a, b = split_heads(do[:, 128 * p : 128 * p + 128], low)
        dom[2 * p] = a
        dom[2 * p + 1] = b

    add_halves(0)
    add_halves(1)

    def grad_copy(j):
        return remote(dx.at[j], dx_in.at[own], (rs_send.at[j], rs_recv.at[own]), None, {"ctx": j // T, "tp": lax.rem(j, T)})

    @pl.loop(0, own + 1)
    def _(j):
        @pl.when(j > 0)
        def _():
            grad_copy(j - 1).start()

        for p in range(HEADS // 2):
            c = slice(128 * p, 128 * p + 128)
            vp = vv[j, :, c]
            dk = None
            for h in (2 * p, 2 * p + 1):
                e = ee[j, h]
                dp = mm_nt(vp, dom[h])
                ds = (e.astype(F32) * (dp - dlt[h, 0:1, :])).astype(BF16)
                dvh = mm(e, dom[h])
                dkh = mm(ds, qm[h])
                dk, dv = (dkh, dvh) if dk is None else (dk + dkh, dv + dvh)
                dqt[64 * h : 64 * h + 64, :] += mm(kt[j, 64 * h : 64 * h + 64, :], ds)
            dk_acc[:, c] = dk.astype(BF16)
            dv_acc[:, c] = dv.astype(BF16)
        dk = dk_acc[...]
        dv = dv_acc[...]
        dxj = mm_nt(dk, wk[...]) + mm_nt(dv, wv[...])
        dx[j] = dxj.astype(BF16)
        dx_own[...] = dxj
        xt = jnp.transpose(xall[j])
        dk_sum[...] += mm(xt, dk)
        dv_sum[...] += mm(xt, dv)

    dq = jnp.transpose((dqt[...] * 0.125).astype(BF16))
    g_w4[0, 0] = mm_tn(xown, dq).astype(BF16)
    g_w4[0, 1] = dk_sum[...].astype(BF16)
    g_w4[1, 0] = dv_sum[...].astype(BF16)
    swap(2).start()
    dx_own[...] += mm_nt(dq, wq[...])

    @pl.loop(own + 1, nblk)
    def _(b):
        remote(dx.at[own], dx_in.at[b], (rs_send.at[b], rs_recv.at[b]), None, {"ctx": 1 - at.c}).wait_recv()
        dx_own[...] += dx_in[b].astype(F32)

    gnf = dx_own[...]
    grad = ga + ln_back(shat, sr, g1v, gnf)
    words_grad[...] = grad
    d_vec[...] = jnp.concatenate([jnp.sum(gnf * shat, axis=0, keepdims=True), d_g2, jnp.zeros((6, width), F32)], axis=0)
    gproj = grad.astype(BF16)
    gproj_w = mm_tn(pooled[...], gproj).astype(BF16)
    hr = gproj_w.shape[0] // (2 * at.F)
    for i in range(at.F):
        for c in range(2):
            d_proj[c, hr * i : hr * i + hr, :] = gproj_w[hr * (2 * i + c) : hr * (2 * i + c) + hr, :]
    gpool[...] = mm_nt(gproj, proj[...])

    add_halves(2)
    for k in range(T):
        pl.when((at.c == 0) & (at.t + k < T) & (k > 0))(lambda k=k: remote(xin.at[own, pl.ds(lead, tail)], xlast.at[own], (x_send.at[2 * k], x_recv.at[2 * k]), None, {"ctx": 0, "tp": at.tp(k)}).wait_send() if k else None)
        pl.when((at.c == 0) | ((at.t + k < T) & (k > 0)))(lambda k=k: remote(xin.at[own, pl.ds(lead, tail)], xlast.at[own], (x_send.at[2 * k + 1], x_recv.at[2 * k + 1]), None, {"ctx": 1 - at.c}).wait_send())
    for i in range(2):
        for n in range(2):
            wide(n, i).wait_send()
            onward(n, i).wait_send()
        for k in range(4):
            side(k, i).wait_send()
    for i in range(3):
        swap(i).wait_send()
        store(i).wait()

    @pl.loop(0, own)
    def _(j):
        grad_copy(j).wait_send()


def word_section(pooled, proj, words_in, cot, vec, xall, w3, wo, zu, zd):
    blk, width = words_in.shape
    T = lax.axis_size("tp")
    nblk = 2 * T
    cu = zu.shape[1]
    ff = 2 * T * cu
    vm = pl.BlockSpec(memory_space=pltpu.VMEM)
    any_ = pl.BlockSpec(memory_space=pl.ANY)
    out_shapes = [((blk, width), BF16), ((3, blk), F32), ((blk, width), F32), ((blk, pooled.shape[1]), F32), ((2, proj.shape[0] // 2, width), BF16), ((8, width), F32)]
    halves = [((2, width, width), BF16), ((width, ff // 2), BF16), ((ff // 2, width), BF16)]
    bufs = [
        ((nblk, blk, width), BF16), ((nblk, blk, width), BF16), ((nblk, blk, width), BF16), ((nblk, width, blk), BF16), ((nblk, width, blk), BF16),
        ((nblk, HEADS // 2, blk, blk), F32), ((nblk, HEADS, blk, blk), BF16), ((HEADS, blk, 128), BF16), ((HEADS, blk, 128), BF16),
        ((HEADS, 8, blk), F32), ((HEADS, 8, blk), F32), ((width, blk), F32), ((width, blk), F32),
        ((3, width, width), BF16), ((width, width), BF16), ((width, ff), BF16), ((ff, width), BF16), ((blk, width), BF16), ((blk, width), BF16), ((HEADS, 8, blk), F32),
        ((width, width), F32), ((width, width), F32), ((nblk, blk, width), BF16), ((blk, width), F32),
        ((2, width, ff // 2), BF16), ((2, ff // 2, width), BF16), ((2, 2, width, width), BF16), ((width, ff // 2), BF16), ((ff // 2, width), BF16), ((2, width, width), BF16),
    ]
    nw = 16
    rows = (CHUNKS[-1][1] - CHUNKS[-1][0]) * (ROWS // 16)
    return pl.pallas_call(
        word_kernel,
        in_specs=[vm] * 5 + [any_] * 5,
        out_specs=[vm] * len(out_shapes) + [any_] * len(halves),
        out_shape=[jax.ShapeDtypeStruct(s, d) for s, d in out_shapes + halves],
        scratch_shapes=[pltpu.VMEM(s, d) for s, d in bufs] + [pltpu.VMEM((nblk, rows, width), BF16)] + [pltpu.SemaphoreType.DMA((n,)) for n in (nw, nw, 3, 3, nblk, nblk, 2 * T, 4 * T, 8)],
        compiler_params=pltpu.CompilerParams(vmem_limit_bytes=VMEM_LIMIT, collective_id=1, has_side_effects=True),
        name="word_section",
    )(pooled, proj, words_in, cot, vec, xall, w3, wo, zu, zd)


def sweep(shape, act, rows=32):
    rows = min(rows, shape[-2])

    @pl.loop(0, shape[-2] // rows)
    def _(i):
        act((ALL,) * (len(shape) - 2) + (span(i * rows, rows), ALL))


class Sum:
    def __init__(self, at, source, bufs, tp_cut, fs_cut, sems, first, wide, halved):
        self.at, self.source, self.sems, self.first, self.wide, self.halved = at, source, sems, first, wide, halved
        self.own, self.away, self.got, self.blocks, self.block, self.pieces, self.done = bufs
        self.hold, self.came = self.away, self.got
        self.near = (at.t + 1 - 2 * lax.rem(at.t, 2), lax.rem(at.t + 2, at.T))
        self.far = at.T - 1 - at.t
        self.fs_base = 5 if halved else at.T - 1
        self.tp_cut, self.fs_cut = tp_cut, fs_cut

    @staticmethod
    def slots(F, T):
        return 6 + (F - 1) + 2 * T

    @staticmethod
    def buffers(half, block, piece, F, T, wide, halved):
        quarter = (block[0] // 2,) + block[1:]
        first = [block, (4,) + quarter, (6,) + quarter, (1, 8, 128)] if halved else [half, half, half, (T - 1,) + block]
        shapes = first + [block, (F - 1,) + piece, ((2, T) if wide else (2,)) + piece]
        return [pltpu.VMEM(sh, BF16) for sh in shapes]

    def swap(self):
        at = self.at
        return remote(self.away, self.got, self.sems, self.first, {"ctx": 1 - at.c})

    def to_tp(self, k):
        src = self.source if self.halved else self.own
        return remote(src.at[self.tp_cut(self.at.tp(k))], self.blocks.at[k - 1], self.sems, self.first + k, {"tp": self.at.tp(k)})

    def to_fs(self, k):
        return remote(self.block.at[self.fs_cut(self.at.fs(k))], self.pieces.at[k - 1], self.sems, self.first + self.fs_base + k, {"fsdp": self.at.fs(k)})

    def share(self, k, x, incoming=False):
        at = self.at
        there = 1 - at.c if x else at.c
        c = there if incoming else at.c
        r = self.done.at[c, at.tp(-k) if incoming else at.t] if self.wide else self.done.at[c]
        return remote(r, r, self.sems, self.first + self.fs_base + at.F + 2 * k + x, {"ctx": there, "tp": at.tp(k)} if k else {"ctx": there})

    def shares(self):
        if not self.wide:
            return [(0, 1)]
        return [(k, x) for k in range(self.at.T) for x in range(2) if k or x]

    def local(self, i):
        src = self.source.at[self.at.c if i == 0 else 1 - self.at.c]
        return pltpu.make_async_copy(src, self.own if i == 0 else self.away, self.loc.at[i])

    def fetch(self, loc):
        self.loc = loc
        for i in range(2):
            self.local(i).start()

    def begin_fetched(self):
        for i in range(2):
            self.local(i).wait()
        self.swap().start()

    def begin(self):
        near, there = self.source.at[self.at.c], self.source.at[1 - self.at.c]

        def act(r):
            self.own[r] = near[r].astype(BF16)
            self.away[r] = there[r].astype(BF16)

        sweep(self.own.shape, act)
        self.swap().start()

    def halves(self):
        self.swap().wait_recv()

        def act(r):
            self.own[r] = (self.own[r].astype(F32) + self.got[r].astype(F32)).astype(BF16)

        sweep(self.own.shape, act)
        for k in range(1, self.at.T):
            self.to_tp(k).start()

    def part(self, t, i):
        cut = list(self.tp_cut(t))
        n = self.own.shape[0] // 2
        if cut[0] == ALL:
            cut[0] = pl.ds(i * n, n)
        else:
            cut[0] = span(t * 2 * n + i * n, n)
        return self.source.at[tuple(cut)]

    def mine(self, i):
        t, j = ((self.at.t, 0), (self.at.t, 1), (self.near[1], 0), (self.near[0], 1))[i]
        return pltpu.make_async_copy(self.part(t, j), self.hold.at[i], self.loc.at[i])

    def near_send(self, n, far):
        at = self.at
        src = self.part(self.far if far else self.near[n], n)
        return remote(src, self.came.at[2 * n + far], self.sems, self.first + 2 * n + far, {"tp": self.near[n]})

    def onward(self, n):
        return remote(self.hold.at[2 + n], self.came.at[4 + n], self.sems, self.first + 4 + n, {"tp": self.near[1 - n]})

    def begin_halved(self):
        for i in range(4):
            self.mine(i).start()
        for n in range(2):
            for far in (1, 0):
                self.near_send(n, far).start()

    def pass_halved(self):
        for i in range(4):
            self.mine(i).wait()
        for n in range(2):
            self.near_send(n, 1).wait_recv()
            mine, came = self.hold.at[2 + n], self.came.at[2 * n + 1]

            def act(r, mine=mine, came=came):
                mine[r] = (mine[r].astype(F32) + came[r].astype(F32)).astype(BF16)

            sweep(mine.shape, act)
        for n in range(2):
            self.onward(n).start()

    def over_near(self):
        n = self.own.shape[0] // 2
        for i in range(2):
            self.near_send(i, 0).wait_recv()
            self.onward(i).wait_recv()
            terms = (self.hold.at[i], self.came.at[2 * i], self.came.at[4 + i])
            block = self.block.at[pl.ds(i * n, n)]

            def act(r, terms=terms, block=block):
                block[r] = sum(v[r].astype(F32) for v in terms).astype(BF16)

            sweep(block.shape, act)
        for k in range(1, self.at.F):
            self.to_fs(k).start()

    def over_tp(self):
        own = self.own.at[self.tp_cut(self.at.t)]
        for k in range(1, self.at.T):
            self.to_tp(k).wait_recv()
        terms = [own] + [self.blocks.at[k - 1] for k in range(1, self.at.T)]

        def act(r):
            self.block[r] = sum(v[r].astype(F32) for v in terms).astype(BF16)

        sweep(self.block.shape, act)
        for k in range(1, self.at.F):
            self.to_fs(k).start()

    def over_fsdp(self):
        at = self.at
        for k in range(1, at.F):
            self.to_fs(k).wait_recv()
        terms = [self.block.at[self.fs_cut(at.f)]] + [self.pieces.at[k - 1] for k in range(1, at.F)]
        done = self.done.at[at.c, at.t] if self.wide else self.done.at[at.c]

        def act(r):
            done[r] = sum(v[r].astype(F32) for v in terms).astype(BF16)

        sweep(done.shape, act)
        for k, x in self.shares():
            self.share(k, x).start()

    def finish(self):
        for k, x in self.shares():
            self.share(k, x, True).wait_recv()

    def drain(self):
        at = self.at
        if self.halved:
            for n in range(2):
                for far in range(2):
                    self.near_send(n, far).wait_send()
                self.onward(n).wait_send()
        else:
            self.swap().wait_send()
            for k in range(1, at.T):
                self.to_tp(k).wait_send()
        for k in range(1, at.F):
            self.to_fs(k).wait_send()
        for k, x in self.shares():
            self.share(k, x).wait_send()


SUMS = [
    ((2, 512, 512), (2, 512, 128), (2, 128, 128), 2, 1, False, True),
    ((512, 1024), (512, 256), (128, 256), 1, 0, False, True),
    ((1024, 512), (256, 512), (256, 128), 0, 1, False, True),
    ((128, 512), (128, 128), (32, 128), 1, 0, True, False),
    ((256, 512), (256, 128), (64, 128), 1, 0, True, False),
    ((128, 1024), (32, 1024), (32, 256), 0, 1, True, False),
    ((256, 512), (256, 128), (64, 128), 1, 0, True, False),
]


def cutter(shape, axis, size):
    def cut(i):
        return tuple(span(i * size, size) if d == axis else ALL for d in range(len(shape)))

    return cut


def reduce_bwd_kernel(tiles, *refs):
    refs = list(refs)
    take = lambda n: [refs.pop(0) for _ in range(n)]
    ins = take(14)
    sources = take(4)
    (d_vec,) = take(1)
    (cg,) = take(1)
    results = take(len(SUMS))
    (vec_out,) = take(1)
    (gca,) = take(1)
    accs = take(len(ACCS))
    at = Place()
    bufs = [take(7) for _ in SUMS]
    vec_in, send, recv, vsend, vrecv, local_sems = refs
    slots = Sum.slots(at.F, at.T)
    a_qo, a_up, a_dn, a_vec = accs
    origin = list(sources) + [a_up, a_dn, a_qo]
    sums = []
    for i, (half, block, piece, ta, fa, wide, halved) in enumerate(SUMS):
        sums.append(Sum(at, origin[i], bufs[i], cutter(half, ta, block[ta]), cutter(block, fa, piece[fa]), (send, recv), i * slots, wide, halved))
        sums[i].loc = local_sems.at[i]
    w4, wup, wdn, pj, up, dn, qo = sums
    step = pl.program_id(0)
    last = 2 * tiles - 1

    plan = {}

    def when(i, *acts):
        plan.setdefault(i, []).extend(acts)

    def open_():
        meet(at.peers())
        w4.begin_halved()
        wup.begin_halved()
        pj.begin_fetched()

    when(0, lambda: call(at.peers()), lambda: pj.fetch(pj.loc))
    when(1, open_)
    when(3, pj.halves)
    when(6, w4.pass_halved, wup.pass_halved, wdn.begin_halved)
    when(8, lambda: vec_begin(), up.begin, dn.begin, pj.over_tp, w4.over_near)
    when(9, lambda: vec_plane(), wup.over_near)
    when(10, wdn.pass_halved, up.halves, dn.halves, pj.over_fsdp)
    when(11, lambda: vec_depth())
    when(13, w4.over_fsdp)
    when(13, wdn.over_near)
    when(14, up.over_tp, dn.over_tp, wup.over_fsdp)

    def vec_copy(i, where):
        return remote(a_vec, vec_in.at[i], (vsend, vrecv), i, where)

    def vec_begin():
        a_vec[3:5, :] = d_vec[0:2, :]
        vec_copy(0, {"ctx": 1 - at.c}).start()

    def vec_plane():
        vec_copy(0, {"ctx": 1 - at.c}).wait()
        a_vec[...] += vec_in[0]
        for k in range(1, at.T):
            vec_copy(k, {"tp": at.tp(k)}).start()

    def vec_depth():
        for k in range(1, at.T):
            vec_copy(k, {"tp": at.tp(k)}).wait()
        a_vec[...] += vec_in[1] + vec_in[2] + vec_in[3]
        for k in range(1, at.F):
            vec_copy(at.T - 1 + k, {"fsdp": at.fs(k)}).start()

    def vec_end():
        for k in range(1, at.F):
            vec_copy(at.T - 1 + k, {"fsdp": at.fs(k)}).wait()
        total = a_vec[...] + (vec_in[4] + vec_in[5] + vec_in[6])
        rows = [jnp.zeros((2, 128), F32)]
        for i, n in ((2, 64), (3, 128), (4, 128)):
            v = jnp.zeros((1, n), F32)
            for f in range(at.F):
                v = jnp.where(at.f == f, total[i : i + 1, f * n : f * n + n], v)
            rows.append(v if n == 128 else jnp.concatenate([v, jnp.zeros((1, n), F32)], axis=1))
        vec_out[...] = jnp.concatenate(rows + [jnp.zeros((3, 128), F32)], axis=0)

    busy = functools.reduce(lambda a, b: a | b, [step == i for i in plan])

    @pl.when(busy)
    def _():
        for i, acts in plan.items():

            @pl.when(step == i)
            def _():
                for act in acts:
                    act()

    char_back_step(step, tiles, ins, cg, gca, accs, False)

    @pl.when(step == last)
    def _():
        qo.begin()
        qo.halves()

        def result(i):
            return pltpu.make_async_copy(sums[i].done, results[i], local_sems.at[i, 0])

        def keep(*which):
            for i in which:
                sums[i].finish()
                result(i).start()

        vec_end()
        keep(0, 1, 3)
        qo.over_tp()
        up.over_fsdp()
        dn.over_fsdp()
        wdn.over_fsdp()
        qo.over_fsdp()
        keep(4, 5, 2)
        for s in sums[:6]:
            s.drain()
        keep(6)
        qo.drain()
        for i in range(len(sums)):
            result(i).wait()


def reduce_backward(x, cnt, saved, gpool, weights, sources, d_vec):
    total = x.shape[0]
    tiles = total // ROWS
    F, T = lax.axis_size("fsdp"), lax.axis_size("tp")
    ins, out = back_specs(tiles, gpool, weights)
    any_ = pl.BlockSpec(memory_space=pl.ANY)
    scratch = [pltpu.VMEM((total, 256), F32)] + [pltpu.VMEM(s, F32) for s in ACCS]
    results = []
    for half, block, piece, _, _, wide, halved in SUMS:
        scratch += Sum.buffers(half, block, piece, F, T, wide, halved)
        results.append(((2, T) if wide else (2,)) + piece)
    count = len(SUMS) * Sum.slots(F, T)
    vecs = 1 + (T - 1) + (F - 1)
    scratch += [pltpu.VMEM((vecs, 8, 512), F32)]
    scratch += [pltpu.SemaphoreType.DMA((n,)) for n in (count, count, vecs, vecs)] + [pltpu.SemaphoreType.DMA((len(SUMS), 4))]
    return pl.pallas_call(
        functools.partial(reduce_bwd_kernel, tiles),
        grid=(2 * tiles,),
        in_specs=ins + [any_] * len(sources) + [full_spec((8, 512))],
        out_specs=[out] + [any_] * len(results) + [full_spec((8, 128))],
        out_shape=[jax.ShapeDtypeStruct((total, 256), F32)] + [jax.ShapeDtypeStruct(s, BF16) for s in results] + [jax.ShapeDtypeStruct((8, 128), F32)],
        scratch_shapes=scratch,
        compiler_params=pltpu.CompilerParams(vmem_limit_bytes=VMEM_LIMIT, collective_id=2, has_side_effects=True, dimension_semantics=("arbitrary",)),
        name="reduce_backward",
    )(x, cnt, *saved, gpool, *weights, *sources, d_vec)


FINAL = [(3, 128, 128), (128, 128), (128, 512), (512, 128), (64, 512), (64, 1024), (256, 256), (64, 768), (64, 256), (1, 64), (1, 64), (1, 64), (1, 128), (1, 128)]


def final_kernel(cg, block, grad, rms, w4, wup, wdn, pj, up, dn, qo, vec, w_qkv, w_up, g1, g2, cg_out, block_out, grad_out, rms_out, *outs):
    cg_out[...] = cg[...]

    @pl.when(pl.program_id(0) == 0)
    def _():
        block_out[...] = block[...]
        grad_out[...] = grad[...]
        rms_out[...] = rms[...]
        o3, o_out, o_wup, o_wdn, o_pj, o_up, o_dn, o_qkv, o_cout = outs[:9]
        o3[0] = w4[0, 0].astype(F32)
        o3[1] = w4[0, 1].astype(F32)
        o3[2] = w4[1, 0].astype(F32)
        o_out[...] = jnp.transpose(w4[1, 1].astype(F32))
        for c in range(2):
            o_wup[:, 256 * c : 256 * c + 256] = wup[c].astype(F32)
            o_wdn[256 * c : 256 * c + 256, :] = wdn[c].astype(F32)
            for t in range(pj.shape[1]):
                i = 2 * t + c
                o_pj[32 * c : 32 * c + 32, 128 * t : 128 * t + 128] = pj[c, t].astype(F32)
                o_up[:, 128 * i : 128 * i + 128] = up[c, t].astype(F32)
                ref, i = (o_qkv, i) if i < 6 else (o_cout, i - 6)
                ref[:, 128 * i : 128 * i + 128] = qo[c, t].astype(F32)
        o_dn[...] = jnp.transpose(dn[...].astype(F32).reshape(256, 256))
        for i, n in enumerate((64, 64, 64, 128, 128)):
            if i > 1:
                outs[9 + i][...] = vec[i : i + 1, :n]
        for i, (w, d, gain) in enumerate(((w_qkv, o_qkv, g1), (w_up, o_up, g2))):
            col = jnp.sum(w[...].astype(F32) * d[...], axis=-1, keepdims=True)
            row = jnp.transpose(jnp.broadcast_to(col, (64, 128)))[0:1, :]
            outs[9 + i][...] = row / gain[...].astype(F32)


def finish(cg, block, grad, rms, parts):
    tiles = 2
    rows = cg.shape[0] // tiles
    small = [block, grad, rms] + list(parts)
    return pl.pallas_call(
        final_kernel,
        grid=(tiles,),
        in_specs=[rows_spec(rows, cg.shape[1])] + [full_spec(v.shape) for v in small],
        out_specs=[rows_spec(rows, cg.shape[1])] + [full_spec(v.shape) for v in small[:3]] + [full_spec(v) for v in FINAL],
        out_shape=[jax.ShapeDtypeStruct(v.shape, v.dtype) for v in [cg] + small[:3]] + [jax.ShapeDtypeStruct(v, F32) for v in FINAL],
        compiler_params=pltpu.CompilerParams(vmem_limit_bytes=VMEM_LIMIT, dimension_semantics=("arbitrary",)),
        name="finish",
    )(cg, block, grad, rms, *parts)


def gather(x, name, axis):
    return lax.all_gather(x, name, axis=axis, tiled=True)


def scatter(x, name, axis):
    return lax.psum_scatter(x, name, scatter_dimension=axis, tiled=True)


def fits(rows):
    return lax.axis_size("fsdp") == 4 and lax.axis_size("tp") == 4 and rows == 64


def local(characters, counts, words_in, cotangent, char_prenorm, char_qkv, char_out, char_midnorm, char_up, char_down,
          pool_query, char_proj, word_prenorm, word_qkv, word_out, word_midnorm, word_up, word_down):
    words, slots, cdim = characters.shape
    x = characters.reshape(words * slots, cdim)
    vectors_in = (char_prenorm, char_midnorm, pool_query, word_prenorm, word_midnorm)
    w3 = jnp.moveaxis(word_qkv, 1, 0)
    direct = fits(char_prenorm.shape[0])
    group_rows = (words * slots // ROWS, ROWS // GROUP, GROUP)
    if direct:
        shards = [char_qkv, char_out, char_up, char_down, char_proj, w3, word_out, word_up, word_down]
        *saved, pooled_low, qo, up, dn, proj, _, w3, wo, zu, zd, vec, cnt, xall = gather_forward(x, counts.reshape(words // 128, 128), words_in, [v.reshape(1, -1) for v in vectors_in], shards)
        dn = dn.reshape(1024, 256)
        cnt = cnt.reshape(group_rows)
    else:
        cnt = jnp.repeat(counts.astype(F32), slots).reshape(group_rows)
        wide = [gather(v.astype(F32), "fsdp", 0) for v in vectors_in]
        vec = jnp.stack([jnp.pad(v, (0, 512 - v.shape[0])) for v in wide] + [jnp.zeros((512,), F32)] * 3)
        qo = jnp.concatenate([gather(char_qkv, "fsdp", 0), gather(char_out, "fsdp", 0)], axis=1)
        up, dn, proj = (gather(w, "fsdp", 0) for w in (char_up, char_down, char_proj))
        w3 = gather(gather(w3, "fsdp", 1), "tp", 2)
        wo = gather(gather(word_out, "fsdp", 1), "tp", 0)
        cu = word_up.shape[1] // 2
        zu = lax.dynamic_slice_in_dim(gather(word_up, "fsdp", 0), lax.axis_index("ctx") * cu, cu, 1)
        zd = lax.dynamic_slice_in_dim(gather(word_down, "fsdp", 1), lax.axis_index("ctx") * cu, cu, 0)
        *saved, pooled_low = char_forward(x, cnt, vec, qo, up, dn)
        start, _ = ln_parts(words_in.astype(F32) + mm(pooled_low, proj))
        xall = gather((start * vec[3:4]).astype(BF16), ("ctx", "tp"), 0).reshape(-1, words, words_in.shape[1])
    (block_out, rms, words_grad, gpool, d_proj, d_vec, h_w4, h_up, h_down) = word_section(pooled_low, proj, words_in, cotangent, vec, xall, w3, wo, zu, zd)
    if direct:
        cg, *parts = reduce_backward(x, cnt, saved, gpool, [vec, qo, up, dn], [h_w4, h_up, h_down, d_proj], d_vec)
        cg, block_out, words_grad, rms, g_qkv4, g_wout, g_wup, g_wdown, g_proj, g_up, g_down, g_qkv, g_out, *vecs = finish(cg, block_out, words_grad, rms, parts + [char_qkv, char_up, char_prenorm.reshape(1, -1), char_midnorm.reshape(1, -1)])
        vecs = [v.reshape(-1) for v in vecs]
    else:
        cg, a_qo, a_up, a_dn, a_vec = char_backward(x, cnt, saved, gpool, vec, qo, up, dn)

        def reduce_char(g):
            g = lax.psum(g.astype(BF16), ("ctx", "tp"))
            return scatter(g, "fsdp", 0).astype(F32)

        def reduce_word(g, tp_axis, fsdp_axis, ctx_axis):
            g = scatter(scatter(g, "tp", tp_axis), "fsdp", fsdp_axis)
            return gather(g, "ctx", ctx_axis).astype(F32)

        lanes = lambda g, n: jnp.moveaxis(g.reshape(2, g.shape[1], -1, n), 0, 2).reshape(g.shape[1], -1)
        hr = char_proj.shape[0] // 2
        g_qo = reduce_char(lanes(a_qo, 128))
        g_qkv, g_out = g_qo[:, :768], g_qo[:, 768:]
        g_up = reduce_char(lanes(a_up, 128))
        g_down = reduce_char(a_dn.reshape(256, 1024).T)
        g_proj = reduce_char(jnp.moveaxis(d_proj.reshape(2, -1, hr, 512), 0, 1).reshape(256, 512))
        g_w4 = reduce_word(h_w4, 2, 1, 0)
        g_qkv4, g_wout = g_w4[:3], g_w4[3].T
        g_wup = reduce_word(h_up, 1, 0, 1)
        g_wdown = reduce_word(h_down, 0, 1, 0)
        vecs = [reduce_char(v) for v in (a_vec[0, :256], a_vec[1, :256], a_vec[2, :256], d_vec[0], d_vec[1])]
    return (
        block_out,
        cg.reshape(words, slots, cdim),
        words_grad,
        rms,
        vecs[0],
        g_qkv,
        g_out,
        vecs[1],
        g_up,
        g_down,
        vecs[2],
        g_proj,
        vecs[3],
        jnp.moveaxis(g_qkv4, 0, 1),
        g_wout,
        vecs[4],
        g_wup,
        g_wdown,
    )


def solution(mesh):
    rows = ("fsdp", "ctx", "tp")
    v, m = P("fsdp"), P("fsdp", None)
    return jax.shard_map(
        local,
        mesh=mesh,
        in_specs=(
            P(rows, None, None), P(rows), P(rows, None), P(rows, None),
            v, m, m, v, m, m, v, m, v, P("fsdp", None, "tp"), P("tp", "fsdp"), v, P("fsdp", "tp"), P("tp", "fsdp"),
        ),
        out_specs=(
            P(rows, None), P(rows, None, None), P(rows, None), P(None, rows),
            v, m, m, v, m, m, v, m, v, P("fsdp", None, "tp"), P("tp", "fsdp"), v, P("fsdp", "tp"), P("tp", "fsdp"),
        ),
        check_vma=False,
    )
```
